128 devices in a mesh: seq: 32 (over y, x, core), head: 4 (over z).
Axes of the slice: x: 4, y: 4, z: 4, core: 2. Of those that a mesh axis runs over, the one named last changes fastest.
Arguments:
- probe_vectors: bfloat16 [8192, 4096], P('seq', 'head'), may hold values from -6 to 6
- source_vectors: bfloat16 [8192, 4096], P('seq', 'head'), may hold values from -6 to 6
- content_vectors: bfloat16 [8192, 4096], P('seq', 'head'), may hold values from -6 to 6
- probe_direction_matrix: bfloat16 [8192, 4096], P('seq', 'head'), may hold values from -6 to 6
- probe_direction_source: bfloat16 [8192, 4096], P('seq', 'head'), may hold values from -6 to 6
- content_direction: bfloat16 [8192, 4096], P('seq', 'head'), may hold values from -6 to 6
- head_table_indices: int32 [32], P('head'), may hold values from 0 to 7
- reset_flags: int32 [8192], P('seq'), may hold values 0 or 1
- projection_matrix: bfloat16 [4096, 4096], P('head'), may hold values from -0.09375 to 0.09375
- regression_goal: bfloat16 [8192, 4096], P('seq'), may hold values from -6 to 6
Outputs:
- hess_q: bfloat16 [8192, 4096], P('seq', 'head')
- hess_k: bfloat16 [8192, 4096], P('seq', 'head')
- hess_v: bfloat16 [8192, 4096], P('seq', 'head')
The draws below stay inside these ranges and needn't reach their ends.
All inputs are finite; a program needn't handle non-finite values. No bound on the sum of `reset_flags` on one device may be relied on, other than what follows from the above.
Results may differ from the reference program's by a relative error of at most 0.024.
Values may be sent and summed in bfloat16 or wider, within the bound.
A program may use at most 128 MiB of HBM per device.

```python
import math
import jax
import jax.numpy as jnp
from jax import lax

D = 4096
HEADS = 32
HEAD_DIM = 128
SPAN_LENGTH = 256
LEVELS = 8
SEQUENCE_LENGTH = 8192
N_SEQ = 32
N_HEAD = 4


def set_ends(drawn, own_key, smallest, top_value):
    index_at = [jax.random.randint(jax.random.fold_in(own_key, axis), (), 0, length) for axis, length in enumerate(drawn.shape)]
    main_axis = drawn.shape.index(max(drawn.shape))
    neighbour = index_at[:main_axis] + [(index_at[main_axis] + 1) % drawn.shape[main_axis]] + index_at[main_axis + 1:]
    return drawn.at[tuple(index_at)].set(smallest).at[tuple(neighbour)].set(top_value)


def levels(own_key, extent, pieces, least, top_value):
    factor_of = 1.0
    for axis_at, blocks in pieces:
        draws = jax.random.uniform(jax.random.fold_in(jax.random.fold_in(own_key, 6), axis_at), (blocks,), jnp.float32, least / len(pieces), top_value / len(pieces))
        factor_of = factor_of * jnp.repeat(jnp.exp(draws), extent[axis_at] // blocks).reshape((-1,) + (1,) * (len(extent) - 1 - axis_at))
    return factor_of


def noise(stream_key, shape, width, most, shards=(), held_as=jnp.bfloat16):
    entries = width * jax.random.normal(stream_key, shape, jnp.float32)
    if shards:
        entries = entries * levels(stream_key, shape, shards, -0.22, 0.18)
    return jnp.clip(entries, -most, most).astype(held_as)


def setup_inputs(seed: int = 0) -> dict:
    streams_of = jax.random.split(jax.random.key(seed), 11)
    probe_vectors = noise(streams_of[0], (SEQUENCE_LENGTH, HEADS * HEAD_DIM), 1.0, 6.0, ((0, 32), (1, 4)))
    source_vectors = noise(streams_of[1], (SEQUENCE_LENGTH, HEADS * HEAD_DIM), 1.0, 6.0, ((0, 32), (1, 4)))
    content_vectors = noise(streams_of[2], (SEQUENCE_LENGTH, HEADS * HEAD_DIM), 1.0, 6.0, ((0, 32), (1, 4)))
    probe_direction_matrix = noise(streams_of[3], (SEQUENCE_LENGTH, HEADS * HEAD_DIM), 1.0, 6.0, ((0, 32), (1, 4)))
    probe_direction_source = noise(streams_of[4], (SEQUENCE_LENGTH, HEADS * HEAD_DIM), 1.0, 6.0, ((0, 32), (1, 4)))
    content_direction = noise(streams_of[5], (SEQUENCE_LENGTH, HEADS * HEAD_DIM), 1.0, 6.0, ((0, 32), (1, 4)))
    head_table_indices = set_ends(jax.random.randint(streams_of[6], (HEADS,), 0, LEVELS), jax.random.fold_in(streams_of[6], 1), 0, LEVELS - 1).astype(jnp.int32)
    reset_flags = set_ends((jax.random.randint(streams_of[7], (SEQUENCE_LENGTH,), 0, SEQUENCE_LENGTH) < 4).astype(jnp.int32), jax.random.fold_in(streams_of[7], 1), 0, 1)
    projection_matrix = noise(streams_of[8], (HEADS * HEAD_DIM, D), (HEADS * HEAD_DIM) ** -0.5, 0.09375, ((0, 4),))
    regression_goal = noise(streams_of[9], (SEQUENCE_LENGTH, D), 1.0, 6.0, ((0, 32),))
    return {"probe_vectors": probe_vectors, "source_vectors": source_vectors, "content_vectors": content_vectors, "probe_direction_matrix": probe_direction_matrix, "probe_direction_source": probe_direction_source, "content_direction": content_direction, "head_table_indices": head_table_indices, "reset_flags": reset_flags, "projection_matrix": projection_matrix, "regression_goal": regression_goal}


RESET_KEPT_SHARE = 0.7
EPS = 1e-06
HIGHEST = lax.Precision.HIGHEST

def log_gammas(head_table_indices, chain_len):
    fraction = head_table_indices.astype(jnp.float32) / (LEVELS - 1)
    rates = jnp.exp(math.log(1.0 / 32.0) + fraction * math.log(16.0 / chain_len))
    return jnp.log1p(-rates)

def segment_rate_exponents(reset_flags, forgetting_exponent):
    running_number = jnp.cumsum(reset_flags).astype(jnp.float32)
    position_indices = jnp.arange(1, reset_flags.shape[0] + 1).astype(jnp.float32)
    return position_indices[:, None] * forgetting_exponent[None, :] + math.log(RESET_KEPT_SHARE) * running_number[:, None]

def block_out(q, k, v, state, fading_rate_exponent):
    length = q.shape[0]
    scale = q.shape[2] ** (-0.5)
    scores = jnp.einsum('thd,shd->hts', q, k * scale, precision=HIGHEST)
    later = lax.broadcasted_iota(jnp.int32, (length, length), 0) >= lax.broadcasted_iota(jnp.int32, (length, length), 1)
    trans = fading_rate_exponent.T
    spread = trans[:, :, None] - trans[:, None, :]
    weights = jnp.where(later[None], jnp.exp(jnp.where(later[None], spread, 0.0)), 0.0)
    inner = jnp.einsum('hts,she->the', scores * weights, v, precision=HIGHEST)
    outer = jnp.exp(fading_rate_exponent)[:, :, None] * jnp.einsum('thd,hde->the', q, state, precision=HIGHEST)
    return inner + outer

def block_state(k, v, fading_rate_exponent):
    scale = k.shape[2] ** (-0.5)
    weights = jnp.exp(fading_rate_exponent[-1][None, :] - fading_rate_exponent)
    return jnp.einsum('shd,she->hde', k * (scale * weights[:, :, None]), v, precision=HIGHEST)

def group_norm(outputs):
    return outputs * lax.rsqrt(lax.optimization_barrier(jnp.mean(outputs * outputs, axis=-1, keepdims=True)) + EPS)

def head_sum(rows, weight):
    columns = rows.shape[1] // N_HEAD
    total_sum = jnp.zeros((rows.shape[0], weight.shape[1]), jnp.float32)
    for group in range(N_HEAD):
        piece = jnp.dot(rows[:, group * columns:(group + 1) * columns], weight[group * columns:(group + 1) * columns], preferred_element_type=jnp.float32)
        piece = lax.optimization_barrier(piece.astype(jnp.bfloat16)).astype(jnp.float32)
        total_sum = total_sum + piece
    return total_sum

def reference(probe_vectors, source_vectors, content_vectors, probe_direction_matrix, probe_direction_source, content_direction, head_table_indices, reset_flags, projection_matrix, regression_goal):

    def blocks(array):
        return array.astype(jnp.float32).reshape(N_SEQ, SPAN_LENGTH, HEADS, HEAD_DIM)
    q_rows, k_rows, v_rows = (blocks(probe_vectors), blocks(source_vectors), blocks(content_vectors))
    q_tan, k_tan, v_tan = (blocks(probe_direction_matrix), blocks(probe_direction_source), blocks(content_direction))
    forgetting_exponent = log_gammas(head_table_indices, float(SEQUENCE_LENGTH))
    fading_rate_exponent = jax.vmap(segment_rate_exponents, (0, None))(reset_flags.reshape(N_SEQ, SPAN_LENGTH), forgetting_exponent)
    decay_all = jnp.exp(fading_rate_exponent[:, -1, :])

    def own_state(item):
        key_b, value_b, key_t, value_t, logs_b = item
        return jax.jvp(lambda a, b: block_state(a, b, logs_b), (key_b, value_b), (key_t, value_t))
    state_own, state_tan = lax.map(own_state, (k_rows, v_rows, k_tan, v_tan, fading_rate_exponent))
    zero_state = jnp.zeros((HEADS, HEAD_DIM, HEAD_DIM), jnp.float32)

    def forward_step(carry, item):
        held, held_tan = carry
        decay_b, own_b, own_t = item
        factor = decay_b[:, None, None]
        return ((held * factor + own_b, held_tan * factor + own_t), (held, held_tan))
    unused_carry, (state_in, state_in_tan) = lax.scan(forward_step, (zero_state, zero_state), (decay_all, state_own, state_tan))
    target_blocks = regression_goal.reshape(N_SEQ, SPAN_LENGTH, D)

    def middle(item):
        q, k, v, qt, kt, vt, state, state_t, logs_b, wanted = item
        outputs, outputs_tan = jax.jvp(lambda a, b, c, d: block_out(a, b, c, d, logs_b), (q, k, v, state), (qt, kt, vt, state_t))
        normed, normed_tan = jax.jvp(group_norm, (outputs,), (outputs_tan,))
        summed = head_sum(normed.reshape(SPAN_LENGTH, -1).astype(jnp.bfloat16), projection_matrix)
        summed_tan = head_sum(normed_tan.reshape(SPAN_LENGTH, -1).astype(jnp.bfloat16), projection_matrix)
        residual = (summed - wanted.astype(jnp.float32)).astype(jnp.bfloat16)
        residual_tan = summed_tan.astype(jnp.bfloat16)
        dims = (((1,), (1,)), ((), ()))
        grad_norm = lax.dot_general(residual, projection_matrix, dims, preferred_element_type=jnp.float32).reshape(SPAN_LENGTH, HEADS, HEAD_DIM)
        grad_norm_tan = lax.dot_general(residual_tan, projection_matrix, dims, preferred_element_type=jnp.float32).reshape(SPAN_LENGTH, HEADS, HEAD_DIM)

        def norm_back(point, cotan):
            return jax.vjp(group_norm, point)[1](cotan)[0]
        grad_out, grad_out_tan = jax.jvp(norm_back, (outputs, grad_norm), (outputs_tan, grad_norm_tan))

        def out_grads(a, b, c, d, g):
            return jax.vjp(lambda a2, b2, c2, d2: block_out(a2, b2, c2, d2, logs_b), a, b, c, d)[1](g)
        primal_g, tangent_g = jax.jvp(out_grads, (q, k, v, state, grad_out), (qt, kt, vt, state_t, grad_out_tan))
        return (tangent_g[0], tangent_g[1], tangent_g[2], primal_g[3], tangent_g[3])
    hess_qb, hess_k1, hess_v1, grad_state, grad_state_tan = lax.map(middle, (q_rows, k_rows, v_rows, q_tan, k_tan, v_tan, state_in, state_in_tan, fading_rate_exponent, target_blocks))

    def reverse_step(carry, item):
        held, held_tan = carry
        decay_b, grad_b, grad_t = item
        factor = decay_b[:, None, None]
        return ((grad_b + factor * held, grad_t + factor * held_tan), (held, held_tan))
    unused_back, (state_cot, state_cot_tan) = lax.scan(reverse_step, (zero_state, zero_state), (decay_all, grad_state, grad_state_tan), reverse=True)

    def last_part(item):
        k, v, kt, vt, cot, cot_t, logs_b = item

        def state_grads(b, c, g):
            return jax.vjp(lambda b2, c2: block_state(b2, c2, logs_b), b, c)[1](g)
        return jax.jvp(state_grads, (k, v, cot), (kt, vt, cot_t))[1]
    hess_k2, hess_v2 = lax.map(last_part, (k_rows, v_rows, k_tan, v_tan, state_cot, state_cot_tan, fading_rate_exponent))
    shape_out = (SEQUENCE_LENGTH, HEADS * HEAD_DIM)
    hess_q = hess_qb.reshape(shape_out).astype(jnp.bfloat16)
    hess_k = (hess_k1 + hess_k2).reshape(shape_out).astype(jnp.bfloat16)
    hess_v = (hess_v1 + hess_v2).reshape(shape_out).astype(jnp.bfloat16)
    return (hess_q, hess_k, hess_v)
```

```python
import functools
import math

import jax
import jax.numpy as jnp
from jax import lax
from jax.experimental import pallas as pl
from jax.experimental.pallas import tpu as pltpu
from jax.sharding import PartitionSpec as P

LEVELS = 8
KEPT_LOG = math.log(0.7)
EPS = 1e-06
F32 = jnp.float32
BF16 = jnp.bfloat16
MESH = pl.DeviceIdType.MESH
FAR = 1e9


def dot(a, b, dims=((1,), (0,))):
    return lax.dot_general(a, b, (dims, ((), ())), preferred_element_type=F32)


def cols(h, d):
    return pl.ds(pl.multiple_of(h * d, d), d)


def decay_tables(flags_ref, dist, fall, pos, cum):
    t = dist.shape[0]
    row = lax.broadcasted_iota(jnp.int32, (t, t), 0)
    col = lax.broadcasted_iota(jnp.int32, (t, t), 1)
    flags = jnp.broadcast_to(flags_ref[...].astype(F32), (t, t))
    cum_col = jnp.sum(jnp.where(col <= row, flags, 0.0), axis=1, keepdims=True)
    flag_col = jnp.sum(jnp.where(col == row, flags, 0.0), axis=1, keepdims=True)
    cum_row = jnp.sum(jnp.where(row <= col, flag_col, 0.0), axis=0, keepdims=True)
    dist[...] = jnp.where(row >= col, (row - col).astype(F32), FAR)
    fall[...] = KEPT_LOG * (cum_col - cum_row)
    pos[...] = lax.broadcasted_iota(jnp.int32, pos.shape, 0).astype(F32)
    cum[...] = KEPT_LOG * jnp.broadcast_to(cum_col, cum.shape)


def barrier_start(n, me, up, down):
    barrier = pltpu.get_barrier_semaphore()
    for z in (up, down):
        pl.semaphore_signal(barrier, inc=1, device_id={"head": z}, device_id_type=MESH)

    @pl.loop(1, n)
    def _(step):
        pl.semaphore_signal(barrier, inc=1, device_id={"seq": lax.rem(me + step, n)}, device_id_type=MESH)


def barrier_end(n):
    pl.semaphore_wait(pltpu.get_barrier_semaphore(), n + 1)


def exchange_start(n, me, src, dst, send_sem, recv_sem):
    @pl.loop(1, n)
    def _(step):
        j = lax.rem(me + step, n)
        pltpu.make_async_remote_copy(
            src_ref=src.at[j], dst_ref=dst.at[me], send_sem=send_sem.at[j], recv_sem=recv_sem.at[me],
            device_id={"seq": j}, device_id_type=MESH,
        ).start()


def exchange_end(n, me, src, dst, send_sem, recv_sem):
    @pl.loop(1, n)
    def _(step):
        j = lax.rem(me + step, n)
        pltpu.make_async_remote_copy(
            src_ref=src.at[j], dst_ref=dst.at[j], send_sem=send_sem.at[j], recv_sem=recv_sem.at[j],
            device_id={"seq": j}, device_id_type=MESH,
        ).wait()


def scan_slots(n, me, length, heads, lg_ref, count_ref, own, recv, back, result, reverse):
    recv[me] = own[me]
    head = me // (n // heads)
    lg = lg_ref[head, :, 0:128]

    def step(i, run):
        j = n - 1 - i if reverse else i
        back[j] = run.astype(BF16)
        factor = jnp.exp(float(length) * lg + KEPT_LOG * count_ref[j])
        return run * factor + recv[j].astype(F32)

    lax.fori_loop(0, n, step, jnp.zeros(recv.shape[1:], F32))
    result[me] = back[me]


def state_of(result, h, per, half):
    rows = result.shape[1] // 2
    part = result[pl.ds(h * per, per), half * rows:(half + 1) * rows, :]
    return part.reshape(per * rows, part.shape[2])


def put_state(own, h, per, half, value):
    rows = own.shape[1] // 2
    own[pl.ds(h * per, per), half * rows:(half + 1) * rows, :] = value.astype(BF16).reshape(per, rows, value.shape[1])


def weights_of(h, d, lg_ref, dist, fall):
    return jnp.exp(dist[...] * lg_ref[h] + fall[...]) * (d ** -0.5)


def remote(src, dst, send_sem, recv_sem, **where):
    return pltpu.make_async_remote_copy(
        src_ref=src, dst_ref=dst, send_sem=send_sem, recv_sem=recv_sem, device_id=where, device_id_type=MESH
    )


def arrival(dst, recv_sem):
    pltpu.make_async_copy(dst, dst, recv_sem).wait()


class GramGather:
    def __init__(self, me, full, send_sem, recv_sem):
        c = lax.rem(me, 2)
        x, y = lax.rem(me // 2, 4), me // 8
        self.me, self.c, self.f, self.s = me, c, x + c * (y - x), y + c * (x - y)
        self.full, self.send_sem, self.recv_sem = full, send_sem, recv_sem
        self.rows = full.shape[1] // 32
        self.started = []

    def at(self, df, s_off, absolute=False):
        f = df if absolute else lax.rem(self.f + df + 4, 4)
        s = lax.rem(self.s + s_off + 4, 4)
        return (f * (1 + 3 * self.c) + s * (4 - 3 * self.c)) * 2 + self.c

    def view(self, piece, half=None):
        rows = pl.ds(pl.multiple_of(piece * self.rows, self.rows), self.rows)
        if half is None:
            return self.full.at[:, rows, :]
        return self.full.at[2 * half:2 * half + 2, rows, :]

    def send(self, piece, to, half=None):
        copy = remote(
            self.view(piece, half), self.view(piece, half),
            self.send_sem.at[len(self.started)], self.recv_sem.at[piece, half or 0], seq=to,
        )
        copy.start()
        self.started.append(copy)

    def wait(self, piece, half=None):
        arrival(self.view(piece, half), self.recv_sem.at[piece, half or 0])

    def spread(self, piece):
        self.send(piece, self.at(0, 1))
        self.send(piece, self.at(0, -1))
        self.send(piece, self.me + 1 - 2 * self.c)

    def round(self, k):
        if k == 0:
            self.send(self.me, self.at(1, 0))
            self.send(self.me, self.at(-1, 0))
            self.spread(self.me)
        elif k == 1:
            for step, half in ((-1, 0), (1, 1)):
                piece = self.at(step, 0)
                self.wait(piece)
                self.send(piece, self.at(-step, 0), half)
                self.spread(piece)
        elif k == 2:
            piece = self.at(2, 0)
            self.wait(piece, 0)
            self.wait(piece, 1)
            self.spread(piece)
        elif k == 3:
            for df in (0, -1, 1, 2):
                for step, half in ((-1, 0), (1, 1)):
                    piece = self.at(df, step)
                    self.wait(piece)
                    self.send(piece, self.at(0, -step), half)
                    self.send(piece, self.me + 1 - 2 * self.c)
        elif k == 4:
            for df in (0, -1, 1, 2):
                piece = self.at(df, 2)
                self.wait(piece, 0)
                self.wait(piece, 1)
                self.send(piece, self.me + 1 - 2 * self.c)
        else:

            @pl.loop(0, 16)
            def _(i):
                self.wait(2 * i + 1 - self.c)

    def finish(self):
        for copy in self.started:
            copy.wait_send()


def kernel(
    n, heads, groups, *refs,
):
    inputs, (lg, flags, w_hbm, goal_hbm), (hq, hk, hv) = refs[:6], refs[6:10], refs[10:13]
    (q, k, v, qt, kt, vt, weight, goal, dist, fall, pos, cum, mine, count, own, recv, back, state, own_b, recv_b, back_b,
     state_b, picked, gram, zall, gz, o_buf, ot_buf, g_buf, gt_buf, hk_buf, hv_buf,
     load_sem, s1, r1, s2, r2, s3, r3, s4, r4, s5, r5, ws, wr, gs, gr, zs, zr) = refs[13:]
    me, z = lax.axis_index("seq"), lax.axis_index("head")
    up, down = lax.rem(z + 1, groups), lax.rem(z + groups - 1, groups)
    far = lax.rem(z + 2, groups)
    length, width = q.shape
    d = width // heads
    per = n // heads
    scale = d ** -0.5
    loads = [
        pltpu.make_async_copy(src, dst, load_sem.at[i])
        for i, (src, dst) in enumerate(
            zip((*inputs, w_hbm, goal_hbm), (q, k, v, qt, kt, vt, weight, goal))
        )
    ]
    for i in (1, 2, 4, 5, 6, 0, 3, 7):
        loads[i].start()
    barrier_start(n, me, up, down)
    decay_tables(flags, dist, fall, pos, cum)
    total = jnp.broadcast_to(jnp.sum(flags[...].astype(F32), axis=1, keepdims=True), (1, 128))
    mine[0] = total
    count[me] = total
    for i in (1, 2, 4, 5):
        loads[i].wait()

    @pl.loop(0, heads)
    def _(h):
        c = cols(h, d)
        w = scale * jnp.exp((length - 1.0 - pos[...]) * lg[h, :, 0:d] + (KEPT_LOG * total - cum[...]))
        kw = (k[:, c].astype(F32) * w).astype(BF16)
        ktw = (kt[:, c].astype(F32) * w).astype(BF16)
        both = dot(kw, jnp.concatenate([v[:, c], vt[:, c]], axis=1), ((0,), (0,)))
        put_state(own, h, per, 0, both[:, :d])
        put_state(own, h, per, 1, both[:, d:] + dot(ktw, v[:, c], ((0,), (0,))))

    loads[6].wait()
    barrier_end(n)
    rows = width // n
    half = rows // 2
    mine_rows = pl.ds(pl.multiple_of(me * rows, rows), rows)
    w_copies = [
        remote(weight.at[mine_rows], picked.at[z], ws.at[0], wr.at[0], head=up),
        remote(weight.at[mine_rows], picked.at[z], ws.at[1], wr.at[1], head=down),
    ]
    for copy in w_copies:
        copy.start()

    @pl.loop(1, n)
    def _(step):
        j = lax.rem(me + step, n)
        remote(mine.at[0], count.at[me], s3.at[j], r3.at[me], seq=j).start()

    exchange_start(n, me, own, recv, s1, r1)
    loads[0].wait()
    loads[3].wait()

    def inner(h):
        c = cols(h, d)
        w = weights_of(h, d, lg, dist, fall)
        a = dot(q[:, c], k[:, c], ((1,), (1,)))
        at = dot(
            jnp.concatenate([qt[:, c], q[:, c]], axis=1), jnp.concatenate([k[:, c], kt[:, c]], axis=1), ((1,), (1,))
        )
        p = (a * w).astype(BF16)
        pt = (at * w).astype(BF16)
        both = dot(p, jnp.concatenate([v[:, c], vt[:, c]], axis=1))
        o_buf[:, c] = both[:, :d]
        ot_buf[:, c] = both[:, d:] + dot(pt, v[:, c])

    pl.loop(0, heads // 2)(inner)
    picked[z] = weight[mine_rows]
    arrival(picked.at[down], wr.at[0])
    w_copies.append(remote(picked.at[down, 0:half], picked.at[down, 0:half], ws.at[2], wr.at[2], head=up))
    w_copies[2].start()
    arrival(picked.at[up], wr.at[1])
    w_copies.append(remote(picked.at[up, half:rows], picked.at[up, half:rows], ws.at[3], wr.at[3], head=down))
    w_copies[3].start()

    @pl.loop(1, n)
    def _(step):
        j = lax.rem(me + step, n)
        remote(mine.at[0], count.at[j], s3.at[j], r3.at[j], seq=j).wait()

    exchange_end(n, me, own, recv, s1, r1)
    scan_slots(n, me, length, heads, lg, count, own, recv, back, state, False)
    exchange_start(n, me, back, state, s2, r2)
    arrival(picked.at[far, 0:half], wr.at[2])
    arrival(picked.at[far, half:rows], wr.at[3])
    tile = 256

    @pl.loop(0, width // tile)
    def _(i):
        c = cols(i, tile)
        part = dot(picked[...].reshape(groups * rows, weight.shape[1]), weight[c, :], ((1,), (1,)))
        gram[:, mine_rows, c] = part.astype(BF16).reshape(groups, rows, tile)

    pl.loop(heads // 2, heads)(inner)
    gather = GramGather(me, gram, gs, gr)
    gather.round(0)
    exchange_end(n, me, back, state, s2, r2)

    def z_send(h):
        c = cols(h, d)
        remote(zall.at[z, :, c], zall.at[z, :, c], zs.at[h, 0], zr.at[h, 0], head=up).start()
        remote(zall.at[z, :, c], zall.at[z, :, c], zs.at[h, 1], zr.at[h, 1], head=down).start()

    @pl.loop(0, heads)
    def _(h):
        c = cols(h, d)
        dq = jnp.exp((pos[...] + 1.0) * lg[h, :, 0:d] + cum[...])
        s = state_of(state, h, per, 0)
        st = state_of(state, h, per, 1)
        both = dot(q[:, c], jnp.concatenate([s, st], axis=1))
        o = o_buf[:, c] + dq * both[:, :d]
        ot = ot_buf[:, c] + dq * (both[:, d:] + dot(qt[:, c], s))
        o_buf[:, c] = o
        ot_buf[:, c] = ot
        r = lax.rsqrt(jnp.mean(o * o, axis=1, keepdims=True) + EPS)
        m = jnp.mean(o * ot, axis=1, keepdims=True)
        zall[z, 0:length, c] = (o * r).astype(BF16)
        zall[z, length:, c] = (r * ot - o * (r * r * r * m)).astype(BF16)

        @pl.when(h > 0)
        def _():
            z_send(h - 1)

    loads[7].wait()
    z_send(heads - 1)

    def relay(h):
        c = slice(h * d, (h + 1) * d)
        arrival(zall.at[down, :, c], zr.at[h, 0])
        remote(zall.at[down, 0:length, c], zall.at[down, 0:length, c], zs.at[h, 2], zr.at[h, 2], head=up).start()
        arrival(zall.at[up, :, c], zr.at[h, 1])
        remote(zall.at[up, length:, c], zall.at[up, length:, c], zs.at[h, 3], zr.at[h, 3], head=down).start()

    def distant(h):
        c = slice(h * d, (h + 1) * d)
        arrival(zall.at[far, 0:length, c], zr.at[h, 2])
        arrival(zall.at[far, length:, c], zr.at[h, 3])

    def add(p, *sources):
        part = slice(2 * p * d, 2 * (p + 1) * d)

        @pl.loop(0, width // tile)
        def _(i):
            c = cols(i, tile)
            value = gz[:, c]
            for g in sources:
                value = value + dot(zall[g, :, part], gram[g, part, c])
            gz[:, c] = value

    gather.round(1)
    relay(0)
    gather.round(2)
    relay(1)
    gather.round(3)
    relay(2)
    gather.round(4)
    relay(3)
    gz[length:, :] = jnp.zeros((length, width), F32)

    @pl.loop(0, width // tile)
    def _(i):
        c = cols(i, tile)
        gz[0:length, c] = -dot(goal[...], weight[c, :], ((1,), (1,)))

    gather.round(5)
    relay(4)
    for p in range(heads // 2):
        add(p, z)
    relay(5)
    add(0, up, down)
    add(1, up, down)
    for h in range(4):
        distant(h)
    relay(6)
    add(0, far)
    add(1, far)
    add(2, up, down)
    relay(7)
    distant(4)
    distant(5)
    add(2, far)
    add(3, up, down)
    distant(6)
    distant(7)
    add(3, far)

    @pl.loop(0, heads)
    def _(h):
        c = cols(h, d)
        dq = jnp.exp((pos[...] + 1.0) * lg[h, :, 0:d] + cum[...])
        o, ot = o_buf[:, c], ot_buf[:, c]
        gzh, gzt = gz[0:length, c], gz[length:, c]
        r = lax.rsqrt(jnp.mean(o * o, axis=1, keepdims=True) + EPS)
        m = jnp.mean(o * ot, axis=1, keepdims=True)
        m1 = jnp.mean(o * gzh, axis=1, keepdims=True)
        m1t = jnp.mean(ot * gzh + o * gzt, axis=1, keepdims=True)
        r3 = r * r * r
        g = r * gzh - (r3 * m1) * o
        gt = r * gzt - (r3 * m) * gzh - (r3 * m1) * ot + (3.0 * r3 * r * r * m * m1 - r3 * m1t) * o
        g_buf[:, c] = g.astype(BF16)
        gt_buf[:, c] = gt.astype(BF16)
        gd = (dq * g).astype(BF16)
        gtd = (dq * gt).astype(BF16)
        both = dot(q[:, c], jnp.concatenate([gd, gtd], axis=1), ((0,), (0,)))
        put_state(own_b, h, per, 0, both[:, :d])
        put_state(own_b, h, per, 1, both[:, d:] + dot(qt[:, c], gd, ((0,), (0,))))

    exchange_start(n, me, own_b, recv_b, s4, r4)

    def inner_back(h):
        c = cols(h, d)
        w = weights_of(h, d, lg, dist, fall)
        dq = jnp.exp((pos[...] + 1.0) * lg[h, :, 0:d] + cum[...])
        qh, kh, vh, qth, kth, vth, g, gt = (x[:, c] for x in (q, k, v, qt, kt, vt, g_buf, gt_buf))
        a = dot(qh, kh, ((1,), (1,)))
        at = dot(jnp.concatenate([qth, qh], axis=1), jnp.concatenate([kh, kth], axis=1), ((1,), (1,)))
        p = (a * w).astype(BF16)
        pt = (at * w).astype(BF16)
        b = (dot(g, vh, ((1,), (1,))) * w).astype(BF16)
        bt = dot(jnp.concatenate([gt, g], axis=1), jnp.concatenate([vh, vth], axis=1), ((1,), (1,)))
        bt = (bt * w).astype(BF16)
        s = state_of(state, h, per, 0)
        st = state_of(state, h, per, 1)
        outer = dot(jnp.concatenate([gt, g], axis=1), jnp.concatenate([s, st], axis=1), ((1,), (1,)))
        hq[:, c] = (
            dot(jnp.concatenate([bt, b], axis=1), jnp.concatenate([kh, kth], axis=0)) + dq * outer
        ).astype(BF16)
        hk_buf[:, c] = dot(jnp.concatenate([bt, b], axis=0), jnp.concatenate([qh, qth], axis=0), ((0,), (0,)))
        hv_buf[:, c] = dot(jnp.concatenate([pt, p], axis=0), jnp.concatenate([g, gt], axis=0), ((0,), (0,)))

    pl.loop(0, heads // 2)(inner_back)
    exchange_end(n, me, own_b, recv_b, s4, r4)
    scan_slots(n, me, length, heads, lg, count, own_b, recv_b, back_b, state_b, True)
    exchange_start(n, me, back_b, state_b, s5, r5)
    pl.loop(heads // 2, heads)(inner_back)
    exchange_end(n, me, back_b, state_b, s5, r5)

    @pl.loop(0, heads)
    def _(h):
        c = cols(h, d)
        w = scale * jnp.exp((length - 1.0 - pos[...]) * lg[h, :, 0:d] + (KEPT_LOG * total - cum[...]))
        s = state_of(state_b, h, per, 0)
        st = state_of(state_b, h, per, 1)
        ks = dot(jnp.concatenate([v[:, c], vt[:, c]], axis=1), jnp.concatenate([st, s], axis=1), ((1,), (1,)))
        vs = dot(jnp.concatenate([k[:, c], kt[:, c]], axis=1), jnp.concatenate([st, s], axis=0))
        hk[:, c] = (hk_buf[:, c] + w * ks).astype(BF16)
        hv[:, c] = (hv_buf[:, c] + w * vs).astype(BF16)

    for copy in w_copies:
        copy.wait_send()
    gather.finish()

    @pl.loop(0, heads)
    def _(h):
        c = cols(h, d)
        whole, top = zall.at[z, :, c], zall.at[z, 0:length, c]
        for i, piece in enumerate((whole, whole, top, top)):
            remote(piece, piece, zs.at[h, i], zr.at[h, i], head=up).wait_send()


def on_device(n, groups, probe, source, content, probe_t, source_t, content_t, table, flags, weight, goal):
    length, width = probe.shape
    heads = table.shape[0]
    d = width // heads
    fraction = table.astype(F32) / (LEVELS - 1)
    rates = jnp.exp(math.log(1.0 / 32.0) + fraction * math.log(16.0 / (length * n)))
    lg = jnp.broadcast_to(jnp.log1p(-rates)[:, None, None], (heads, 1, length))
    flags = flags.reshape(1, length)
    vmem = pl.BlockSpec(memory_space=pltpu.VMEM)
    hbm = pl.BlockSpec(memory_space=pl.ANY)
    slots = pltpu.VMEM((n, 2 * heads * d // n, d), BF16)
    narrow, wide = pltpu.VMEM((length, width), BF16), pltpu.VMEM((length, width), F32)
    rows = width // n
    dma = pltpu.SemaphoreType.DMA
    out = jax.ShapeDtypeStruct((length, width), BF16)
    return pl.pallas_call(
        functools.partial(kernel, n, heads, groups),
        out_shape=(out, out, out),
        in_specs=[hbm] * 6 + [vmem] * 2 + [hbm] * 2,
        out_specs=[vmem] * 3,
        scratch_shapes=[
            *[narrow] * 6, pltpu.VMEM(weight.shape, BF16), pltpu.VMEM(goal.shape, BF16),
            pltpu.VMEM((length, length), F32), pltpu.VMEM((length, length), F32),
            pltpu.VMEM((length, d), F32), pltpu.VMEM((length, d), F32),
            pltpu.VMEM((1, 1, 128), F32), pltpu.VMEM((n, 1, 128), F32),
            *[slots] * 8,
            pltpu.VMEM((groups, rows, weight.shape[1]), BF16),
            pltpu.VMEM((groups, width, width), BF16),
            pltpu.VMEM((groups, 2 * length, width), BF16),
            pltpu.VMEM((2 * length, width), F32),
            wide, wide, narrow, narrow, wide, wide,
            dma((8,)), *[dma((n,))] * 10, dma((4,)), dma((4,)), dma((36,)), dma((n, 2)), dma((heads, 4)), dma((heads, 4)),
        ],
        compiler_params=pltpu.CompilerParams(collective_id=0, has_side_effects=True, vmem_limit_bytes=62 << 20),
        name="retention_hvp",
    )(probe, source, content, probe_t, source_t, content_t, lg, flags, weight, goal)


def solution(mesh):
    n, groups = mesh.shape["seq"], mesh.shape["head"]
    both = P("seq", "head")
    return jax.shard_map(
        functools.partial(on_device, n, groups),
        mesh=mesh,
        in_specs=(both,) * 6 + (P("head"), P("seq"), P("head", None), P("seq", None)),
        out_specs=(both,) * 3,
        check_vma=False,
    )
```

```python
import functools
import math

import jax
import jax.numpy as jnp
from jax import lax
from jax.experimental import pallas as pl
from jax.experimental.pallas import tpu as pltpu
from jax.sharding import PartitionSpec as P

LEVELS = 8
KEPT_LOG = math.log(0.7)
EPS = 1e-06
F32 = jnp.float32
BF16 = jnp.bfloat16
MESH = pl.DeviceIdType.MESH
FAR = 1e9


def dot(a, b, dims=((1,), (0,))):
    return lax.dot_general(a, b, (dims, ((), ())), preferred_element_type=F32)


def cols(h, d):
    return pl.ds(pl.multiple_of(h * d, d), d)


def decay_tables(flags_ref, dist, fall, pos, cum):
    t = dist.shape[0]
    row = lax.broadcasted_iota(jnp.int32, (t, t), 0)
    col = lax.broadcasted_iota(jnp.int32, (t, t), 1)
    flags = jnp.broadcast_to(flags_ref[...].astype(F32), (t, t))
    cum_col = jnp.sum(jnp.where(col <= row, flags, 0.0), axis=1, keepdims=True)
    flag_col = jnp.sum(jnp.where(col == row, flags, 0.0), axis=1, keepdims=True)
    cum_row = jnp.sum(jnp.where(row <= col, flag_col, 0.0), axis=0, keepdims=True)
    dist[...] = jnp.where(row >= col, (row - col).astype(F32), FAR)
    fall[...] = KEPT_LOG * (cum_col - cum_row)
    pos[...] = lax.broadcasted_iota(jnp.int32, pos.shape, 0).astype(F32)
    cum[...] = KEPT_LOG * jnp.broadcast_to(cum_col, cum.shape)


def barrier_start(n, me, up, down):
    barrier = pltpu.get_barrier_semaphore()
    for z in (up, down):
        pl.semaphore_signal(barrier, inc=1, device_id={"head": z}, device_id_type=MESH)

    @pl.loop(1, n)
    def _(step):
        pl.semaphore_signal(barrier, inc=1, device_id={"seq": lax.rem(me + step, n)}, device_id_type=MESH)


def barrier_end(n):
    pl.semaphore_wait(pltpu.get_barrier_semaphore(), n + 1)


def weights_of(h, d, lg_ref, dist, fall):
    return jnp.exp(dist[...] * lg_ref[h] + fall[...]) * (d ** -0.5)


def remote(src, dst, send_sem, recv_sem, **where):
    return pltpu.make_async_remote_copy(
        src_ref=src, dst_ref=dst, send_sem=send_sem, recv_sem=recv_sem, device_id=where, device_id_type=MESH
    )


def arrival(dst, recv_sem):
    pltpu.make_async_copy(dst, dst, recv_sem).wait()


class GramGather:
    def __init__(self, me, full, send_sem, recv_sem):
        c = lax.rem(me, 2)
        x, y = lax.rem(me // 2, 4), me // 8
        self.me, self.c, self.f, self.s = me, c, x + c * (y - x), y + c * (x - y)
        self.full, self.send_sem, self.recv_sem = full, send_sem, recv_sem
        self.rows = full.shape[1] // 32
        self.started = []

    def at(self, df, s_off, absolute=False):
        f = df if absolute else lax.rem(self.f + df + 4, 4)
        s = lax.rem(self.s + s_off + 4, 4)
        return (f * (1 + 3 * self.c) + s * (4 - 3 * self.c)) * 2 + self.c

    def view(self, piece, half=None):
        rows = pl.ds(pl.multiple_of(piece * self.rows, self.rows), self.rows)
        if half is None:
            return self.full.at[:, rows, :]
        return self.full.at[2 * half:2 * half + 2, rows, :]

    def send(self, piece, to, half=None):
        copy = remote(
            self.view(piece, half), self.view(piece, half),
            self.send_sem.at[len(self.started)], self.recv_sem.at[piece, half or 0], seq=to,
        )
        copy.start()
        self.started.append(copy)

    def wait(self, piece, half=None):
        arrival(self.view(piece, half), self.recv_sem.at[piece, half or 0])

    def spread(self, piece):
        self.send(piece, self.at(0, 1))
        self.send(piece, self.at(0, -1))
        self.send(piece, self.me + 1 - 2 * self.c)

    def round(self, k):
        if k == 0:
            self.send(self.me, self.at(1, 0))
            self.send(self.me, self.at(-1, 0))
            self.spread(self.me)
        elif k == 1:
            for step, half in ((-1, 0), (1, 1)):
                piece = self.at(step, 0)
                self.wait(piece)
                self.send(piece, self.at(-step, 0), half)
                self.spread(piece)
        elif k == 2:
            piece = self.at(2, 0)
            self.wait(piece, 0)
            self.wait(piece, 1)
            self.spread(piece)
        elif k == 3:
            for df in (0, -1, 1, 2):
                for step, half in ((-1, 0), (1, 1)):
                    piece = self.at(df, step)
                    self.wait(piece)
                    self.send(piece, self.at(0, -step), half)
                    self.send(piece, self.me + 1 - 2 * self.c)
        elif k == 4:
            for df in (0, -1, 1, 2):
                piece = self.at(df, 2)
                self.wait(piece, 0)
                self.wait(piece, 1)
                self.send(piece, self.me + 1 - 2 * self.c)
        else:

            @pl.loop(0, 16)
            def _(i):
                self.wait(2 * i + 1 - self.c)

    def finish(self):
        for copy in self.started:
            copy.wait_send()


class Scan:
    def __init__(self, me, n, heads, length, lg, count, buffers, sems, reverse):
        self.own, self.gift, self.peer, self.tot, self.recv, self.back, self.entry, self.state, self.gift2 = buffers
        self.pair_sem, self.s1, self.r1, self.s2, self.r2 = sems
        self.c, self.chip, self.chips = lax.rem(me, 2), me // 2, n // 2
        self.sibling = me + 1 - 2 * self.c
        self.half = heads // 2
        self.length, self.lg, self.count, self.reverse = length, lg, count, reverse
        self.per = self.chips // self.half
        self.rows = self.tot.shape[1] // 2
        self.d = self.tot.shape[2]

    def mine(self, i):
        return self.half * self.c + i

    def theirs(self, i):
        return self.half * (1 - self.c) + i

    def give(self):
        self.gift_copy = remote(self.gift, self.peer, self.pair_sem.at[0], self.pair_sem.at[1], seq=self.sibling)
        self.gift_copy.start()

    def decay(self, h, core):
        return jnp.exp(float(self.length) * self.lg[h, :, 0:self.d] + KEPT_LOG * self.count[2 * self.chip + core])

    def ordered(self, i, part):
        mine, peer = self.own[i, part].astype(F32), self.peer[i, part].astype(F32)
        return jnp.where(self.c == 0, mine, peer), jnp.where(self.c == 0, peer, mine)

    def combine(self):
        @pl.loop(0, self.half)
        def _(i):
            factor = self.decay(self.mine(i), 0 if self.reverse else 1)
            for part in range(2):
                first, second = self.ordered(i, part)
                total = first + factor * second if self.reverse else first * factor + second
                self.tot[pl.ds(i * self.per, self.per), part * self.rows:(part + 1) * self.rows, :] = (
                    total.astype(BF16).reshape(self.per, self.rows, self.d)
                )

    def spread(self, src, dst, send_sem, recv_sem):
        @pl.loop(1, self.chips)
        def _(step):
            p = lax.rem(self.chip + step, self.chips)
            remote(src.at[p], dst.at[self.chip], send_sem.at[p], recv_sem.at[self.chip], seq=2 * p + self.c).start()

    def collect(self, src, dst, send_sem, recv_sem):
        @pl.loop(1, self.chips)
        def _(step):
            p = lax.rem(self.chip + step, self.chips)
            remote(src.at[p], dst.at[p], send_sem.at[p], recv_sem.at[p], seq=2 * p + self.c).wait()

    def out(self):
        self.spread(self.tot, self.recv, self.s1, self.r1)

    def out_wait(self):
        self.collect(self.tot, self.recv, self.s1, self.r1)

    def scan(self):
        self.recv[self.chip] = self.tot[self.chip]
        lg = self.lg[self.mine(self.chip // self.per), :, 0:self.d]

        def step(i, run):
            p = self.chips - 1 - i if self.reverse else i
            self.back[p] = run.astype(BF16)
            factor = jnp.exp(2.0 * self.length * lg + KEPT_LOG * (self.count[2 * p] + self.count[2 * p + 1]))
            return run * factor + self.recv[p].astype(F32)

        lax.fori_loop(0, self.chips, step, jnp.zeros(self.recv.shape[1:], F32))
        self.entry[self.chip] = self.back[self.chip]

    def home(self):
        self.spread(self.back, self.entry, self.s2, self.r2)

    def home_wait(self):
        self.collect(self.back, self.entry, self.s2, self.r2)

    def settle(self):
        @pl.loop(0, self.half)
        def _(i):
            factor = self.decay(self.mine(i), 1 if self.reverse else 0)
            for part in range(2):
                first, second = self.ordered(i, part)
                edge = self.entry[pl.ds(i * self.per, self.per), part * self.rows:(part + 1) * self.rows, :]
                edge = edge.reshape(self.d, self.d).astype(F32)
                inside = factor * edge + (second if self.reverse else first)
                keep = (self.c == 1) if self.reverse else (self.c == 0)
                self.gift2[i, part] = jnp.where(keep, inside, edge).astype(BF16)
                self.state[self.mine(i), part] = jnp.where(keep, edge, inside).astype(BF16)

        spot = self.state.at[pl.ds(self.mine(0), self.half)]
        self.gift2_copy = remote(self.gift2, spot, self.pair_sem.at[2], self.pair_sem.at[3], seq=self.sibling)
        self.gift2_copy.start()

    def settle_wait(self):
        arrival(self.state.at[pl.ds(self.theirs(0), self.half)], self.pair_sem.at[3])

    def finish(self):
        self.gift_copy.wait_send()
        self.gift2_copy.wait_send()


def kernel(n, heads, groups, *refs):
    inputs, (table, flags, w_hbm, goal_hbm), (hq, hk, hv) = refs[:6], refs[6:10], refs[10:13]
    (q, k, v, qt, kt, vt, weight, goal, dist, fall, pos, cum, lg, mine, count) = refs[13:28]
    ahead, behind = refs[28:37], refs[37:46]
    (picked, gram, zall, gz, o_buf, ot_buf, g_buf, gt_buf, hk_buf, hv_buf) = refs[46:56]
    ahead_sems, behind_sems = refs[56:61], refs[61:66]
    (load_sem, cs, cr, ws, wr, gs, gr, zs, zr) = refs[66:]
    me, z = lax.axis_index("seq"), lax.axis_index("head")
    up, down = lax.rem(z + 1, groups), lax.rem(z + groups - 1, groups)
    far = lax.rem(z + 2, groups)
    length, width = q.shape
    d = width // heads
    scale = d ** -0.5
    rows = width // n
    mine_rows = pl.ds(pl.multiple_of(me * rows, rows), rows)
    sources = (*inputs, w_hbm.at[mine_rows], w_hbm, goal_hbm)
    loads = [
        pltpu.make_async_copy(src, dst, load_sem.at[i])
        for i, (src, dst) in enumerate(zip(sources, (q, k, v, qt, kt, vt, picked.at[z], weight, goal)))
    ]
    for i in (6, 1, 2, 4, 5, 0, 3, 7, 8):
        loads[i].start()
    barrier_start(n, me, up, down)

    @pl.loop(0, heads)
    def _(h):
        fraction = jnp.full((1, length), table[h], jnp.int32).astype(F32) / (LEVELS - 1)
        rates = jnp.exp(math.log(1.0 / 32.0) + fraction * math.log(16.0 / (length * n)))
        lg[h] = jnp.log1p(-rates)

    decay_tables(flags, dist, fall, pos, cum)
    total = jnp.broadcast_to(jnp.sum(flags[...].astype(F32), axis=1, keepdims=True), (1, 128))
    mine[0] = total
    count[me] = total
    forward = Scan(me, n, heads, length, lg, count, ahead, ahead_sems, False)
    backward = Scan(me, n, heads, length, lg, count, behind, behind_sems, True)
    for i in (1, 2, 4, 5):
        loads[i].wait()

    def own_state(h, target, i):
        c = cols(h, d)
        w = scale * jnp.exp((length - 1.0 - pos[...]) * lg[h, :, 0:d] + (KEPT_LOG * total - cum[...]))
        kw = (k[:, c].astype(F32) * w).astype(BF16)
        ktw = (kt[:, c].astype(F32) * w).astype(BF16)
        both = dot(kw, jnp.concatenate([v[:, c], vt[:, c]], axis=1), ((0,), (0,)))
        target[i, 0] = both[:, :d].astype(BF16)
        target[i, 1] = (both[:, d:] + dot(ktw, v[:, c], ((0,), (0,)))).astype(BF16)

    pl.loop(0, heads // 2)(lambda i: own_state(forward.theirs(i), forward.gift, i))
    loads[6].wait()
    barrier_end(n)
    half = rows // 2
    w_copies = [
        remote(picked.at[z], picked.at[z], ws.at[0], wr.at[0], head=up),
        remote(picked.at[z], picked.at[z], ws.at[1], wr.at[1], head=down),
    ]
    for copy in w_copies:
        copy.start()
    remote(mine.at[0], count.at[me], cs.at[forward.sibling], cr.at[me], seq=forward.sibling).start()
    forward.give()

    @pl.loop(1, n)
    def _(step):
        j = lax.rem(me + step, n)

        @pl.when(j != forward.sibling)
        def _():
            remote(mine.at[0], count.at[me], cs.at[j], cr.at[me], seq=j).start()

    pl.loop(0, heads // 2)(lambda i: own_state(forward.mine(i), forward.own, i))
    arrival(count.at[forward.sibling], cr.at[forward.sibling])
    arrival(forward.peer, forward.pair_sem.at[1])
    forward.combine()
    forward.out()
    loads[0].wait()
    loads[3].wait()

    def inner(h):
        c = cols(h, d)
        w = weights_of(h, d, lg, dist, fall)
        a = dot(q[:, c], k[:, c], ((1,), (1,)))
        at = dot(
            jnp.concatenate([qt[:, c], q[:, c]], axis=1), jnp.concatenate([k[:, c], kt[:, c]], axis=1), ((1,), (1,))
        )
        p = (a * w).astype(BF16)
        pt = (at * w).astype(BF16)
        both = dot(p, jnp.concatenate([v[:, c], vt[:, c]], axis=1))
        o_buf[:, c] = both[:, :d]
        ot_buf[:, c] = both[:, d:] + dot(pt, v[:, c])

    pl.loop(0, heads // 2)(inner)
    @pl.loop(1, n)
    def _(step):
        j = lax.rem(me + step, n)

        @pl.when(j != forward.sibling)
        def _():
            arrival(count.at[j], cr.at[j])

    forward.out_wait()
    forward.scan()
    forward.home()
    arrival(picked.at[down], wr.at[0])
    w_copies.append(remote(picked.at[down, 0:half], picked.at[down, 0:half], ws.at[2], wr.at[2], head=up))
    w_copies[2].start()
    arrival(picked.at[up], wr.at[1])
    w_copies.append(remote(picked.at[up, half:rows], picked.at[up, half:rows], ws.at[3], wr.at[3], head=down))
    w_copies[3].start()
    pl.loop(heads // 2, heads)(inner)
    forward.home_wait()
    forward.settle()

    def z_send(i):
        c = cols(lax.rem(forward.mine(i), heads), d)
        remote(zall.at[z, :, c], zall.at[z, :, c], zs.at[i, 0], zr.at[i, 0], head=up).start()
        remote(zall.at[z, :, c], zall.at[z, :, c], zs.at[i, 1], zr.at[i, 1], head=down).start()

    def output(i):
        h = lax.rem(forward.mine(i), heads)
        c = cols(h, d)
        dq = jnp.exp((pos[...] + 1.0) * lg[h, :, 0:d] + cum[...])
        s, st = forward.state[h, 0], forward.state[h, 1]
        both = dot(q[:, c], jnp.concatenate([s, st], axis=1))
        o = o_buf[:, c] + dq * both[:, :d]
        ot = ot_buf[:, c] + dq * (both[:, d:] + dot(qt[:, c], s))
        o_buf[:, c] = o
        ot_buf[:, c] = ot
        r = lax.rsqrt(jnp.mean(o * o, axis=1, keepdims=True) + EPS)
        m = jnp.mean(o * ot, axis=1, keepdims=True)
        zall[z, 0:length, c] = (o * r).astype(BF16)
        zall[z, length:, c] = (r * ot - o * (r * r * r * m)).astype(BF16)

        @pl.when(i > 0)
        def _():
            z_send(i - 1)

    pl.loop(0, heads // 2)(output)
    forward.settle_wait()
    pl.loop(heads // 2, heads)(output)
    z_send(heads - 1)
    arrival(picked.at[far, 0:half], wr.at[2])
    arrival(picked.at[far, half:rows], wr.at[3])
    loads[7].wait()
    tile = 256

    @pl.loop(0, width // tile)
    def _(i):
        c = cols(i, tile)
        part = dot(picked[...].reshape(groups * rows, weight.shape[1]), weight[c, :], ((1,), (1,)))
        gram[:, mine_rows, c] = part.astype(BF16).reshape(groups, rows, tile)

    loads[8].wait()

    def goal_tile(i):
        c = slice(i * tile, (i + 1) * tile)
        gz[0:length, c] = -dot(goal[...], weight[c, :], ((1,), (1,)))

    def chunk(i):
        return cols(lax.rem(forward.mine(i), heads), d)

    def relay(i):
        c = chunk(i)
        arrival(zall.at[down, :, c], zr.at[i, 0])
        remote(zall.at[down, 0:length, c], zall.at[down, 0:length, c], zs.at[i, 2], zr.at[i, 2], head=up).start()
        arrival(zall.at[up, :, c], zr.at[i, 1])
        remote(zall.at[up, length:, c], zall.at[up, length:, c], zs.at[i, 3], zr.at[i, 3], head=down).start()

    def distant(i):
        c = chunk(i)
        arrival(zall.at[far, 0:length, c], zr.at[i, 2])
        arrival(zall.at[far, length:, c], zr.at[i, 3])

    def add(first, number, *sources):
        part = pl.ds(pl.multiple_of(lax.rem(forward.mine(first), heads) * d, 2 * d), number * d)

        @pl.loop(0, width // tile)
        def _(i):
            c = cols(i, tile)
            value = gz[:, c]
            for g in sources:
                value = value + dot(zall[g, :, part], gram[g, part, c])
            gz[:, c] = value

    gather = GramGather(me, gram, gs, gr)
    gather.round(0)
    goal_tile(0)
    goal_tile(1)
    gather.round(1)
    relay(0)
    goal_tile(2)
    gather.round(2)
    relay(1)
    goal_tile(3)
    gather.round(3)
    relay(2)
    gather.round(4)
    relay(3)
    gather.round(5)
    relay(4)

    @pl.loop(0, width // tile)
    def _(i):
        c = cols(i, tile)
        gz[0:length, c] = gz[0:length, c] + dot(zall[z, 0:length, :], gram[z, :, c])
        gz[length:, c] = dot(zall[z, length:, :], gram[z, :, c])

    relay(5)
    add(0, 4, up, down)
    relay(6)
    for i in range(4):
        distant(i)
    add(0, 4, far)
    add(4, 2, up, down)
    relay(7)
    distant(4)
    distant(5)
    add(4, 2, far)
    add(6, 2, up, down)
    distant(6)
    distant(7)
    add(6, 2, far)

    def norm_back(h, target, i):
        c = cols(h, d)
        dq = jnp.exp((pos[...] + 1.0) * lg[h, :, 0:d] + cum[...])
        o, ot = o_buf[:, c], ot_buf[:, c]
        gzh, gzt = gz[0:length, c], gz[length:, c]
        r = lax.rsqrt(jnp.mean(o * o, axis=1, keepdims=True) + EPS)
        m = jnp.mean(o * ot, axis=1, keepdims=True)
        m1 = jnp.mean(o * gzh, axis=1, keepdims=True)
        m1t = jnp.mean(ot * gzh + o * gzt, axis=1, keepdims=True)
        r3 = r * r * r
        g = r * gzh - (r3 * m1) * o
        gt = r * gzt - (r3 * m) * gzh - (r3 * m1) * ot + (3.0 * r3 * r * r * m * m1 - r3 * m1t) * o
        g_buf[:, c] = g.astype(BF16)
        gt_buf[:, c] = gt.astype(BF16)
        gd = (dq * g).astype(BF16)
        gtd = (dq * gt).astype(BF16)
        both = dot(q[:, c], jnp.concatenate([gd, gtd], axis=1), ((0,), (0,)))
        target[i, 0] = both[:, :d].astype(BF16)
        target[i, 1] = (both[:, d:] + dot(qt[:, c], gd, ((0,), (0,)))).astype(BF16)

    pl.loop(0, heads // 2)(lambda i: norm_back(backward.theirs(i), backward.gift, i))
    backward.give()
    pl.loop(0, heads // 2)(lambda i: norm_back(backward.mine(i), backward.own, i))
    arrival(backward.peer, backward.pair_sem.at[1])
    backward.combine()
    backward.out()

    def inner_back(h):
        c = cols(h, d)
        w = weights_of(h, d, lg, dist, fall)
        dq = jnp.exp((pos[...] + 1.0) * lg[h, :, 0:d] + cum[...])
        qh, kh, vh, qth, kth, vth, g, gt = (x[:, c] for x in (q, k, v, qt, kt, vt, g_buf, gt_buf))
        a = dot(qh, kh, ((1,), (1,)))
        at = dot(jnp.concatenate([qth, qh], axis=1), jnp.concatenate([kh, kth], axis=1), ((1,), (1,)))
        p = (a * w).astype(BF16)
        pt = (at * w).astype(BF16)
        b = (dot(g, vh, ((1,), (1,))) * w).astype(BF16)
        bt = dot(jnp.concatenate([gt, g], axis=1), jnp.concatenate([vh, vth], axis=1), ((1,), (1,)))
        bt = (bt * w).astype(BF16)
        s, st = forward.state[h, 0], forward.state[h, 1]
        outer = dot(jnp.concatenate([gt, g], axis=1), jnp.concatenate([s, st], axis=1), ((1,), (1,)))
        hq[:, c] = (
            dot(jnp.concatenate([bt, b], axis=1), jnp.concatenate([kh, kth], axis=0)) + dq * outer
        ).astype(BF16)
        hk_buf[:, c] = dot(jnp.concatenate([bt, b], axis=0), jnp.concatenate([qh, qth], axis=0), ((0,), (0,)))
        hv_buf[:, c] = dot(jnp.concatenate([pt, p], axis=0), jnp.concatenate([g, gt], axis=0), ((0,), (0,)))

    pl.loop(0, heads // 2)(inner_back)
    backward.out_wait()
    backward.scan()
    backward.home()
    pl.loop(heads // 2, heads)(inner_back)
    backward.home_wait()
    backward.settle()

    def last(i):
        h = lax.rem(backward.mine(i), heads)
        c = cols(h, d)
        w = scale * jnp.exp((length - 1.0 - pos[...]) * lg[h, :, 0:d] + (KEPT_LOG * total - cum[...]))
        s, st = backward.state[h, 0], backward.state[h, 1]
        ks = dot(jnp.concatenate([v[:, c], vt[:, c]], axis=1), jnp.concatenate([st, s], axis=1), ((1,), (1,)))
        vs = dot(jnp.concatenate([k[:, c], kt[:, c]], axis=1), jnp.concatenate([st, s], axis=0))
        hk[:, c] = (hk_buf[:, c] + w * ks).astype(BF16)
        hv[:, c] = (hv_buf[:, c] + w * vs).astype(BF16)

    pl.loop(0, heads // 2)(last)
    backward.settle_wait()
    pl.loop(heads // 2, heads)(last)
    forward.finish()
    backward.finish()
    for copy in w_copies:
        copy.wait_send()
    gather.finish()

    @pl.loop(1, n)
    def _(step):
        j = lax.rem(me + step, n)
        remote(mine.at[0], count.at[me], cs.at[j], cr.at[me], seq=j).wait_send()

    @pl.loop(0, heads)
    def _(i):
        c = cols(i, d)
        whole, top = zall.at[z, :, c], zall.at[z, 0:length, c]
        for kind, piece in enumerate((whole, whole, top, top)):
            remote(piece, piece, zs.at[i, kind], zr.at[i, kind], head=up).wait_send()


def store_kernel(*refs):
    copies = [pltpu.make_async_copy(refs[i], refs[3 + i], refs[6].at[i]) for i in range(3)]
    for copy in copies:
        copy.start()
    for copy in copies:
        copy.wait()


def on_device(n, groups, probe, source, content, probe_t, source_t, content_t, table, flags, weight, goal):
    length, width = probe.shape
    heads = table.shape[0]
    d = width // heads
    flags = flags.reshape(1, length)
    vmem, smem, hbm = (pl.BlockSpec(memory_space=m) for m in (pltpu.VMEM, pltpu.SMEM, pltpu.HBM))
    pair = pltpu.VMEM((heads // 2, 2, d, d), BF16)
    slots = pltpu.VMEM((n // 2, 2 * heads * d // n, d), BF16)
    scan = [pair, pair, pair, slots, slots, slots, slots, pltpu.VMEM((heads, 2, d, d), BF16), pair]
    narrow, wide = pltpu.VMEM((length, width), BF16), pltpu.VMEM((length, width), F32)
    rows = width // n
    dma = pltpu.SemaphoreType.DMA
    out = jax.ShapeDtypeStruct((length, width), BF16)
    results = pl.pallas_call(
        functools.partial(kernel, n, heads, groups),
        out_shape=(out, out, out),
        in_specs=[hbm] * 6 + [smem, vmem] + [hbm] * 2,
        out_specs=[vmem] * 3,
        scratch_shapes=[
            *[narrow] * 6, pltpu.VMEM(weight.shape, BF16), pltpu.VMEM(goal.shape, BF16),
            pltpu.VMEM((length, length), F32), pltpu.VMEM((length, length), F32),
            pltpu.VMEM((length, d), F32), pltpu.VMEM((length, d), F32),
            pltpu.VMEM((heads, 1, length), F32), pltpu.VMEM((1, 1, d), F32), pltpu.VMEM((n, 1, d), F32),
            *scan, *scan,
            pltpu.VMEM((groups, rows, weight.shape[1]), BF16),
            pltpu.VMEM((groups, width, width), BF16),
            pltpu.VMEM((groups, 2 * length, width), BF16),
            pltpu.VMEM((2 * length, width), F32),
            wide, wide, narrow, narrow, wide, wide,
            *([dma((4,))] + [dma((n // 2,))] * 4) * 2,
            dma((9,)), dma((n,)), dma((n,)), dma((4,)), dma((4,)), dma((36,)), dma((n, 2)), dma((heads, 4)), dma((heads, 4)),
        ],
        compiler_params=pltpu.CompilerParams(collective_id=0, has_side_effects=True, vmem_limit_bytes=52 << 20),
        name="retention_hvp",
    )(probe, source, content, probe_t, source_t, content_t, table, flags, weight, goal)
    return pl.pallas_call(
        store_kernel,
        out_shape=(out, out, out),
        in_specs=[vmem] * 3,
        out_specs=[hbm] * 3,
        scratch_shapes=[dma((3,))],
        compiler_params=pltpu.CompilerParams(vmem_limit_bytes=4 << 20),
        name="store",
    )(*results)


def solution(mesh):
    n, groups = mesh.shape["seq"], mesh.shape["head"]
    both = P("seq", "head")
    return jax.shard_map(
        functools.partial(on_device, n, groups),
        mesh=mesh,
        in_specs=(both,) * 6 + (P("head"), P("seq"), P("head", None), P("seq", None)),
        out_specs=(both,) * 3,
        check_vma=False,
    )
```

```python
import functools
import math

import jax
import jax.numpy as jnp
from jax import lax
from jax.experimental import pallas as pl
from jax.experimental.pallas import tpu as pltpu
from jax.sharding import PartitionSpec as P

LEVELS = 8
KEPT_LOG = math.log(0.7)
EPS = 1e-06
F32 = jnp.float32
BF16 = jnp.bfloat16
MESH = pl.DeviceIdType.MESH
FAR = 1e9
UNROLL = 2


def dot(a, b, dims=((1,), (0,))):
    return lax.dot_general(a, b, (dims, ((), ())), preferred_element_type=F32)


def cols(h, d):
    return pl.ds(pl.multiple_of(h * d, d), d)


def decay_tables(flags_ref, dist, fall, pos, cum):
    t = dist.shape[0]
    row = lax.broadcasted_iota(jnp.int32, (t, t), 0)
    col = lax.broadcasted_iota(jnp.int32, (t, t), 1)
    flags = jnp.broadcast_to(flags_ref[...].astype(F32), (t, t))
    cum_col = jnp.sum(jnp.where(col <= row, flags, 0.0), axis=1, keepdims=True)
    flag_col = jnp.sum(jnp.where(col == row, flags, 0.0), axis=1, keepdims=True)
    cum_row = jnp.sum(jnp.where(row <= col, flag_col, 0.0), axis=0, keepdims=True)
    dist[...] = jnp.where(row >= col, (row - col).astype(F32), FAR)
    fall[...] = KEPT_LOG * (cum_col - cum_row)
    pos[...] = lax.broadcasted_iota(jnp.int32, pos.shape, 0).astype(F32)
    cum[...] = KEPT_LOG * jnp.broadcast_to(cum_col, cum.shape)


def barrier_start(n, me, up, down):
    barrier = pltpu.get_barrier_semaphore()
    for z in (up, down):
        pl.semaphore_signal(barrier, inc=1, device_id={"head": z}, device_id_type=MESH)

    @pl.loop(1, n)
    def _(step):
        pl.semaphore_signal(barrier, inc=1, device_id={"seq": lax.rem(me + step, n)}, device_id_type=MESH)


def barrier_end(n):
    pl.semaphore_wait(pltpu.get_barrier_semaphore(), n + 1)


def weights_of(h, d, lg_ref, dist, fall):
    return jnp.exp(dist[...] * lg_ref[h] + fall[...]) * (d ** -0.5)


def remote(src, dst, send_sem, recv_sem, **where):
    return pltpu.make_async_remote_copy(
        src_ref=src, dst_ref=dst, send_sem=send_sem, recv_sem=recv_sem, device_id=where, device_id_type=MESH
    )


def arrival(dst, recv_sem):
    pltpu.make_async_copy(dst, dst, recv_sem).wait()


class GramGather:
    def __init__(self, me, full, send_sem, recv_sem):
        c = lax.rem(me, 2)
        x, y = lax.rem(me // 2, 4), me // 8
        self.me, self.c, self.f, self.s = me, c, x + c * (y - x), y + c * (x - y)
        self.full, self.send_sem, self.recv_sem = full, send_sem, recv_sem
        self.rows = full.shape[1] // 32

    def at(self, df, s_off, absolute=False):
        f = df if absolute else lax.rem(self.f + df + 4, 4)
        s = lax.rem(self.s + s_off + 4, 4)
        return (f * (1 + 3 * self.c) + s * (4 - 3 * self.c)) * 2 + self.c

    def view(self, piece, half=None):
        rows = pl.ds(pl.multiple_of(piece * self.rows, self.rows), self.rows)
        if half is None:
            return self.full.at[:, rows, :]
        return self.full.at[2 * half:2 * half + 2, rows, :]

    def send(self, piece, to, lane, half=None):
        view = self.view(piece, half)
        remote(view, view, self.send_sem.at[0], self.recv_sem.at[lane], seq=to).start()

    def wait(self, piece, lane):
        arrival(self.view(piece), self.recv_sem.at[lane])

    def spread(self, piece, df):
        self.send(piece, self.at(0, 1), self.lane(-1, df))
        self.send(piece, self.at(0, -1), self.lane(1, df))
        self.sideways(piece)

    def sideways(self, piece):
        self.send(piece, self.me + 1 - 2 * self.c, 12)

    def lane(self, step, df):
        return 3 + (4 if step == 1 else 0) + df % 4

    def pass_on(self, step, df, half):
        piece = self.at(df, step)
        self.wait(piece, self.lane(step, df))
        self.send(piece, self.at(0, -step), 11, half)
        self.sideways(piece)

    def round(self, k):
        if k == 0:
            self.send(self.me, self.at(1, 0), 0)
            self.send(self.me, self.at(-1, 0), 1)
            self.spread(self.me, 0)
        elif k == 1:
            for step, half in ((-1, 0), (1, 1)):
                self.wait(self.at(step, 0), half)
                self.send(self.at(step, 0), self.at(-step, 0), 2, half)
            for step in (-1, 1):
                self.spread(self.at(step, 0), step)
            for step, half in ((-1, 0), (1, 1)):
                self.pass_on(step, 0, half)
        elif k == 2:
            self.wait(self.at(2, 0), 2)
            self.spread(self.at(2, 0), 2)
        elif k == 3:
            for df in (-1, 1):
                for step, half in ((-1, 0), (1, 1)):
                    self.pass_on(step, df, half)
        elif k == 4:
            for step, half in ((-1, 0), (1, 1)):
                self.pass_on(step, 2, half)
        elif k == 5:
            four = self.full.at[:, 0:4 * self.rows, :]
            arrival(four, self.recv_sem.at[11])
            for df in range(4):
                self.sideways(self.at(df, 2))
        else:
            arrival(self.full.at[:, 0:16 * self.rows, :], self.recv_sem.at[12])

    def finish(self):
        sent = self.full.at[:, 0:31 * self.rows, :]
        pltpu.make_async_copy(sent, sent, self.send_sem.at[0]).wait()


class Scan:
    def __init__(self, me, n, heads, length, lg, count, buffers, sems, reverse):
        self.own, self.gift, self.peer, self.tot, self.recv, self.back, self.entry, self.state, self.gift2 = buffers
        self.pair_sem, hop_sem = sems
        self.s1, self.r1, self.s2, self.r2 = (hop_sem.at[i] for i in range(4))
        self.c, self.chip, self.chips = lax.rem(me, 2), me // 2, n // 2
        self.sibling = me + 1 - 2 * self.c
        self.half = heads // 2
        self.length, self.lg, self.count, self.reverse = length, lg, count, reverse
        self.per = self.chips // self.half
        self.rows = self.tot.shape[1] // 2
        self.d = self.tot.shape[2]

    def mine(self, i):
        return self.half * self.c + i

    def theirs(self, i):
        return self.half * (1 - self.c) + i

    def give(self):
        self.gift_copy = remote(self.gift, self.peer, self.pair_sem.at[0], self.pair_sem.at[1], seq=self.sibling)
        self.gift_copy.start()

    def decay(self, h, core):
        return jnp.exp(float(self.length) * self.lg[h, :, 0:self.d] + KEPT_LOG * self.count[2 * self.chip + core])

    def ordered(self, i, part):
        mine, peer = self.own[i, part].astype(F32), self.peer[i, part].astype(F32)
        return jnp.where(self.c == 0, mine, peer), jnp.where(self.c == 0, peer, mine)

    def combine(self):
        @pl.loop(0, self.half)
        def _(i):
            factor = self.decay(self.mine(i), 0 if self.reverse else 1)
            for part in range(2):
                first, second = self.ordered(i, part)
                total = first + factor * second if self.reverse else first * factor + second
                self.tot[pl.ds(i * self.per, self.per), part * self.rows:(part + 1) * self.rows, :] = (
                    total.astype(BF16).reshape(self.per, self.rows, self.d)
                )

    def spread(self, src, dst, send_sem, recv_sem):
        @pl.loop(1, self.chips)
        def _(step):
            p = lax.rem(self.chip + step, self.chips)
            remote(src.at[p], dst.at[self.chip], send_sem, recv_sem, seq=2 * p + self.c).start()

    def collect(self, src, dst, send_sem, recv_sem):
        sent, got = src.at[0:self.chips - 1], dst.at[0:self.chips - 1]
        pltpu.make_async_copy(sent, sent, send_sem).wait()
        arrival(got, recv_sem)

    def out(self):
        self.spread(self.tot, self.recv, self.s1, self.r1)

    def out_wait(self):
        self.collect(self.tot, self.recv, self.s1, self.r1)

    def scan(self):
        self.recv[self.chip] = self.tot[self.chip]
        lg = self.lg[self.mine(self.chip // self.per), :, 0:self.d]

        def step(i, run):
            p = self.chips - 1 - i if self.reverse else i
            self.back[p] = run.astype(BF16)
            factor = jnp.exp(2.0 * self.length * lg + KEPT_LOG * (self.count[2 * p] + self.count[2 * p + 1]))
            return run * factor + self.recv[p].astype(F32)

        lax.fori_loop(0, self.chips, step, jnp.zeros(self.recv.shape[1:], F32))
        self.entry[self.chip] = self.back[self.chip]

    def home(self):
        self.spread(self.back, self.entry, self.s2, self.r2)

    def home_wait(self):
        self.collect(self.back, self.entry, self.s2, self.r2)

    def settle(self):
        @pl.loop(0, self.half)
        def _(i):
            factor = self.decay(self.mine(i), 1 if self.reverse else 0)
            for part in range(2):
                first, second = self.ordered(i, part)
                edge = self.entry[pl.ds(i * self.per, self.per), part * self.rows:(part + 1) * self.rows, :]
                edge = edge.reshape(self.d, self.d).astype(F32)
                inside = factor * edge + (second if self.reverse else first)
                keep = (self.c == 1) if self.reverse else (self.c == 0)
                self.gift2[i, part] = jnp.where(keep, inside, edge).astype(BF16)
                self.state[self.mine(i), part] = jnp.where(keep, edge, inside).astype(BF16)

        self.gift2_copies = [
            remote(
                self.gift2.at[i], self.state.at[self.mine(i)],
                self.pair_sem.at[2], self.pair_sem.at[3 + i], seq=self.sibling,
            )
            for i in range(self.half)
        ]
        for copy in self.gift2_copies:
            copy.start()

    def settle_wait(self, i):
        arrival(self.state.at[self.theirs(i)], self.pair_sem.at[3 + i])

    def finish(self):
        pltpu.make_async_copy(self.gift2, self.gift2, self.pair_sem.at[2]).wait()


def kernel(n, heads, groups, *refs):
    inputs, (table_hbm, flags_hbm, w_hbm, goal_hbm), results = refs[:6], refs[6:10], refs[10:13]
    (q, k, v, qt, kt, vt, weight, goal, dist, fall, pos, cum, lg, mine, count) = refs[13:28]
    ahead, behind = refs[28:37], refs[37:46]
    (picked, gram, zall, gz, o_buf, ot_buf, g_buf, gt_buf, hk_buf, hv_buf) = refs[46:56]
    ahead_sems, behind_sems = refs[56:58], refs[58:60]
    (load_sem, cs, cr, ws, wr, gs, gr, zs, zr) = refs[60:69]
    (hq, hk, hv, g_rest, gt_rest, table, flags, out_sem) = refs[69:]
    me, z = lax.axis_index("seq"), lax.axis_index("head")
    up, down = lax.rem(z + 1, groups), lax.rem(z + groups - 1, groups)
    far = lax.rem(z + 2, groups)
    length, width = q.shape
    d = width // heads
    scale = d ** -0.5
    rows = width // n
    mine_rows = pl.ds(pl.multiple_of(me * rows, rows), rows)
    sources = (*inputs, w_hbm.at[mine_rows], w_hbm, goal_hbm, table_hbm, flags_hbm)
    loads = [
        pltpu.make_async_copy(src, dst, load_sem.at[i])
        for i, (src, dst) in enumerate(zip(sources, (q, k, v, qt, kt, vt, picked.at[z], weight, goal, table, flags)))
    ]
    for i in (9, 10, 6, 1, 2, 4, 5, 0, 3, 7, 8):
        loads[i].start()
    barrier_start(n, me, up, down)
    loads[9].wait()
    loads[10].wait()

    @pl.loop(0, heads)
    def _(h):
        fraction = jnp.full((1, length), table[h], jnp.int32).astype(F32) / (LEVELS - 1)
        rates = jnp.exp(math.log(1.0 / 32.0) + fraction * math.log(16.0 / (length * n)))
        lg[h] = jnp.log1p(-rates)

    decay_tables(flags, dist, fall, pos, cum)
    total = jnp.broadcast_to(jnp.sum(flags[...].astype(F32), axis=1, keepdims=True), (1, 128))
    mine[0] = total
    count[me] = total
    forward = Scan(me, n, heads, length, lg, count, ahead, ahead_sems, False)
    backward = Scan(me, n, heads, length, lg, count, behind, behind_sems, True)
    for i in (1, 2, 4, 5):
        loads[i].wait()

    def own_state(h, target, i):
        c = cols(h, d)
        w = scale * jnp.exp((length - 1.0 - pos[...]) * lg[h, :, 0:d] + (KEPT_LOG * total - cum[...]))
        kw = (k[:, c].astype(F32) * w).astype(BF16)
        ktw = (kt[:, c].astype(F32) * w).astype(BF16)
        both = dot(kw, jnp.concatenate([v[:, c], vt[:, c]], axis=1), ((0,), (0,)))
        target[i, 0] = both[:, :d].astype(BF16)
        target[i, 1] = (both[:, d:] + dot(ktw, v[:, c], ((0,), (0,)))).astype(BF16)

    loads[6].wait()
    barrier_end(n)
    half = rows // 2
    low, high = slice(0, half), slice(half, rows)

    def w_send(slot, part, lane, to):
        remote(picked.at[slot, part], picked.at[slot, part], ws.at[0], wr.at[lane], head=to).start()

    w_send(z, low, 0, up)
    w_send(z, high, 1, down)
    w_send(z, high, 2, up)
    w_send(z, low, 2, down)
    pl.loop(0, heads // 2, unroll=UNROLL)(lambda i: own_state(forward.theirs(i), forward.gift, i))
    remote(mine.at[0], count.at[me], cs.at[0], cr.at[0], seq=forward.sibling).start()
    forward.give()

    pl.loop(0, heads // 2, unroll=UNROLL)(lambda i: own_state(forward.mine(i), forward.own, i))
    arrival(count.at[forward.sibling], cr.at[0])
    arrival(forward.peer, forward.pair_sem.at[1])
    forward.combine()
    forward.out()
    loads[0].wait()
    loads[3].wait()

    def inner(h):
        c = cols(h, d)
        w = weights_of(h, d, lg, dist, fall)
        a = dot(q[:, c], k[:, c], ((1,), (1,)))
        at = dot(
            jnp.concatenate([qt[:, c], q[:, c]], axis=1), jnp.concatenate([k[:, c], kt[:, c]], axis=1), ((1,), (1,))
        )
        p = (a * w).astype(BF16)
        pt = (at * w).astype(BF16)
        both = dot(p, jnp.concatenate([v[:, c], vt[:, c]], axis=1))
        o_buf[:, c] = both[:, :d]
        ot_buf[:, c] = both[:, d:] + dot(pt, v[:, c])

    @pl.loop(1, n)
    def _(step):
        j = lax.rem(me + step, n)

        @pl.when(j != forward.sibling)
        def _():
            remote(mine.at[0], count.at[me], cs.at[0], cr.at[1], seq=j).start()

    pl.loop(0, heads // 2)(inner)
    arrival(picked.at[down, low], wr.at[0])
    w_send(down, low, 2, up)
    arrival(picked.at[up, high], wr.at[1])
    w_send(up, high, 2, down)
    arrival(count.at[0:n - 2], cr.at[1])
    forward.out_wait()
    forward.scan()
    forward.home()
    pl.loop(heads // 2, heads)(inner)
    arrival(picked.at[0:2], wr.at[2])
    loads[7].wait()
    tile = 256

    @pl.loop(0, width // tile)
    def _(i):
        c = cols(i, tile)
        part = dot(picked[...].reshape(groups * rows, weight.shape[1]), weight[c, :], ((1,), (1,)))
        gram[:, mine_rows, c] = part.astype(BF16).reshape(groups, rows, tile)

    gather = GramGather(me, gram, gs, gr)
    forward.home_wait()
    forward.settle()
    gather.round(0)

    def z_send(i):
        c = cols(lax.rem(forward.mine(i), heads), d)
        remote(zall.at[z, :, c], zall.at[z, :, c], zs.at[0], zr.at[2 * i], head=up).start()
        remote(zall.at[z, :, c], zall.at[z, :, c], zs.at[0], zr.at[2 * i + 1], head=down).start()

    def output(i):
        h = lax.rem(forward.mine(i), heads)
        c = cols(h, d)
        dq = jnp.exp((pos[...] + 1.0) * lg[h, :, 0:d] + cum[...])
        s, st = forward.state[h, 0], forward.state[h, 1]
        both = dot(q[:, c], jnp.concatenate([s, st], axis=1))
        o = o_buf[:, c] + dq * both[:, :d]
        ot = ot_buf[:, c] + dq * (both[:, d:] + dot(qt[:, c], s))
        o_buf[:, c] = o
        ot_buf[:, c] = ot
        r = lax.rsqrt(jnp.mean(o * o, axis=1, keepdims=True) + EPS)
        m = jnp.mean(o * ot, axis=1, keepdims=True)
        zall[z, 0:length, c] = (o * r).astype(BF16)
        zall[z, length:, c] = (r * ot - o * (r * r * r * m)).astype(BF16)

        if isinstance(i, int):
            z_send(i - 1)
        else:
            pl.when(i > 0)(lambda: z_send(i - 1))

    pl.loop(0, heads // 2)(output)
    for i in range(heads // 2, heads):
        forward.settle_wait(i - heads // 2)
        output(i)
    z_send(heads - 1)
    loads[8].wait()

    def goal_tile(i):
        c = slice(i * tile, (i + 1) * tile)
        gz[0:length, c] = -dot(goal[...], weight[c, :], ((1,), (1,)))

    def chunk(i):
        return cols(lax.rem(forward.mine(i), heads), d)

    groups_of = (0, 0, 0, 0, 1, 1, 2, 2)

    def relay(i):
        c = chunk(i)
        lane = 2 * heads + groups_of[i]
        arrival(zall.at[down, :, c], zr.at[2 * i])
        piece = zall.at[down, 0:length, c]
        remote(piece, piece, zs.at[0], zr.at[lane], head=up).start()
        arrival(zall.at[up, :, c], zr.at[2 * i + 1])
        piece = zall.at[up, length:, c]
        remote(piece, piece, zs.at[0], zr.at[lane], head=down).start()

    def span(first, number):
        return pl.ds(pl.multiple_of(lax.rem(forward.mine(first), heads) * d, number * d), number * d)

    def distant(first, number):
        arrival(zall.at[far, :, span(first, number)], zr.at[2 * heads + groups_of[first]])

    def add(first, number, *sources):
        part = span(first, number)

        @pl.loop(0, width // tile)
        def _(i):
            c = cols(i, tile)
            for r in (slice(0, length), slice(length, 2 * length)):
                gz[r, c] = sum((dot(zall[g, r, part], gram[g, part, c]) for g in sources), gz[r, c])

    goal_tile(0)
    goal_tile(1)
    gather.round(1)
    relay(0)
    goal_tile(2)
    relay(1)
    gather.round(2)
    goal_tile(3)
    relay(2)
    gather.round(3)
    relay(3)
    gather.round(4)
    relay(4)
    relay(5)
    gather.round(5)
    gather.round(6)
    @pl.loop(0, width // tile)
    def _(i):
        c = cols(i, tile)
        gz[0:length, c] = gz[0:length, c] + dot(zall[z, 0:length, :], gram[z, :, c])
        gz[length:, c] = dot(zall[z, length:, :], gram[z, :, c])

    relay(6)
    add(0, 4, up, down)
    relay(7)
    add(4, 4, up, down)
    distant(0, 4)
    add(0, 4, far)
    distant(4, 2)
    add(4, 2, far)
    distant(6, 2)
    add(6, 2, far)

    def norm_back(h, target, i):
        c = cols(h, d)
        dq = jnp.exp((pos[...] + 1.0) * lg[h, :, 0:d] + cum[...])
        o, ot = o_buf[:, c], ot_buf[:, c]
        gzh, gzt = gz[0:length, c], gz[length:, c]
        r = lax.rsqrt(jnp.mean(o * o, axis=1, keepdims=True) + EPS)
        r2 = r * r
        r3 = r2 * r
        mean = jnp.mean(o * ot, axis=1, keepdims=True)
        m = r3 * mean
        m1 = r3 * jnp.mean(o * gzh, axis=1, keepdims=True)
        m1t = r3 * jnp.mean(ot * gzh + o * gzt, axis=1, keepdims=True)
        g = r * gzh - m1 * o
        gt = r * gzt - m * gzh - m1 * ot + (3.0 * r2 * mean * m1 - m1t) * o
        for value, top, rest in ((g, g_buf, g_rest), (gt, gt_buf, gt_rest)):
            high = value.astype(BF16)
            top[:, c] = high
            rest[:, c] = (value - high.astype(F32)).astype(BF16)
        gd = (dq * g).astype(BF16)
        gtd = (dq * gt).astype(BF16)
        both = dot(q[:, c], jnp.concatenate([gd, gtd], axis=1), ((0,), (0,)))
        target[i, 0] = both[:, :d].astype(BF16)
        target[i, 1] = (both[:, d:] + dot(qt[:, c], gd, ((0,), (0,)))).astype(BF16)

    pl.loop(0, heads // 2, unroll=UNROLL)(lambda i: norm_back(backward.theirs(i), backward.gift, i))
    backward.give()
    pl.loop(0, heads // 2, unroll=UNROLL)(lambda i: norm_back(backward.mine(i), backward.own, i))
    arrival(backward.peer, backward.pair_sem.at[1])
    backward.combine()
    backward.out()

    def inner_back(h):
        c = cols(h, d)
        w = weights_of(h, d, lg, dist, fall)
        dq = jnp.exp((pos[...] + 1.0) * lg[h, :, 0:d] + cum[...])
        qh, kh, vh, qth, kth, vth, g, gt = (x[:, c] for x in (q, k, v, qt, kt, vt, g_buf, gt_buf))
        a = dot(qh, kh, ((1,), (1,)))
        at = dot(jnp.concatenate([qth, qh], axis=1), jnp.concatenate([kh, kth], axis=1), ((1,), (1,)))
        p = (a * w).astype(BF16)
        pt = (at * w).astype(BF16)
        g_lo, gt_lo = g_rest[:, c], gt_rest[:, c]
        b = dot(jnp.concatenate([g, g_lo], axis=1), jnp.concatenate([vh, vh], axis=1), ((1,), (1,)))
        b = (b * w).astype(BF16)
        bt = dot(
            jnp.concatenate([gt, gt_lo, g, g_lo], axis=1), jnp.concatenate([vh, vh, vth, vth], axis=1), ((1,), (1,))
        )
        bt = (bt * w).astype(BF16)
        s, st = forward.state[h, 0], forward.state[h, 1]
        outer = dot(jnp.concatenate([gt, g], axis=1), jnp.concatenate([s, st], axis=1), ((1,), (1,)))
        hq[:, c] = (
            dot(jnp.concatenate([bt, b], axis=1), jnp.concatenate([kh, kth], axis=0)) + dq * outer
        ).astype(BF16)
        hk_buf[:, c] = dot(jnp.concatenate([bt, b], axis=0), jnp.concatenate([qh, qth], axis=0), ((0,), (0,)))
        hv_buf[:, c] = dot(
            jnp.concatenate([pt, p, pt, p], axis=0), jnp.concatenate([g, gt, g_lo, gt_lo], axis=0), ((0,), (0,))
        )

    pl.loop(0, heads // 2)(inner_back)
    forward.finish()
    forward.gift_copy.wait_send()
    backward.gift_copy.wait_send()
    gather.finish()

    pltpu.make_async_copy(count.at[0:n - 1], count.at[0:n - 1], cs.at[0]).wait()
    pltpu.make_async_copy(picked.at[0:3], picked.at[0:3], ws.at[0]).wait()
    pltpu.make_async_copy(zall.at[0:3], zall.at[0:3], zs.at[0]).wait()

    backward.out_wait()
    backward.scan()
    backward.home()
    pl.loop(heads // 2, heads)(inner_back)
    pltpu.make_async_copy(hq, results[0], out_sem.at[0]).start()
    backward.home_wait()
    backward.settle()

    def last(i):
        h = lax.rem(backward.mine(i), heads)
        c = cols(h, d)
        w = scale * jnp.exp((length - 1.0 - pos[...]) * lg[h, :, 0:d] + (KEPT_LOG * total - cum[...]))
        s, st = backward.state[h, 0], backward.state[h, 1]
        ks = dot(jnp.concatenate([v[:, c], vt[:, c]], axis=1), jnp.concatenate([st, s], axis=1), ((1,), (1,)))
        vs = dot(jnp.concatenate([k[:, c], kt[:, c]], axis=1), jnp.concatenate([st, s], axis=0))
        hk[:, c] = (hk_buf[:, c] + w * ks).astype(BF16)
        hv[:, c] = (hv_buf[:, c] + w * vs).astype(BF16)

    def emit(kind, h):
        c = cols(h, d)
        pltpu.make_async_copy((hk, hv)[kind].at[:, c], results[1 + kind].at[:, c], out_sem.at[1 + kind]).start()

    for i in range(heads):
        if i >= heads // 2:
            backward.settle_wait(i - heads // 2)
        last(i)
        if i:
            emit(0, lax.rem(backward.mine(i - 1), heads))
            emit(1, lax.rem(backward.mine(i - 1), heads))
    emit(0, lax.rem(backward.mine(heads - 1), heads))
    emit(1, lax.rem(backward.mine(heads - 1), heads))
    backward.finish()
    for kind, buffer in enumerate((hq, hk, hv)):
        pltpu.make_async_copy(buffer, results[kind], out_sem.at[kind]).wait()


def store_kernel(*refs):
    copies = [pltpu.make_async_copy(refs[i], refs[3 + i], refs[6].at[i]) for i in range(3)]
    for copy in copies:
        copy.start()
    for copy in copies:
        copy.wait()


def on_device(n, groups, probe, source, content, probe_t, source_t, content_t, table, flags, weight, goal):
    length, width = probe.shape
    heads = table.shape[0]
    d = width // heads
    flags = flags.reshape(1, length)
    vmem, hbm = (pl.BlockSpec(memory_space=m) for m in (pltpu.VMEM, pltpu.HBM))
    pair = pltpu.VMEM((heads // 2, 2, d, d), BF16)
    slots = pltpu.VMEM((n // 2, 2 * heads * d // n, d), BF16)
    scan = [pair, pair, pair, slots, slots, slots, slots, pltpu.VMEM((heads, 2, d, d), BF16), pair]
    narrow, wide = pltpu.VMEM((length, width), BF16), pltpu.VMEM((length, width), F32)
    rows = width // n
    dma = pltpu.SemaphoreType.DMA
    out = jax.ShapeDtypeStruct((length, width), BF16)
    results = pl.pallas_call(
        functools.partial(kernel, n, heads, groups),
        out_shape=(out, out, out),
        in_specs=[hbm] * 10,
        out_specs=[pl.BlockSpec(memory_space=pl.ANY)] * 3,
        scratch_shapes=[
            *[narrow] * 6, pltpu.VMEM(weight.shape, BF16), pltpu.VMEM(goal.shape, BF16),
            pltpu.VMEM((length, length), F32), pltpu.VMEM((length, length), F32),
            pltpu.VMEM((length, d), F32), pltpu.VMEM((length, d), F32),
            pltpu.VMEM((heads, 1, length), F32), pltpu.VMEM((1, 1, d), F32), pltpu.VMEM((n, 1, d), F32),
            *scan, *scan,
            pltpu.VMEM((groups, rows, weight.shape[1]), BF16),
            pltpu.VMEM((groups, width, width), BF16),
            pltpu.VMEM((groups, 2 * length, width), BF16),
            pltpu.VMEM((2 * length, width), F32),
            wide, wide, narrow, narrow, wide, wide,
            *[dma((3 + heads // 2,)), dma((4,))] * 2,
            dma((11,)), dma((1,)), dma((2,)), dma((1,)), dma((3,)), dma((1,)), dma((13,)), dma((1,)), dma((2 * heads + 3,)),
            narrow, narrow, narrow, narrow, narrow, pltpu.SMEM(table.shape, jnp.int32), pltpu.VMEM(flags.shape, jnp.int32),
            dma((3,)),
        ],
        compiler_params=pltpu.CompilerParams(collective_id=0, has_side_effects=True, vmem_limit_bytes=52 << 20),
        name="retention_hvp",
    )(probe, source, content, probe_t, source_t, content_t, *(pltpu.with_memory_space_constraint(x, pltpu.HBM) for x in (table, flags)), weight, goal)
    return pl.pallas_call(
        store_kernel,
        out_shape=(out, out, out),
        in_specs=[vmem] * 3,
        out_specs=[hbm] * 3,
        scratch_shapes=[dma((3,))],
        compiler_params=pltpu.CompilerParams(vmem_limit_bytes=4 << 20),
        name="store",
    )(*results)


def solution(mesh):
    n, groups = mesh.shape["seq"], mesh.shape["head"]
    both = P("seq", "head")
    return jax.shard_map(
        functools.partial(on_device, n, groups),
        mesh=mesh,
        in_specs=(both,) * 6 + (P("head"), P("seq"), P("head", None), P("seq", None)),
        out_specs=(both,) * 3,
        check_vma=False,
    )
```

```python
import functools
import math

import jax
import jax.numpy as jnp
from jax import lax
from jax.experimental import pallas as pl
from jax.experimental.pallas import tpu as pltpu
from jax.sharding import PartitionSpec as P

LEVELS = 8
KEPT_LOG = math.log(0.7)
EPS = 1e-06
F32 = jnp.float32
BF16 = jnp.bfloat16
MESH = pl.DeviceIdType.MESH
FAR = 1e9
UNROLL = 2


def dot(a, b, dims=((1,), (0,))):
    return lax.dot_general(a, b, (dims, ((), ())), preferred_element_type=F32)


def cols(h, d):
    return pl.ds(pl.multiple_of(h * d, d), d)


def decay_tables(flags_ref, dist, fall, pos, cum):
    t = dist.shape[0]
    row = lax.broadcasted_iota(jnp.int32, (t, t), 0)
    col = lax.broadcasted_iota(jnp.int32, (t, t), 1)
    flags = jnp.broadcast_to(flags_ref[...].astype(F32), (t, t))
    cum_col = jnp.sum(jnp.where(col <= row, flags, 0.0), axis=1, keepdims=True)
    flag_col = jnp.sum(jnp.where(col == row, flags, 0.0), axis=1, keepdims=True)
    cum_row = jnp.sum(jnp.where(row <= col, flag_col, 0.0), axis=0, keepdims=True)
    dist[...] = jnp.where(row >= col, (row - col).astype(F32), FAR)
    fall[...] = KEPT_LOG * (cum_col - cum_row)
    pos[...] = lax.broadcasted_iota(jnp.int32, pos.shape, 0).astype(F32)
    cum[...] = KEPT_LOG * jnp.broadcast_to(cum_col, cum.shape)


def barrier_start(n, me, up, down):
    barrier = pltpu.get_barrier_semaphore()
    for z in (up, down):
        pl.semaphore_signal(barrier, inc=1, device_id={"head": z}, device_id_type=MESH)

    @pl.loop(1, n)
    def _(step):
        pl.semaphore_signal(barrier, inc=1, device_id={"seq": lax.rem(me + step, n)}, device_id_type=MESH)


def barrier_end(n):
    pl.semaphore_wait(pltpu.get_barrier_semaphore(), n + 1)


def weights_of(h, d, lg_ref, dist, fall):
    return jnp.exp(dist[...] * lg_ref[h] + fall[...]) * (d ** -0.5)


def remote(src, dst, send_sem, recv_sem, **where):
    return pltpu.make_async_remote_copy(
        src_ref=src, dst_ref=dst, send_sem=send_sem, recv_sem=recv_sem, device_id=where, device_id_type=MESH
    )


def arrival(dst, recv_sem):
    pltpu.make_async_copy(dst, dst, recv_sem).wait()


class GramGather:
    def __init__(self, me, full, part, parts, send_sem, recv_sem):
        c = lax.rem(me, 2)
        x, y = lax.rem(me // 2, 4), me // 8
        self.me, self.c, self.f, self.s = me, c, x + c * (y - x), y + c * (x - y)
        columns = full.shape[2] // parts
        self.full = full.at[:, :, part * columns:(part + 1) * columns]
        self.send_sem, self.recv_sem, self.base = send_sem.at[part], recv_sem, 13 * part
        self.rows = full.shape[1] // 32

    def at(self, df, s_off, absolute=False):
        f = df if absolute else lax.rem(self.f + df + 4, 4)
        s = lax.rem(self.s + s_off + 4, 4)
        return (f * (1 + 3 * self.c) + s * (4 - 3 * self.c)) * 2 + self.c

    def view(self, piece, half=None):
        rows = pl.ds(pl.multiple_of(piece * self.rows, self.rows), self.rows)
        if half is None:
            return self.full.at[:, rows, :]
        return self.full.at[2 * half:2 * half + 2, rows, :]

    def send(self, piece, to, lane, half=None):
        view = self.view(piece, half)
        remote(view, view, self.send_sem, self.recv_sem.at[self.base + lane], seq=to).start()

    def wait(self, piece, lane):
        arrival(self.view(piece), self.recv_sem.at[self.base + lane])

    def spread(self, piece, df):
        self.send(piece, self.at(0, 1), self.lane(-1, df))
        self.send(piece, self.at(0, -1), self.lane(1, df))
        self.sideways(piece)

    def sideways(self, piece):
        self.send(piece, self.me + 1 - 2 * self.c, 12)

    def lane(self, step, df):
        return 3 + (4 if step == 1 else 0) + df % 4

    def pass_on(self, step, df, half):
        piece = self.at(df, step)
        self.wait(piece, self.lane(step, df))
        self.send(piece, self.at(0, -step), 11, half)
        self.sideways(piece)

    def round(self, k):
        if k == 0:
            self.send(self.me, self.at(1, 0), 0)
            self.send(self.me, self.at(-1, 0), 1)
            self.spread(self.me, 0)
        elif k == 1:
            for step, half in ((-1, 0), (1, 1)):
                self.wait(self.at(step, 0), half)
                self.send(self.at(step, 0), self.at(-step, 0), 2, half)
            for step in (-1, 1):
                self.spread(self.at(step, 0), step)
            for step, half in ((-1, 0), (1, 1)):
                self.pass_on(step, 0, half)
        elif k == 2:
            self.wait(self.at(2, 0), 2)
            self.spread(self.at(2, 0), 2)
        elif k == 3:
            for df in (-1, 1):
                for step, half in ((-1, 0), (1, 1)):
                    self.pass_on(step, df, half)
        elif k == 4:
            for step, half in ((-1, 0), (1, 1)):
                self.pass_on(step, 2, half)
        elif k == 5:
            four = self.full.at[:, 0:4 * self.rows, :]
            arrival(four, self.recv_sem.at[self.base + 11])
            for df in range(4):
                self.sideways(self.at(df, 2))
        else:
            arrival(self.full.at[:, 0:16 * self.rows, :], self.recv_sem.at[self.base + 12])

    def finish(self):
        sent = self.full.at[:, 0:31 * self.rows, :]
        pltpu.make_async_copy(sent, sent, self.send_sem).wait()


class Scan:
    PARTS = 2

    def __init__(self, me, n, heads, length, lg, count, buffers, sems, reverse):
        self.own, self.gift, self.peer, self.tot, self.recv, self.back, self.entry, self.state, self.gift2 = buffers
        self.pair_sem, self.hop_sem = sems
        self.c, self.chip, self.chips = lax.rem(me, 2), me // 2, n // 2
        self.sibling = me + 1 - 2 * self.c
        self.half = heads // 2
        self.step = self.half // self.PARTS
        self.length, self.lg, self.count, self.reverse = length, lg, count, reverse
        self.per = self.chips // self.step
        self.rows = self.tot.shape[1] // 2
        self.d = self.tot.shape[2]

    def mine(self, i):
        return self.half * self.c + i

    def theirs(self, i):
        return self.half * (1 - self.c) + i

    def members(self, part):
        return range(part * self.step, (part + 1) * self.step)

    def give(self, part):
        some = slice(part * self.step, (part + 1) * self.step)
        remote(
            self.gift.at[some], self.peer.at[some], self.pair_sem.at[0], self.pair_sem.at[2 + part], seq=self.sibling
        ).start()

    def give_wait(self, part):
        arrival(self.peer.at[part * self.step:(part + 1) * self.step], self.pair_sem.at[2 + part])

    def decay(self, h, core):
        return jnp.exp(float(self.length) * self.lg[h, :, 0:self.d] + KEPT_LOG * self.count[2 * self.chip + core])

    def ordered(self, i, half):
        mine, peer = self.own[i, half].astype(F32), self.peer[i, half].astype(F32)
        return jnp.where(self.c == 0, mine, peer), jnp.where(self.c == 0, peer, mine)

    def slices(self, i):
        first = (i // self.step) * self.chips + (i % self.step) * self.per
        return slice(first, first + self.per)

    def combine(self, part):
        for i in self.members(part):
            factor = self.decay(self.mine(i), 0 if self.reverse else 1)
            for half in range(2):
                first, second = self.ordered(i, half)
                total = first + factor * second if self.reverse else first * factor + second
                self.tot[self.slices(i), half * self.rows:(half + 1) * self.rows, :] = (
                    total.astype(BF16).reshape(self.per, self.rows, self.d)
                )

    def spread(self, part, src, dst, hop):
        base = part * self.chips
        send_sem, recv_sem = self.hop_sem.at[4 * part + 2 * hop], self.hop_sem.at[4 * part + 2 * hop + 1]

        @pl.loop(1, self.chips)
        def _(step):
            p = lax.rem(self.chip + step, self.chips)
            remote(src.at[base + p], dst.at[base + self.chip], send_sem, recv_sem, seq=2 * p + self.c).start()

    def collect(self, part, src, dst, hop):
        sent, got = src.at[0:self.chips - 1], dst.at[0:self.chips - 1]
        pltpu.make_async_copy(sent, sent, self.hop_sem.at[4 * part + 2 * hop]).wait()
        arrival(got, self.hop_sem.at[4 * part + 2 * hop + 1])

    def out(self, part):
        self.spread(part, self.tot, self.recv, 0)

    def out_wait(self, part):
        self.collect(part, self.tot, self.recv, 0)

    def scan(self, part):
        base = part * self.chips
        self.recv[base + self.chip] = self.tot[base + self.chip]
        lg = self.lg[self.mine(part * self.step + self.chip // self.per), :, 0:self.d]

        def step(i, run):
            p = self.chips - 1 - i if self.reverse else i
            self.back[base + p] = run.astype(BF16)
            factor = jnp.exp(2.0 * self.length * lg + KEPT_LOG * (self.count[2 * p] + self.count[2 * p + 1]))
            return run * factor + self.recv[base + p].astype(F32)

        lax.fori_loop(0, self.chips, step, jnp.zeros(self.recv.shape[1:], F32))
        self.entry[base + self.chip] = self.back[base + self.chip]

    def home(self, part):
        self.spread(part, self.back, self.entry, 1)

    def home_wait(self, part):
        self.collect(part, self.back, self.entry, 1)

    def settle(self, part):
        for i in self.members(part):
            factor = self.decay(self.mine(i), 1 if self.reverse else 0)
            for half in range(2):
                first, second = self.ordered(i, half)
                edge = self.entry[self.slices(i), half * self.rows:(half + 1) * self.rows, :]
                edge = edge.reshape(self.d, self.d).astype(F32)
                inside = factor * edge + (second if self.reverse else first)
                keep = (self.c == 1) if self.reverse else (self.c == 0)
                self.gift2[i, half] = jnp.where(keep, inside, edge).astype(BF16)
                self.state[self.mine(i), half] = jnp.where(keep, edge, inside).astype(BF16)
        for i in self.members(part):
            remote(
                self.gift2.at[i], self.state.at[self.mine(i)],
                self.pair_sem.at[1], self.pair_sem.at[4 + i], seq=self.sibling,
            ).start()

    def settle_wait(self, i):
        arrival(self.state.at[self.theirs(i)], self.pair_sem.at[4 + i])

    def finish(self):
        pltpu.make_async_copy(self.gift, self.gift, self.pair_sem.at[0]).wait()
        pltpu.make_async_copy(self.gift2, self.gift2, self.pair_sem.at[1]).wait()


def kernel(n, heads, groups, *refs):
    inputs, (table_hbm, flags_hbm, w_hbm, goal_hbm), results = refs[:6], refs[6:10], refs[10:13]
    (q, k, v, qt, kt, vt, weight, goal, dist, fall, pos, cum, lg, mine, count) = refs[13:28]
    ahead, behind = refs[28:37], refs[37:46]
    (picked, gram, zall, gz, o_buf, ot_buf, g_buf, gt_buf, hk_buf, hv_buf) = refs[46:56]
    ahead_sems, behind_sems = refs[56:58], refs[58:60]
    (load_sem, cs, cr, ws, wr, gs, gr, zs, zr) = refs[60:69]
    (hq, hk, hv, g_rest, gt_rest, r_buf, rb_buf, q_turned, qt_turned, table, flags, out_sem) = refs[69:]
    me, z = lax.axis_index("seq"), lax.axis_index("head")
    up, down = lax.rem(z + 1, groups), lax.rem(z + groups - 1, groups)
    far = lax.rem(z + 2, groups)
    length, width = q.shape
    d = width // heads
    scale = d ** -0.5
    rows = width // n
    mine_rows = pl.ds(pl.multiple_of(me * rows, rows), rows)
    sources = (*inputs, w_hbm.at[mine_rows], w_hbm, goal_hbm, table_hbm, flags_hbm)
    loads = [
        pltpu.make_async_copy(src, dst, load_sem.at[i])
        for i, (src, dst) in enumerate(zip(sources, (q, k, v, qt, kt, vt, picked.at[z], weight, goal, table, flags)))
    ]
    for i in (9, 10, 6, 1, 2, 4, 5, 0, 3, 7, 8):
        loads[i].start()
    barrier_start(n, me, up, down)
    loads[9].wait()
    loads[10].wait()

    @pl.loop(0, heads)
    def _(h):
        fraction = jnp.full((1, length), table[h], jnp.int32).astype(F32) / (LEVELS - 1)
        rates = jnp.exp(math.log(1.0 / 32.0) + fraction * math.log(16.0 / (length * n)))
        lg[h] = jnp.log1p(-rates)

    decay_tables(flags, dist, fall, pos, cum)
    total = jnp.broadcast_to(jnp.sum(flags[...].astype(F32), axis=1, keepdims=True), (1, 128))
    mine[0] = total
    count[me] = total
    forward = Scan(me, n, heads, length, lg, count, ahead, ahead_sems, False)
    backward = Scan(me, n, heads, length, lg, count, behind, behind_sems, True)
    for i in (1, 2, 4, 5):
        loads[i].wait()

    def own_state(h, target, i):
        c = cols(h, d)
        w = scale * jnp.exp((length - 1.0 - pos[...]) * lg[h, :, 0:d] + (KEPT_LOG * total - cum[...]))
        kw = (k[:, c].astype(F32) * w).astype(BF16)
        ktw = (kt[:, c].astype(F32) * w).astype(BF16)
        both = dot(kw, jnp.concatenate([v[:, c], vt[:, c]], axis=1), ((0,), (0,)))
        target[i, 0] = both[:, :d].astype(BF16)
        target[i, 1] = (both[:, d:] + dot(ktw, v[:, c], ((0,), (0,)))).astype(BF16)

    loads[6].wait()
    barrier_end(n)
    half = rows // 2
    low, high = slice(0, half), slice(half, rows)

    def w_send(slot, part, lane, to):
        remote(picked.at[slot, part], picked.at[slot, part], ws.at[0], wr.at[lane], head=to).start()

    w_send(z, low, 0, up)
    w_send(z, high, 1, down)
    w_send(z, high, 2, up)
    w_send(z, low, 2, down)
    remote(mine.at[0], count.at[me], cs.at[0], cr.at[0], seq=forward.sibling).start()

    def own_part(part, whose, target):
        pl.loop(2 * part, 2 * part + 2, unroll=2)(lambda i: own_state(whose(i), target, i))

    own_part(0, forward.theirs, forward.gift)
    forward.give(0)
    own_part(0, forward.mine, forward.own)
    own_part(1, forward.theirs, forward.gift)
    forward.give(1)
    arrival(count.at[forward.sibling], cr.at[0])
    forward.give_wait(0)
    forward.combine(0)
    forward.out(0)
    own_part(1, forward.mine, forward.own)
    forward.give_wait(1)
    forward.combine(1)
    forward.out(1)
    loads[0].wait()
    loads[3].wait()

    def inner(h):
        c = cols(h, d)
        w = weights_of(h, d, lg, dist, fall)
        a = dot(q[:, c], k[:, c], ((1,), (1,)))
        at = dot(
            jnp.concatenate([qt[:, c], q[:, c]], axis=1), jnp.concatenate([k[:, c], kt[:, c]], axis=1), ((1,), (1,))
        )
        p = (a * w).astype(BF16)
        pt = (at * w).astype(BF16)
        both = dot(p, jnp.concatenate([v[:, c], vt[:, c]], axis=1))
        o_buf[:, c] = both[:, :d]
        ot_buf[:, c] = both[:, d:] + dot(pt, v[:, c])

    @pl.loop(1, n)
    def _(step):
        j = lax.rem(me + step, n)

        @pl.when(j != forward.sibling)
        def _():
            remote(mine.at[0], count.at[me], cs.at[0], cr.at[1], seq=j).start()

    pl.loop(0, heads // 2)(inner)
    arrival(picked.at[down, low], wr.at[0])
    w_send(down, low, 2, up)
    arrival(picked.at[up, high], wr.at[1])
    w_send(up, high, 2, down)
    arrival(count.at[0:n - 2], cr.at[1])
    forward.out_wait(0)
    forward.scan(0)
    forward.home(0)
    forward.out_wait(1)
    forward.scan(1)
    forward.home(1)
    pl.loop(heads // 2, heads)(inner)
    tile = 256

    def gram_tile(i):
        c = slice(i * tile, (i + 1) * tile)
        part = dot(picked[...].reshape(groups * rows, weight.shape[1]), weight[c, :], ((1,), (1,)))
        gram[:, mine_rows, c] = part.astype(BF16).reshape(groups, rows, tile)

    gathers = [GramGather(me, gram, part, 2, gs, gr) for part in range(2)]

    def head_of(i):
        part, place = i // 4, i % 4
        return forward.mine(2 * part + place) if place < 2 else forward.theirs(2 * part + place - 2)

    def z_send(i):
        c = cols(head_of(i), d)
        remote(zall.at[z, :, c], zall.at[z, :, c], zs.at[0], zr.at[2 * i], head=up).start()
        remote(zall.at[z, :, c], zall.at[z, :, c], zs.at[0], zr.at[2 * i + 1], head=down).start()

    def output(i):
        h = head_of(i)
        c = cols(h, d)
        dq = jnp.exp((pos[...] + 1.0) * lg[h, :, 0:d] + cum[...])
        s, st = forward.state[h, 0], forward.state[h, 1]
        both = dot(q[:, c], jnp.concatenate([s, st], axis=1))
        o = o_buf[:, c] + dq * both[:, :d]
        ot = ot_buf[:, c] + dq * (both[:, d:] + dot(qt[:, c], s))
        o_buf[:, c] = o
        ot_buf[:, c] = ot
        r = lax.rsqrt(jnp.mean(o * o, axis=1, keepdims=True) + EPS)
        m = jnp.mean(o * ot, axis=1, keepdims=True)
        zall[z, 0:length, c] = (o * r).astype(BF16)
        zall[z, length:, c] = (r * ot - o * (r * r * r * m)).astype(BF16)

        if i % 4:
            z_send(i - 1)

    forward.home_wait(0)
    forward.settle(0)
    output(0)
    output(1)
    for i in range(2):
        forward.settle_wait(i)
        output(2 + i)
    z_send(3)
    arrival(picked.at[0:2], wr.at[2])
    loads[7].wait()
    for part in range(2):
        gram_tile(2 * part)
        gram_tile(2 * part + 1)
        gathers[part].round(0)
    forward.home_wait(1)
    forward.settle(1)
    output(4)
    output(5)
    for i in range(2):
        forward.settle_wait(2 + i)
        output(6 + i)
    z_send(7)
    loads[8].wait()

    def goal_tile(i):
        c = slice(i * tile, (i + 1) * tile)
        gz[0:length, c] = -dot(goal[...], weight[c, :], ((1,), (1,)))

    groups_of = (0, 0, 0, 0, 1, 1, 2, 2)

    def relay(i):
        c = cols(head_of(i), d)
        lane = 2 * heads + groups_of[i]
        arrival(zall.at[down, :, c], zr.at[2 * i])
        piece = zall.at[down, 0:length, c]
        remote(piece, piece, zs.at[0], zr.at[lane], head=up).start()
        arrival(zall.at[up, :, c], zr.at[2 * i + 1])
        piece = zall.at[up, length:, c]
        remote(piece, piece, zs.at[0], zr.at[lane], head=down).start()

    def distant(first, number):
        arrival(zall.at[far, :, 0:number * d], zr.at[2 * heads + groups_of[first]])

    def add(pairs, source):
        parts = [pl.ds(pl.multiple_of(head_of(2 * p) * d, 2 * d), 2 * d) for p in pairs]

        for i in range(width // tile):
            c = slice(i * tile, (i + 1) * tile)
            for r in (slice(0, length), slice(length, 2 * length)):
                gz[r, c] = sum((dot(zall[source, r, p], gram[source, p, c]) for p in parts), gz[r, c])

    def add_whole(first, last, *sources, fresh=False):
        for i in range(first, last):
            c = slice(i * tile, (i + 1) * tile)
            for r in (slice(0, length), slice(length, 2 * length)):
                start = 0.0 if fresh and r.start else gz[r, c]
                gz[r, c] = sum((dot(zall[g, r, :], gram[g, :, c]) for g in sources), start)

    def prepare(h):
        c = cols(h, d)
        dq = jnp.exp((pos[...] + 1.0) * lg[h, :, 0:d] + cum[...])
        o, ot = o_buf[:, c], ot_buf[:, c]
        r = lax.rsqrt(jnp.mean(o * o, axis=1, keepdims=True) + EPS)
        m = r * r * jnp.mean(o * ot, axis=1, keepdims=True)
        zf = o * r
        o_buf[:, c] = zf
        ot_buf[:, c] = r * ot - zf * m
        r_buf[:, c] = jnp.broadcast_to(r, o.shape)
        rb_buf[:, c] = jnp.broadcast_to(m, o.shape)
        q_turned[c, :] = (q[:, c].astype(F32) * dq).T.astype(BF16)
        qt_turned[c, :] = (qt[:, c].astype(F32) * dq).T.astype(BF16)

    goal_tile(0)
    gathers[0].round(1)
    relay(0)
    gathers[1].round(1)
    goal_tile(1)
    relay(1)
    gathers[0].round(2)
    goal_tile(2)
    gathers[1].round(2)
    relay(2)
    gathers[0].round(3)
    goal_tile(3)
    gathers[1].round(3)
    relay(3)
    gathers[0].round(4)
    relay(4)
    pl.loop(0, 4)(prepare)
    gathers[1].round(4)
    relay(5)
    gathers[0].round(5)
    relay(6)
    pl.loop(4, 8)(prepare)
    gathers[1].round(5)
    gathers[0].round(6)
    add_whole(0, 2, z, fresh=True)
    relay(7)
    gathers[1].round(6)
    add_whole(2, 4, z, fresh=True)
    add_whole(0, 4, up, down)
    distant(0, 4)
    add((0, 1), far)
    distant(4, 2)
    add((2,), far)
    distant(6, 2)
    add((3,), far)

    def norm_back(h, target, i):
        c = cols(h, d)
        zf, ztf = o_buf[:, c], ot_buf[:, c]
        gzh, gzt = gz[0:length, c], gz[length:, c]
        a = jnp.mean(zf * gzh, axis=1, keepdims=True)
        at = jnp.mean(ztf * gzh + zf * gzt, axis=1, keepdims=True)
        r = r_buf[:, c]
        g = r * (gzh - zf * a)
        gt = r * (gzt - ztf * a - zf * at) - rb_buf[:, c] * g
        for value, top, rest in ((g, g_buf, g_rest), (gt, gt_buf, gt_rest)):
            high = value.astype(BF16)
            top[:, c] = high
            rest[:, c] = (value - high.astype(F32)).astype(BF16)
        both = dot(q_turned[c, :], jnp.concatenate([g, gt], axis=1).astype(BF16))
        target[i, 0] = both[:, :d].astype(BF16)
        target[i, 1] = (both[:, d:] + dot(qt_turned[c, :], g.astype(BF16))).astype(BF16)

    def norm_part(part, whose, target):
        pl.loop(2 * part, 2 * part + 2, unroll=2)(lambda i: norm_back(whose(i), target, i))

    norm_part(0, backward.theirs, backward.gift)
    backward.give(0)
    norm_part(0, backward.mine, backward.own)
    backward.give_wait(0)
    backward.combine(0)
    backward.out(0)
    norm_part(1, backward.theirs, backward.gift)
    backward.give(1)
    norm_part(1, backward.mine, backward.own)
    backward.give_wait(1)
    backward.combine(1)
    backward.out(1)

    def inner_back(h):
        c = cols(h, d)
        w = weights_of(h, d, lg, dist, fall)
        dq = jnp.exp((pos[...] + 1.0) * lg[h, :, 0:d] + cum[...])
        qh, kh, vh, qth, kth, vth, g, gt = (x[:, c] for x in (q, k, v, qt, kt, vt, g_buf, gt_buf))
        a = dot(qh, kh, ((1,), (1,)))
        at = dot(jnp.concatenate([qth, qh], axis=1), jnp.concatenate([kh, kth], axis=1), ((1,), (1,)))
        p = (a * w).astype(BF16)
        pt = (at * w).astype(BF16)
        g_lo, gt_lo = g_rest[:, c], gt_rest[:, c]
        b = dot(jnp.concatenate([g, g_lo], axis=1), jnp.concatenate([vh, vh], axis=1), ((1,), (1,)))
        b = (b * w).astype(BF16)
        bt = dot(
            jnp.concatenate([gt, gt_lo, g, g_lo], axis=1), jnp.concatenate([vh, vh, vth, vth], axis=1), ((1,), (1,))
        )
        bt = (bt * w).astype(BF16)
        s, st = forward.state[h, 0], forward.state[h, 1]
        outer = dot(jnp.concatenate([gt, g], axis=1), jnp.concatenate([s, st], axis=1), ((1,), (1,)))
        hq[:, c] = (
            dot(jnp.concatenate([bt, b], axis=1), jnp.concatenate([kh, kth], axis=0)) + dq * outer
        ).astype(BF16)
        hk_buf[:, c] = dot(jnp.concatenate([bt, b], axis=0), jnp.concatenate([qh, qth], axis=0), ((0,), (0,)))
        hv_buf[:, c] = dot(
            jnp.concatenate([pt, p, pt, p], axis=0), jnp.concatenate([g, gt, g_lo, gt_lo], axis=0), ((0,), (0,))
        )

    pl.loop(0, 3)(inner_back)
    forward.finish()
    for gather in gathers:
        gather.finish()

    pltpu.make_async_copy(count.at[0:n - 1], count.at[0:n - 1], cs.at[0]).wait()
    pltpu.make_async_copy(picked.at[0:3], picked.at[0:3], ws.at[0]).wait()
    pltpu.make_async_copy(zall.at[0:3], zall.at[0:3], zs.at[0]).wait()

    backward.out_wait(0)
    backward.scan(0)
    backward.home(0)
    pl.loop(3, 5)(inner_back)
    backward.out_wait(1)
    backward.scan(1)
    backward.home(1)
    pl.loop(5, heads)(inner_back)
    pltpu.make_async_copy(hq, results[0], out_sem.at[0]).start()

    def last(i):
        h = lax.rem(backward.mine(i), heads)
        c = cols(h, d)
        w = scale * jnp.exp((length - 1.0 - pos[...]) * lg[h, :, 0:d] + (KEPT_LOG * total - cum[...]))
        s, st = backward.state[h, 0], backward.state[h, 1]
        ks = dot(jnp.concatenate([v[:, c], vt[:, c]], axis=1), jnp.concatenate([st, s], axis=1), ((1,), (1,)))
        vs = dot(jnp.concatenate([k[:, c], kt[:, c]], axis=1), jnp.concatenate([st, s], axis=0))
        hk[:, c] = (hk_buf[:, c] + w * ks).astype(BF16)
        hv[:, c] = (hv_buf[:, c] + w * vs).astype(BF16)

    def emit(kind, h):
        c = cols(h, d)
        pltpu.make_async_copy((hk, hv)[kind].at[:, c], results[1 + kind].at[:, c], out_sem.at[1 + kind]).start()

    def finish(i):
        last(i)
        if i:
            emit(0, lax.rem(backward.mine(i - 1), heads))
            emit(1, lax.rem(backward.mine(i - 1), heads))

    backward.home_wait(0)
    backward.settle(0)
    finish(0)
    finish(1)
    backward.home_wait(1)
    backward.settle(1)
    finish(2)
    finish(3)
    for i in range(heads // 2):
        backward.settle_wait(i)
        finish(heads // 2 + i)
    emit(0, lax.rem(backward.mine(heads - 1), heads))
    emit(1, lax.rem(backward.mine(heads - 1), heads))
    backward.finish()
    for kind, buffer in enumerate((hq, hk, hv)):
        pltpu.make_async_copy(buffer, results[kind], out_sem.at[kind]).wait()


def store_kernel(*refs):
    copies = [pltpu.make_async_copy(refs[i], refs[3 + i], refs[6].at[i]) for i in range(3)]
    for copy in copies:
        copy.start()
    for copy in copies:
        copy.wait()


def on_device(n, groups, probe, source, content, probe_t, source_t, content_t, table, flags, weight, goal):
    length, width = probe.shape
    heads = table.shape[0]
    d = width // heads
    flags = flags.reshape(1, length)
    vmem, hbm = (pl.BlockSpec(memory_space=m) for m in (pltpu.VMEM, pltpu.HBM))
    pair = pltpu.VMEM((heads // 2, 2, d, d), BF16)
    slots = pltpu.VMEM((n // 2 * Scan.PARTS, 2 * heads * d // n // Scan.PARTS, d), BF16)
    scan = [pair, pair, pair, slots, slots, slots, slots, pltpu.VMEM((heads, 2, d, d), BF16), pair]
    narrow, wide = pltpu.VMEM((length, width), BF16), pltpu.VMEM((length, width), F32)
    rows = width // n
    dma = pltpu.SemaphoreType.DMA
    out = jax.ShapeDtypeStruct((length, width), BF16)
    results = pl.pallas_call(
        functools.partial(kernel, n, heads, groups),
        out_shape=(out, out, out),
        in_specs=[hbm] * 10,
        out_specs=[pl.BlockSpec(memory_space=pl.ANY)] * 3,
        scratch_shapes=[
            *[narrow] * 6, pltpu.VMEM(weight.shape, BF16), pltpu.VMEM(goal.shape, BF16),
            pltpu.VMEM((length, length), F32), pltpu.VMEM((length, length), F32),
            pltpu.VMEM((length, d), F32), pltpu.VMEM((length, d), F32),
            pltpu.VMEM((heads, 1, length), F32), pltpu.VMEM((1, 1, d), F32), pltpu.VMEM((n, 1, d), F32),
            *scan, *scan,
            pltpu.VMEM((groups, rows, weight.shape[1]), BF16),
            pltpu.VMEM((groups, width, width), BF16),
            pltpu.VMEM((groups, 2 * length, width), BF16),
            pltpu.VMEM((2 * length, width), F32),
            wide, wide, narrow, narrow, wide, wide,
            *[dma((4 + heads // 2,)), dma((4 * Scan.PARTS,))] * 2,
            dma((11,)), dma((1,)), dma((2,)), dma((1,)), dma((3,)), dma((2,)), dma((26,)), dma((1,)), dma((2 * heads + 3,)),
            narrow, narrow, narrow, narrow, narrow, wide, wide,
            pltpu.VMEM((width, length), BF16), pltpu.VMEM((width, length), BF16), pltpu.SMEM(table.shape, jnp.int32), pltpu.VMEM(flags.shape, jnp.int32),
            dma((3,)),
        ],
        compiler_params=pltpu.CompilerParams(collective_id=0, has_side_effects=True, vmem_limit_bytes=52 << 20),
        name="retention_hvp",
    )(probe, source, content, probe_t, source_t, content_t, *(pltpu.with_memory_space_constraint(x, pltpu.HBM) for x in (table, flags)), weight, goal)
    return pl.pallas_call(
        store_kernel,
        out_shape=(out, out, out),
        in_specs=[vmem] * 3,
        out_specs=[hbm] * 3,
        scratch_shapes=[dma((3,))],
        compiler_params=pltpu.CompilerParams(vmem_limit_bytes=4 << 20),
        name="store",
    )(*results)


def solution(mesh):
    n, groups = mesh.shape["seq"], mesh.shape["head"]
    both = P("seq", "head")
    return jax.shard_map(
        functools.partial(on_device, n, groups),
        mesh=mesh,
        in_specs=(both,) * 6 + (P("head"), P("seq"), P("head", None), P("seq", None)),
        out_specs=(both,) * 3,
        check_vma=False,
    )
```

```python
import functools
import math

import jax
import jax.numpy as jnp
from jax import lax
from jax.experimental import pallas as pl
from jax.experimental.pallas import tpu as pltpu
from jax.sharding import PartitionSpec as P

LEVELS = 8
KEPT_LOG = math.log(0.7)
EPS = 1e-06
F32 = jnp.float32
BF16 = jnp.bfloat16
MESH = pl.DeviceIdType.MESH
FAR = 1e9
UNROLL = 2


def dot(a, b, dims=((1,), (0,))):
    return lax.dot_general(a, b, (dims, ((), ())), preferred_element_type=F32)


def cols(h, d):
    return pl.ds(pl.multiple_of(h * d, d), d)


def reset_counts(flags_ref, pos, cum):
    t = pos.shape[0]
    row = lax.broadcasted_iota(jnp.int32, (t, t), 0)
    col = lax.broadcasted_iota(jnp.int32, (t, t), 1)
    flags = jnp.broadcast_to(flags_ref[...].astype(F32), (t, t))
    cum_col = jnp.sum(jnp.where(col <= row, flags, 0.0), axis=1, keepdims=True)
    pos[...] = lax.broadcasted_iota(jnp.int32, pos.shape, 0).astype(F32)
    cum[...] = KEPT_LOG * jnp.broadcast_to(cum_col, cum.shape)


def decay_tables(flags_ref, dist, fall):
    t = dist.shape[0]
    row = lax.broadcasted_iota(jnp.int32, (t, t), 0)
    col = lax.broadcasted_iota(jnp.int32, (t, t), 1)
    flags = jnp.broadcast_to(flags_ref[...].astype(F32), (t, t))
    cum_col = jnp.sum(jnp.where(col <= row, flags, 0.0), axis=1, keepdims=True)
    flag_col = jnp.sum(jnp.where(col == row, flags, 0.0), axis=1, keepdims=True)
    cum_row = jnp.sum(jnp.where(row <= col, flag_col, 0.0), axis=0, keepdims=True)
    dist[...] = jnp.where(row >= col, (row - col).astype(F32), FAR)
    fall[...] = KEPT_LOG * (cum_col - cum_row)


def barrier_start(n, me, up, down):
    barrier = pltpu.get_barrier_semaphore()
    for z in (up, down):
        pl.semaphore_signal(barrier, inc=1, device_id={"head": z}, device_id_type=MESH)

    @pl.loop(1, n)
    def _(step):
        pl.semaphore_signal(barrier, inc=1, device_id={"seq": lax.rem(me + step, n)}, device_id_type=MESH)


def barrier_end(n):
    pl.semaphore_wait(pltpu.get_barrier_semaphore(), n + 1)


def weights_of(h, d, lg_ref, dist, fall):
    return jnp.exp(dist[...] * lg_ref[h] + fall[...]) * (d ** -0.5)


def remote(src, dst, send_sem, recv_sem, **where):
    return pltpu.make_async_remote_copy(
        src_ref=src, dst_ref=dst, send_sem=send_sem, recv_sem=recv_sem, device_id=where, device_id_type=MESH
    )


def arrival(dst, recv_sem):
    pltpu.make_async_copy(dst, dst, recv_sem).wait()


class GramGather:
    def __init__(self, me, full, part, parts, send_sem, recv_sem):
        c = lax.rem(me, 2)
        x, y = lax.rem(me // 2, 4), me // 8
        self.me, self.c, self.f, self.s = me, c, x + c * (y - x), y + c * (x - y)
        columns = full.shape[2] // parts
        self.full = full.at[:, :, part * columns:(part + 1) * columns]
        self.send_sem, self.recv_sem, self.base = send_sem.at[part], recv_sem, 13 * part
        self.rows = full.shape[1] // 32

    def at(self, df, s_off, absolute=False):
        f = df if absolute else lax.rem(self.f + df + 4, 4)
        s = lax.rem(self.s + s_off + 4, 4)
        return (f * (1 + 3 * self.c) + s * (4 - 3 * self.c)) * 2 + self.c

    def view(self, piece, half=None):
        rows = pl.ds(pl.multiple_of(piece * self.rows, self.rows), self.rows)
        if half is None:
            return self.full.at[:, rows, :]
        return self.full.at[2 * half:2 * half + 2, rows, :]

    def send(self, piece, to, lane, half=None):
        view = self.view(piece, half)
        remote(view, view, self.send_sem, self.recv_sem.at[self.base + lane], seq=to).start()

    def wait(self, piece, lane):
        arrival(self.view(piece), self.recv_sem.at[self.base + lane])

    def spread(self, piece, df):
        self.send(piece, self.at(0, 1), self.lane(-1, df))
        self.send(piece, self.at(0, -1), self.lane(1, df))
        self.sideways(piece)

    def sideways(self, piece):
        self.send(piece, self.me + 1 - 2 * self.c, 12)

    def lane(self, step, df):
        return 3 + (4 if step == 1 else 0) + df % 4

    def pass_on(self, step, df, half):
        piece = self.at(df, step)
        self.wait(piece, self.lane(step, df))
        self.send(piece, self.at(0, -step), 11, half)
        self.sideways(piece)

    def round(self, k):
        if k == 0:
            self.send(self.me, self.at(1, 0), 0)
            self.send(self.me, self.at(-1, 0), 1)
            self.spread(self.me, 0)
        elif k == 1:
            for step, half in ((-1, 0), (1, 1)):
                self.wait(self.at(step, 0), half)
                self.send(self.at(step, 0), self.at(-step, 0), 2, half)
            for step in (-1, 1):
                self.spread(self.at(step, 0), step)
            for step, half in ((-1, 0), (1, 1)):
                self.pass_on(step, 0, half)
        elif k == 2:
            self.wait(self.at(2, 0), 2)
            self.spread(self.at(2, 0), 2)
        elif k == 3:
            for df in (-1, 1):
                for step, half in ((-1, 0), (1, 1)):
                    self.pass_on(step, df, half)
        elif k == 4:
            for step, half in ((-1, 0), (1, 1)):
                self.pass_on(step, 2, half)
        elif k == 5:
            four = self.full.at[:, 0:4 * self.rows, :]
            arrival(four, self.recv_sem.at[self.base + 11])
            for df in range(4):
                self.sideways(self.at(df, 2))
        else:
            arrival(self.full.at[:, 0:16 * self.rows, :], self.recv_sem.at[self.base + 12])

    def finish(self):
        sent = self.full.at[:, 0:31 * self.rows, :]
        pltpu.make_async_copy(sent, sent, self.send_sem).wait()


class Scan:
    PARTS = 2

    def __init__(self, me, n, heads, length, lg, count, buffers, sems, reverse):
        self.own, self.gift, self.peer, self.tot, self.recv, self.back, self.entry, self.state, self.gift2 = buffers
        self.pair_sem, self.hop_sem = sems
        self.c, self.chip, self.chips = lax.rem(me, 2), me // 2, n // 2
        self.sibling = me + 1 - 2 * self.c
        self.half = heads // 2
        self.step = self.half // self.PARTS
        self.length, self.lg, self.count, self.reverse = length, lg, count, reverse
        self.per = self.chips // self.step
        self.rows = self.tot.shape[1] // 2
        self.d = self.tot.shape[2]

    def mine(self, i):
        return self.half * self.c + i

    def theirs(self, i):
        return self.half * (1 - self.c) + i

    def members(self, part):
        return range(part * self.step, (part + 1) * self.step)

    def give(self, part):
        some = slice(part * self.step, (part + 1) * self.step)
        remote(
            self.gift.at[some], self.peer.at[some], self.pair_sem.at[0], self.pair_sem.at[2 + part], seq=self.sibling
        ).start()

    def give_wait(self, part):
        arrival(self.peer.at[part * self.step:(part + 1) * self.step], self.pair_sem.at[2 + part])

    def decay(self, h, core):
        return jnp.exp(float(self.length) * self.lg[h, :, 0:self.d] + KEPT_LOG * self.count[2 * self.chip + core])

    def ordered(self, i, half):
        mine, peer = self.own[i, half].astype(F32), self.peer[i, half].astype(F32)
        return jnp.where(self.c == 0, mine, peer), jnp.where(self.c == 0, peer, mine)

    def slices(self, i):
        first = (i // self.step) * self.chips + (i % self.step) * self.per
        return slice(first, first + self.per)

    def combine(self, part):
        for i in self.members(part):
            factor = self.decay(self.mine(i), 0 if self.reverse else 1)
            for half in range(2):
                first, second = self.ordered(i, half)
                total = first + factor * second if self.reverse else first * factor + second
                self.tot[self.slices(i), half * self.rows:(half + 1) * self.rows, :] = (
                    total.astype(BF16).reshape(self.per, self.rows, self.d)
                )

    def spread(self, part, src, dst, hop):
        base = part * self.chips
        send_sem, recv_sem = self.hop_sem.at[4 * part + 2 * hop], self.hop_sem.at[4 * part + 2 * hop + 1]

        x, y = lax.rem(self.chip, 4), self.chip // 4
        for dy, dx in sorted(
            ((a, b) for a in range(4) for b in range(4) if a or b), key=lambda t: -min(t[0], 4 - t[0]) - min(t[1], 4 - t[1])
        ):
            p = lax.rem(y + dy, 4) * 4 + lax.rem(x + dx, 4)
            remote(src.at[base + p], dst.at[base + self.chip], send_sem, recv_sem, seq=2 * p + self.c).start()

    def collect(self, part, src, dst, hop):
        sent, got = src.at[0:self.chips - 1], dst.at[0:self.chips - 1]
        pltpu.make_async_copy(sent, sent, self.hop_sem.at[4 * part + 2 * hop]).wait()
        arrival(got, self.hop_sem.at[4 * part + 2 * hop + 1])

    def out(self, part):
        self.spread(part, self.tot, self.recv, 0)

    def out_wait(self, part):
        self.collect(part, self.tot, self.recv, 0)

    def scan(self, part):
        base = part * self.chips
        self.recv[base + self.chip] = self.tot[base + self.chip]
        lg = self.lg[self.mine(part * self.step + self.chip // self.per), :, 0:self.d]

        def step(i, run):
            p = self.chips - 1 - i if self.reverse else i
            self.back[base + p] = run.astype(BF16)
            factor = jnp.exp(2.0 * self.length * lg + KEPT_LOG * (self.count[2 * p] + self.count[2 * p + 1]))
            return run * factor + self.recv[base + p].astype(F32)

        lax.fori_loop(0, self.chips, step, jnp.zeros(self.recv.shape[1:], F32))
        self.entry[base + self.chip] = self.back[base + self.chip]

    def home(self, part):
        self.spread(part, self.back, self.entry, 1)

    def home_wait(self, part):
        self.collect(part, self.back, self.entry, 1)

    def settle(self, part):
        for i in self.members(part):
            factor = self.decay(self.mine(i), 1 if self.reverse else 0)
            for half in range(2):
                first, second = self.ordered(i, half)
                edge = self.entry[self.slices(i), half * self.rows:(half + 1) * self.rows, :]
                edge = edge.reshape(self.d, self.d).astype(F32)
                inside = factor * edge + (second if self.reverse else first)
                keep = (self.c == 1) if self.reverse else (self.c == 0)
                self.gift2[i, half] = jnp.where(keep, inside, edge).astype(BF16)
                self.state[self.mine(i), half] = jnp.where(keep, edge, inside).astype(BF16)
        for i in self.members(part):
            remote(
                self.gift2.at[i], self.state.at[self.mine(i)],
                self.pair_sem.at[1], self.pair_sem.at[4 + i], seq=self.sibling,
            ).start()

    def settle_wait(self, i):
        arrival(self.state.at[self.theirs(i)], self.pair_sem.at[4 + i])

    def finish(self):
        pltpu.make_async_copy(self.gift, self.gift, self.pair_sem.at[0]).wait()
        pltpu.make_async_copy(self.gift2, self.gift2, self.pair_sem.at[1]).wait()


def kernel(n, heads, groups, *refs):
    inputs, (table_hbm, flags_hbm, w_hbm, goal_hbm), results = refs[:6], refs[6:10], refs[10:13]
    (q, qt, both_kv, weight, goal, dist, fall, pos, cum, lg, mine, count) = refs[13:25]
    k, v, kt, vt = (both_kv.at[i] for i in range(4))
    refs = (None,) * 3 + refs
    ahead, behind = refs[28:37], refs[37:46]
    (picked, gram, zall, gz, o_buf, ot_buf, g_buf, gt_buf, hk_buf, hv_buf) = refs[46:56]
    ahead_sems, behind_sems = refs[56:58], refs[58:60]
    (load_sem, cs, cr, ws, wr, gs, gr, zs, zr) = refs[60:69]
    (hq, hk, hv, g_rest, gt_rest, r_buf, rb_buf, q_turned, qt_turned, table, flags, out_sem) = refs[69:]
    me, z = lax.axis_index("seq"), lax.axis_index("head")
    up, down = lax.rem(z + 1, groups), lax.rem(z + groups - 1, groups)
    far = lax.rem(z + 2, groups)
    length, width = q.shape
    d = width // heads
    scale = d ** -0.5
    rows = width // n
    mine_rows = pl.ds(pl.multiple_of(me * rows, rows), rows)
    core = lax.rem(me, 2)
    mine_columns = pl.ds(pl.multiple_of(core * (width // 2), width // 2), width // 2)
    their_columns = pl.ds(pl.multiple_of((1 - core) * (width // 2), width // 2), width // 2)
    sources = (table_hbm, flags_hbm, w_hbm.at[mine_rows], inputs[0], inputs[3], w_hbm, goal_hbm)
    loads = [
        pltpu.make_async_copy(src, dst, load_sem.at[i])
        for i, (src, dst) in enumerate(zip(sources, (table, flags, picked.at[z], q, qt, weight, goal)))
    ]
    loads[0].start()
    loads[1].start()
    for sem, columns in ((7, their_columns), (8, mine_columns)):
        for i, j in enumerate((1, 2, 4, 5)):
            pltpu.make_async_copy(inputs[j].at[:, columns], both_kv.at[i, :, columns], load_sem.at[sem]).start()
        if sem == 7:
            loads[2].start()
    for load in loads[3:]:
        load.start()
    barrier_start(n, me, up, down)
    loads[0].wait()
    loads[1].wait()

    @pl.loop(0, heads)
    def _(h):
        fraction = jnp.full((1, length), table[h], jnp.int32).astype(F32) / (LEVELS - 1)
        rates = jnp.exp(math.log(1.0 / 32.0) + fraction * math.log(16.0 / (length * n)))
        lg[h] = jnp.log1p(-rates)

    reset_counts(flags, pos, cum)
    total = jnp.broadcast_to(jnp.sum(flags[...].astype(F32), axis=1, keepdims=True), (1, 128))
    mine[0] = total
    count[me] = total
    forward = Scan(me, n, heads, length, lg, count, ahead, ahead_sems, False)
    backward = Scan(me, n, heads, length, lg, count, behind, behind_sems, True)
    arrival(both_kv.at[:, :, their_columns], load_sem.at[7])

    def own_state(h, target, i):
        c = cols(h, d)
        w = scale * jnp.exp((length - 1.0 - pos[...]) * lg[h, :, 0:d] + (KEPT_LOG * total - cum[...]))
        kw = (k[:, c].astype(F32) * w).astype(BF16)
        ktw = (kt[:, c].astype(F32) * w).astype(BF16)
        both = dot(kw, jnp.concatenate([v[:, c], vt[:, c]], axis=1), ((0,), (0,)))
        target[i, 0] = both[:, :d].astype(BF16)
        target[i, 1] = (both[:, d:] + dot(ktw, v[:, c], ((0,), (0,)))).astype(BF16)

    def own_part(part, whose, target):
        pl.loop(2 * part, 2 * part + 2, unroll=2)(lambda i: own_state(whose(i), target, i))

    own_part(0, forward.theirs, forward.gift)
    own_part(1, forward.theirs, forward.gift)
    loads[2].wait()
    barrier_end(n)
    half = rows // 2
    low, high = slice(0, half), slice(half, rows)

    def w_send(slot, part, lane, to):
        remote(picked.at[slot, part], picked.at[slot, part], ws.at[0], wr.at[lane], head=to).start()

    w_send(z, low, 0, up)
    w_send(z, high, 1, down)
    w_send(z, high, 2, up)
    w_send(z, low, 2, down)
    remote(mine.at[0], count.at[me], cs.at[0], cr.at[0], seq=forward.sibling).start()

    forward.give(0)
    forward.give(1)
    arrival(both_kv.at[:, :, mine_columns], load_sem.at[8])
    own_part(0, forward.mine, forward.own)
    arrival(count.at[forward.sibling], cr.at[0])
    forward.give_wait(0)
    forward.combine(0)
    forward.out(0)
    own_part(1, forward.mine, forward.own)
    forward.give_wait(1)
    forward.combine(1)
    forward.out(1)
    loads[3].wait()
    loads[4].wait()

    def inner(h):
        c = cols(h, d)
        w = weights_of(h, d, lg, dist, fall)
        a = dot(q[:, c], k[:, c], ((1,), (1,)))
        at = dot(
            jnp.concatenate([qt[:, c], q[:, c]], axis=1), jnp.concatenate([k[:, c], kt[:, c]], axis=1), ((1,), (1,))
        )
        p = (a * w).astype(BF16)
        pt = (at * w).astype(BF16)
        both = dot(p, jnp.concatenate([v[:, c], vt[:, c]], axis=1))
        o_buf[:, c] = both[:, :d]
        ot_buf[:, c] = both[:, d:] + dot(pt, v[:, c])

    @pl.loop(1, n)
    def _(step):
        j = lax.rem(me + step, n)

        @pl.when(j != forward.sibling)
        def _():
            remote(mine.at[0], count.at[me], cs.at[0], cr.at[1], seq=j).start()

    decay_tables(flags, dist, fall)
    pl.loop(0, heads // 2)(inner)
    arrival(picked.at[down, low], wr.at[0])
    w_send(down, low, 2, up)
    arrival(picked.at[up, high], wr.at[1])
    w_send(up, high, 2, down)
    arrival(count.at[0:n - 2], cr.at[1])
    forward.out_wait(0)
    forward.scan(0)
    forward.home(0)
    forward.out_wait(1)
    forward.scan(1)
    forward.home(1)
    pl.loop(heads // 2, heads)(inner)
    tile = 256

    def gram_tile(i):
        c = slice(i * tile, (i + 1) * tile)
        part = dot(picked[...].reshape(groups * rows, weight.shape[1]), weight[c, :], ((1,), (1,)))
        gram[:, mine_rows, c] = part.astype(BF16).reshape(groups, rows, tile)

    gathers = [GramGather(me, gram, part, 2, gs, gr) for part in range(2)]

    def head_of(i):
        part, place = i // 4, i % 4
        return forward.mine(2 * part + place) if place < 2 else forward.theirs(2 * part + place - 2)

    def z_send(i):
        c = cols(head_of(i), d)
        remote(zall.at[z, :, c], zall.at[z, :, c], zs.at[0], zr.at[i], head=up).start()
        remote(zall.at[z, :, c], zall.at[z, :, c], zs.at[0], zr.at[i], head=down).start()

    def output(i):
        h = head_of(i)
        c = cols(h, d)
        dq = jnp.exp((pos[...] + 1.0) * lg[h, :, 0:d] + cum[...])
        s, st = forward.state[h, 0], forward.state[h, 1]
        both = dot(q[:, c], jnp.concatenate([s, st], axis=1))
        o = o_buf[:, c] + dq * both[:, :d]
        ot = ot_buf[:, c] + dq * (both[:, d:] + dot(qt[:, c], s))
        o_buf[:, c] = o
        ot_buf[:, c] = ot
        r = lax.rsqrt(jnp.mean(o * o, axis=1, keepdims=True) + EPS)
        m = jnp.mean(o * ot, axis=1, keepdims=True)
        zall[z, 0:length, c] = (o * r).astype(BF16)
        zall[z, length:, c] = (r * ot - o * (r * r * r * m)).astype(BF16)

        z_send(i)

    forward.home_wait(0)
    forward.settle(0)
    output(0)
    output(1)
    for i in range(2):
        forward.settle_wait(i)
        output(2 + i)
    arrival(picked.at[0:2], wr.at[2])
    loads[5].wait()
    for part in range(2):
        gram_tile(2 * part)
        gram_tile(2 * part + 1)
        gathers[part].round(0)
    forward.home_wait(1)
    forward.settle(1)
    output(4)
    output(5)
    for i in range(2):
        forward.settle_wait(2 + i)
        output(6 + i)
    loads[6].wait()

    def goal_tile(i):
        c = slice(i * tile, (i + 1) * tile)
        gz[0:length, c] = -dot(goal[...], weight[c, :], ((1,), (1,)))

    groups_of = (0, 0, 0, 0, 1, 1, 2, 2)

    def near(i):
        arrival(zall.at[0:2, :, cols(head_of(i), d)], zr.at[i])

    def forward_on(i):
        c = cols(head_of(i), d)
        lane = heads + groups_of[i]
        piece = zall.at[down, 0:length, c]
        remote(piece, piece, zs.at[0], zr.at[lane], head=up).start()
        piece = zall.at[up, length:, c]
        remote(piece, piece, zs.at[0], zr.at[lane], head=down).start()

    def relay(i):
        near(i)
        forward_on(i)

    def relay_early(i):
        near(i)
        pl.when(core == 0)(lambda: forward_on(i))

    def forward_late():
        @pl.when(core == 1)
        def _():
            forward_on(6)
            forward_on(7)

    def distant(first, number):
        arrival(zall.at[far, :, 0:number * d], zr.at[heads + groups_of[first]])

    def add(pairs, source):
        parts = [pl.ds(pl.multiple_of(head_of(2 * p) * d, 2 * d), 2 * d) for p in pairs]

        for i in range(width // tile):
            c = slice(i * tile, (i + 1) * tile)
            for r in (slice(0, length), slice(length, 2 * length)):
                gz[r, c] = sum((dot(zall[source, r, p], gram[source, p, c]) for p in parts), gz[r, c])

    def add_whole(first, last, *sources, fresh=False):
        for i in range(first, last):
            c = slice(i * tile, (i + 1) * tile)
            for r in (slice(0, length), slice(length, 2 * length)):
                start = 0.0 if fresh and r.start else gz[r, c]
                gz[r, c] = sum((dot(zall[g, r, :], gram[g, :, c]) for g in sources), start)

    def prepare(h):
        c = cols(h, d)
        dq = jnp.exp((pos[...] + 1.0) * lg[h, :, 0:d] + cum[...])
        o, ot = o_buf[:, c], ot_buf[:, c]
        r = lax.rsqrt(jnp.mean(o * o, axis=1, keepdims=True) + EPS)
        m = r * r * jnp.mean(o * ot, axis=1, keepdims=True)
        zf = o * r
        o_buf[:, c] = zf
        ot_buf[:, c] = r * ot - zf * m
        r_buf[:, c] = jnp.broadcast_to(r, o.shape)
        rb_buf[:, c] = jnp.broadcast_to(m, o.shape)
        q_turned[c, :] = (q[:, c].astype(F32) * dq).T.astype(BF16)
        qt_turned[c, :] = (qt[:, c].astype(F32) * dq).T.astype(BF16)

    goal_tile(0)
    gathers[0].round(1)
    relay(0)
    gathers[1].round(1)
    goal_tile(1)
    relay(1)
    gathers[0].round(2)
    goal_tile(2)
    gathers[1].round(2)
    relay(2)
    gathers[0].round(3)
    goal_tile(3)
    gathers[1].round(3)
    relay(3)
    gathers[0].round(4)
    relay(4)
    pl.loop(0, 4)(prepare)
    gathers[1].round(4)
    relay(5)
    gathers[0].round(5)
    relay_early(6)
    pl.loop(4, 8)(prepare)
    gathers[1].round(5)
    gathers[0].round(6)
    add_whole(0, 2, z, fresh=True)
    relay_early(7)
    gathers[1].round(6)
    add_whole(2, 4, z, fresh=True)
    add_whole(0, 2, up, down)
    forward_late()
    add_whole(2, 4, up, down)
    distant(0, 4)
    add((0, 1), far)
    distant(4, 2)
    add((2,), far)
    distant(6, 2)
    add((3,), far)

    def norm_back(h, target, i):
        c = cols(h, d)
        zf, ztf = o_buf[:, c], ot_buf[:, c]
        gzh, gzt = gz[0:length, c], gz[length:, c]
        a = jnp.mean(zf * gzh, axis=1, keepdims=True)
        at = jnp.mean(ztf * gzh + zf * gzt, axis=1, keepdims=True)
        r = r_buf[:, c]
        g = r * (gzh - zf * a)
        gt = r * (gzt - ztf * a - zf * at) - rb_buf[:, c] * g
        for value, top, rest in ((g, g_buf, g_rest), (gt, gt_buf, gt_rest)):
            high = value.astype(BF16)
            top[:, c] = high
            rest[:, c] = (value - high.astype(F32)).astype(BF16)
        both = dot(q_turned[c, :], jnp.concatenate([g, gt], axis=1).astype(BF16))
        target[i, 0] = both[:, :d].astype(BF16)
        target[i, 1] = (both[:, d:] + dot(qt_turned[c, :], g.astype(BF16))).astype(BF16)

    def norm_part(part, whose, target):
        pl.loop(2 * part, 2 * part + 2, unroll=2)(lambda i: norm_back(whose(i), target, i))

    norm_part(0, backward.theirs, backward.gift)
    backward.give(0)
    norm_part(1, backward.theirs, backward.gift)
    backward.give(1)
    norm_part(0, backward.mine, backward.own)
    backward.give_wait(0)
    backward.combine(0)
    backward.out(0)
    norm_part(1, backward.mine, backward.own)
    backward.give_wait(1)
    backward.combine(1)
    backward.out(1)

    def inner_back(h):
        c = cols(h, d)
        w = weights_of(h, d, lg, dist, fall)
        dq = jnp.exp((pos[...] + 1.0) * lg[h, :, 0:d] + cum[...])
        qh, kh, vh, qth, kth, vth, g, gt = (x[:, c] for x in (q, k, v, qt, kt, vt, g_buf, gt_buf))
        a = dot(qh, kh, ((1,), (1,)))
        at = dot(jnp.concatenate([qth, qh], axis=1), jnp.concatenate([kh, kth], axis=1), ((1,), (1,)))
        p = (a * w).astype(BF16)
        pt = (at * w).astype(BF16)
        g_lo, gt_lo = g_rest[:, c], gt_rest[:, c]
        b = dot(jnp.concatenate([g, g_lo], axis=1), jnp.concatenate([vh, vh], axis=1), ((1,), (1,)))
        b = (b * w).astype(BF16)
        bt = dot(
            jnp.concatenate([gt, gt_lo, g, g_lo], axis=1), jnp.concatenate([vh, vh, vth, vth], axis=1), ((1,), (1,))
        )
        bt = (bt * w).astype(BF16)
        s, st = forward.state[h, 0], forward.state[h, 1]
        outer = dot(jnp.concatenate([gt, g], axis=1), jnp.concatenate([s, st], axis=1), ((1,), (1,)))
        hq[:, c] = (
            dot(jnp.concatenate([bt, b], axis=1), jnp.concatenate([kh, kth], axis=0)) + dq * outer
        ).astype(BF16)
        hk_buf[:, c] = dot(jnp.concatenate([bt, b], axis=0), jnp.concatenate([qh, qth], axis=0), ((0,), (0,)))
        hv_buf[:, c] = dot(
            jnp.concatenate([pt, p, pt, p], axis=0), jnp.concatenate([g, gt, g_lo, gt_lo], axis=0), ((0,), (0,))
        )

    pl.loop(0, 4)(inner_back)
    forward.finish()
    for gather in gathers:
        gather.finish()

    pltpu.make_async_copy(count.at[0:n - 1], count.at[0:n - 1], cs.at[0]).wait()
    pltpu.make_async_copy(picked.at[0:3], picked.at[0:3], ws.at[0]).wait()
    pltpu.make_async_copy(zall.at[0:3], zall.at[0:3], zs.at[0]).wait()

    backward.out_wait(0)
    backward.scan(0)
    backward.home(0)
    backward.out_wait(1)
    backward.scan(1)
    backward.home(1)
    pl.loop(4, heads)(inner_back)
    pltpu.make_async_copy(hq, results[0], out_sem.at[0]).start()

    def last(i):
        h = lax.rem(backward.mine(i), heads)
        c = cols(h, d)
        w = scale * jnp.exp((length - 1.0 - pos[...]) * lg[h, :, 0:d] + (KEPT_LOG * total - cum[...]))
        s, st = backward.state[h, 0], backward.state[h, 1]
        ks = dot(jnp.concatenate([v[:, c], vt[:, c]], axis=1), jnp.concatenate([st, s], axis=1), ((1,), (1,)))
        vs = dot(jnp.concatenate([k[:, c], kt[:, c]], axis=1), jnp.concatenate([st, s], axis=0))
        hk[:, c] = (hk_buf[:, c] + w * ks).astype(BF16)
        hv[:, c] = (hv_buf[:, c] + w * vs).astype(BF16)

    def emit(kind, h):
        c = cols(h, d)
        pltpu.make_async_copy((hk, hv)[kind].at[:, c], results[1 + kind].at[:, c], out_sem.at[1 + kind]).start()

    def finish(i):
        last(i)
        emit(0, lax.rem(backward.mine(i), heads))
        emit(1, lax.rem(backward.mine(i), heads))

    backward.home_wait(0)
    backward.settle(0)
    finish(0)
    finish(1)
    backward.home_wait(1)
    backward.settle(1)
    finish(2)
    finish(3)
    for i in range(heads // 2):
        backward.settle_wait(i)
        finish(heads // 2 + i)
    backward.finish()
    for kind, buffer in enumerate((hq, hk, hv)):
        pltpu.make_async_copy(buffer, results[kind], out_sem.at[kind]).wait()


def store_kernel(*refs):
    copies = [pltpu.make_async_copy(refs[i], refs[3 + i], refs[6].at[i]) for i in range(3)]
    for copy in copies:
        copy.start()
    for copy in copies:
        copy.wait()


def on_device(n, groups, probe, source, content, probe_t, source_t, content_t, table, flags, weight, goal):
    length, width = probe.shape
    heads = table.shape[0]
    d = width // heads
    flags = flags.reshape(1, length)
    vmem, hbm = (pl.BlockSpec(memory_space=m) for m in (pltpu.VMEM, pltpu.HBM))
    pair = pltpu.VMEM((heads // 2, 2, d, d), BF16)
    slots = pltpu.VMEM((n // 2 * Scan.PARTS, 2 * heads * d // n // Scan.PARTS, d), BF16)
    scan = [pair, pair, pair, slots, slots, slots, slots, pltpu.VMEM((heads, 2, d, d), BF16), pair]
    narrow, wide = pltpu.VMEM((length, width), BF16), pltpu.VMEM((length, width), F32)
    rows = width // n
    dma = pltpu.SemaphoreType.DMA
    out = jax.ShapeDtypeStruct((length, width), BF16)
    results = pl.pallas_call(
        functools.partial(kernel, n, heads, groups),
        out_shape=(out, out, out),
        in_specs=[hbm] * 10,
        out_specs=[pl.BlockSpec(memory_space=pl.ANY)] * 3,
        scratch_shapes=[
            narrow, narrow, pltpu.VMEM((4, length, width), BF16), pltpu.VMEM(weight.shape, BF16), pltpu.VMEM(goal.shape, BF16),
            pltpu.VMEM((length, length), F32), pltpu.VMEM((length, length), F32),
            pltpu.VMEM((length, d), F32), pltpu.VMEM((length, d), F32),
            pltpu.VMEM((heads, 1, length), F32), pltpu.VMEM((1, 1, d), F32), pltpu.VMEM((n, 1, d), F32),
            *scan, *scan,
            pltpu.VMEM((groups, rows, weight.shape[1]), BF16),
            pltpu.VMEM((groups, width, width), BF16),
            pltpu.VMEM((groups, 2 * length, width), BF16),
            pltpu.VMEM((2 * length, width), F32),
            wide, wide, narrow, narrow, wide, wide,
            *[dma((4 + heads // 2,)), dma((4 * Scan.PARTS,))] * 2,
            dma((9,)), dma((1,)), dma((2,)), dma((1,)), dma((3,)), dma((2,)), dma((26,)), dma((1,)), dma((heads + 3,)),
            narrow, narrow, narrow, narrow, narrow, wide, wide,
            pltpu.VMEM((width, length), BF16), pltpu.VMEM((width, length), BF16), pltpu.SMEM(table.shape, jnp.int32), pltpu.VMEM(flags.shape, jnp.int32),
            dma((3,)),
        ],
        compiler_params=pltpu.CompilerParams(collective_id=0, has_side_effects=True, vmem_limit_bytes=52 << 20),
        name="retention_hvp",
    )(probe, source, content, probe_t, source_t, content_t, *(pltpu.with_memory_space_constraint(x, pltpu.HBM) for x in (table, flags)), weight, goal)
    return pl.pallas_call(
        store_kernel,
        out_shape=(out, out, out),
        in_specs=[vmem] * 3,
        out_specs=[hbm] * 3,
        scratch_shapes=[dma((3,))],
        compiler_params=pltpu.CompilerParams(vmem_limit_bytes=4 << 20),
        name="store",
    )(*results)


def solution(mesh):
    n, groups = mesh.shape["seq"], mesh.shape["head"]
    both = P("seq", "head")
    return jax.shard_map(
        functools.partial(on_device, n, groups),
        mesh=mesh,
        in_specs=(both,) * 6 + (P("head"), P("seq"), P("head", None), P("seq", None)),
        out_specs=(both,) * 3,
        check_vma=False,
    )
```

```python
import functools
import math

import jax
import jax.numpy as jnp
from jax import lax
from jax.experimental import pallas as pl
from jax.experimental.pallas import tpu as pltpu
from jax.sharding import PartitionSpec as P

LEVELS = 8
KEPT_LOG = math.log(0.7)
EPS = 1e-06
F32 = jnp.float32
BF16 = jnp.bfloat16
MESH = pl.DeviceIdType.MESH
FAR = 1e9
UNROLL = 2


def dot(a, b, dims=((1,), (0,))):
    return lax.dot_general(a, b, (dims, ((), ())), preferred_element_type=F32)


def cols(h, d):
    return pl.ds(pl.multiple_of(h * d, d), d)


def reset_counts(flags_ref, pos, cum):
    t = pos.shape[0]
    row = lax.broadcasted_iota(jnp.int32, (t, t), 0)
    col = lax.broadcasted_iota(jnp.int32, (t, t), 1)
    flags = jnp.broadcast_to(flags_ref[...].astype(F32), (t, t))
    cum_col = jnp.sum(jnp.where(col <= row, flags, 0.0), axis=1, keepdims=True)
    pos[...] = lax.broadcasted_iota(jnp.int32, pos.shape, 0).astype(F32)
    cum[...] = KEPT_LOG * jnp.broadcast_to(cum_col, cum.shape)


def decay_tables(flags_ref, dist, fall):
    t = dist.shape[0]
    row = lax.broadcasted_iota(jnp.int32, (t, t), 0)
    col = lax.broadcasted_iota(jnp.int32, (t, t), 1)
    flags = jnp.broadcast_to(flags_ref[...].astype(F32), (t, t))
    cum_col = jnp.sum(jnp.where(col <= row, flags, 0.0), axis=1, keepdims=True)
    flag_col = jnp.sum(jnp.where(col == row, flags, 0.0), axis=1, keepdims=True)
    cum_row = jnp.sum(jnp.where(row <= col, flag_col, 0.0), axis=0, keepdims=True)
    dist[...] = jnp.where(row >= col, (row - col).astype(F32), FAR)
    fall[...] = KEPT_LOG * (cum_col - cum_row)


def barrier_start(n, me, up, down):
    barrier = pltpu.get_barrier_semaphore()
    for z in (up, down):
        pl.semaphore_signal(barrier, inc=1, device_id={"head": z}, device_id_type=MESH)

    @pl.loop(1, n)
    def _(step):
        pl.semaphore_signal(barrier, inc=1, device_id={"seq": lax.rem(me + step, n)}, device_id_type=MESH)


def barrier_end(n):
    pl.semaphore_wait(pltpu.get_barrier_semaphore(), n + 1)


def weights_of(h, d, lg_ref, dist, fall):
    return jnp.exp(dist[...] * lg_ref[h] + fall[...]) * (d ** -0.5)


def remote(src, dst, send_sem, recv_sem, **where):
    return pltpu.make_async_remote_copy(
        src_ref=src, dst_ref=dst, send_sem=send_sem, recv_sem=recv_sem, device_id=where, device_id_type=MESH
    )


def arrival(dst, recv_sem):
    pltpu.make_async_copy(dst, dst, recv_sem).wait()


class GramGather:
    def __init__(self, me, full, part, parts, send_sem, recv_sem):
        c = lax.rem(me, 2)
        x, y = lax.rem(me // 2, 4), me // 8
        self.me, self.c, self.f, self.s = me, c, x + c * (y - x), y + c * (x - y)
        columns = full.shape[2] // parts
        self.full = full.at[:, :, part * columns:(part + 1) * columns]
        self.send_sem, self.recv_sem, self.base = send_sem.at[part], recv_sem, 13 * part
        self.rows = full.shape[1] // 32

    def at(self, df, s_off, absolute=False):
        f = df if absolute else lax.rem(self.f + df + 4, 4)
        s = lax.rem(self.s + s_off + 4, 4)
        return (f * (1 + 3 * self.c) + s * (4 - 3 * self.c)) * 2 + self.c

    def view(self, piece, half=None):
        rows = pl.ds(pl.multiple_of(piece * self.rows, self.rows), self.rows)
        if half is None:
            return self.full.at[:, rows, :]
        return self.full.at[2 * half:2 * half + 2, rows, :]

    def send(self, piece, to, lane, half=None):
        view = self.view(piece, half)
        remote(view, view, self.send_sem, self.recv_sem.at[self.base + lane], seq=to).start()

    def wait(self, piece, lane):
        arrival(self.view(piece), self.recv_sem.at[self.base + lane])

    def spread(self, piece, df):
        self.send(piece, self.at(0, 1), self.lane(-1, df))
        self.send(piece, self.at(0, -1), self.lane(1, df))
        self.sideways(piece)

    def sideways(self, piece):
        self.send(piece, self.me + 1 - 2 * self.c, 12)

    def lane(self, step, df):
        return 3 + (4 if step == 1 else 0) + df % 4

    def pass_on(self, step, df, half):
        piece = self.at(df, step)
        self.wait(piece, self.lane(step, df))
        self.send(piece, self.at(0, -step), 11, half)
        self.sideways(piece)

    def round(self, k):
        if k == 0:
            self.send(self.me, self.at(1, 0), 0)
            self.send(self.me, self.at(-1, 0), 1)
            self.spread(self.me, 0)
        elif k == 1:
            for step, half in ((-1, 0), (1, 1)):
                self.wait(self.at(step, 0), half)
                self.send(self.at(step, 0), self.at(-step, 0), 2, half)
            for step in (-1, 1):
                self.spread(self.at(step, 0), step)
            for step, half in ((-1, 0), (1, 1)):
                self.pass_on(step, 0, half)
        elif k == 2:
            self.wait(self.at(2, 0), 2)
            self.spread(self.at(2, 0), 2)
        elif k == 3:
            for df in (-1, 1):
                for step, half in ((-1, 0), (1, 1)):
                    self.pass_on(step, df, half)
        elif k == 4:
            for step, half in ((-1, 0), (1, 1)):
                self.pass_on(step, 2, half)
        elif k == 5:
            four = self.full.at[:, 0:4 * self.rows, :]
            arrival(four, self.recv_sem.at[self.base + 11])
            for df in range(4):
                self.sideways(self.at(df, 2))
        else:
            arrival(self.full.at[:, 0:16 * self.rows, :], self.recv_sem.at[self.base + 12])

    def finish(self):
        sent = self.full.at[:, 0:31 * self.rows, :]
        pltpu.make_async_copy(sent, sent, self.send_sem).wait()


class Scan:
    PARTS = 2

    def __init__(self, me, n, heads, length, lg, count, totals, buffers, sems, reverse):
        self.own, self.gift, self.peer, self.tot, self.recv, self.back, self.entry, self.state, self.gift2 = buffers
        self.pair_sem, self.hop_sem = sems
        self.c, self.chip, self.chips = lax.rem(me, 2), me // 2, n // 2
        self.sibling = me + 1 - 2 * self.c
        self.half = heads // 2
        self.step = self.half // self.PARTS
        self.length, self.lg, self.count, self.totals, self.reverse = length, lg, count, totals, reverse
        self.per = self.chips // self.step
        self.rows = self.tot.shape[1] // 2
        self.d = self.tot.shape[2]

    def mine(self, i):
        return self.half * self.c + i

    def theirs(self, i):
        return self.half * (1 - self.c) + i

    def members(self, part):
        return range(part * self.step, (part + 1) * self.step)

    def give(self, part):
        some = slice(part * self.step, (part + 1) * self.step)
        remote(
            self.gift.at[some], self.peer.at[some], self.pair_sem.at[0], self.pair_sem.at[2 + part], seq=self.sibling
        ).start()

    def give_wait(self, part):
        arrival(self.peer.at[part * self.step:(part + 1) * self.step], self.pair_sem.at[2 + part])

    def decay(self, h, core):
        return jnp.exp(float(self.length) * self.lg[h, :, 0:self.d] + KEPT_LOG * self.count[core])

    def ordered(self, i, half):
        mine, peer = self.own[i, half].astype(F32), self.peer[i, half].astype(F32)
        return jnp.where(self.c == 0, mine, peer), jnp.where(self.c == 0, peer, mine)

    def slices(self, i):
        first = (i // self.step) * self.chips + (i % self.step) * self.per
        return slice(first, first + self.per)

    def combine(self, part):
        for i in self.members(part):
            factor = self.decay(self.mine(i), 0 if self.reverse else 1)
            for half in range(2):
                first, second = self.ordered(i, half)
                total = first + factor * second if self.reverse else first * factor + second
                self.tot[self.slices(i), half * self.rows:(half + 1) * self.rows, :] = (
                    total.astype(BF16).reshape(self.per, self.rows, self.d)
                )

    def others(self):
        x, y = lax.rem(self.chip, 4), self.chip // 4
        for dy, dx in sorted(
            ((a, b) for a in range(4) for b in range(4) if a or b), key=lambda t: -min(t[0], 4 - t[0]) - min(t[1], 4 - t[1])
        ):
            yield lax.rem(y + dy, 4) * 4 + lax.rem(x + dx, 4)

    def spread(self, part, src, dst, hop):
        base = part * self.chips
        send_sem, recv_sem = self.hop_sem.at[4 * part + 2 * hop], self.hop_sem.at[4 * part + 2 * hop + 1]
        for p in self.others():
            remote(src.at[base + p], dst.at[base + self.chip], send_sem, recv_sem, seq=2 * p + self.c).start()

    def collect(self, part, src, dst, hop):
        sent, got = src.at[0:self.chips - 1], dst.at[0:self.chips - 1]
        pltpu.make_async_copy(sent, sent, self.hop_sem.at[4 * part + 2 * hop]).wait()
        arrival(got, self.hop_sem.at[4 * part + 2 * hop + 1])

    def out(self, part):
        self.spread(part, self.tot, self.recv, 0)

    def out_wait(self, part):
        self.collect(part, self.tot, self.recv, 0)

    def scan(self, part):
        base = part * self.chips
        self.recv[base + self.chip] = self.tot[base + self.chip]
        lg = self.lg[self.mine(part * self.step + self.chip // self.per), :, 0:self.d]

        def step(i, run):
            p = self.chips - 1 - i if self.reverse else i
            self.back[base + p] = run.astype(BF16)
            factor = jnp.exp(2.0 * self.length * lg + KEPT_LOG * self.totals[p])
            return run * factor + self.recv[base + p].astype(F32)

        lax.fori_loop(0, self.chips, step, jnp.zeros(self.recv.shape[1:], F32), unroll=self.chips)
        self.entry[base + self.chip] = self.back[base + self.chip]

    def home(self, part):
        self.spread(part, self.back, self.entry, 1)

    def home_wait(self, part):
        self.collect(part, self.back, self.entry, 1)

    def settle(self, part):
        for i in self.members(part):
            factor = self.decay(self.mine(i), 1 if self.reverse else 0)
            for half in range(2):
                first, second = self.ordered(i, half)
                edge = self.entry[self.slices(i), half * self.rows:(half + 1) * self.rows, :]
                edge = edge.reshape(self.d, self.d).astype(F32)
                inside = factor * edge + (second if self.reverse else first)
                keep = (self.c == 1) if self.reverse else (self.c == 0)
                self.gift2[i, half] = jnp.where(keep, inside, edge).astype(BF16)
                self.state[self.mine(i), half] = jnp.where(keep, edge, inside).astype(BF16)
        for i in self.members(part):
            remote(
                self.gift2.at[i], self.state.at[self.mine(i)],
                self.pair_sem.at[1], self.pair_sem.at[4 + i], seq=self.sibling,
            ).start()

    def settle_wait(self, i):
        arrival(self.state.at[self.theirs(i)], self.pair_sem.at[4 + i])

    def finish(self):
        pltpu.make_async_copy(self.gift, self.gift, self.pair_sem.at[0]).wait()
        pltpu.make_async_copy(self.gift2, self.gift2, self.pair_sem.at[1]).wait()


def kernel(n, heads, groups, *refs):
    inputs, (table_hbm, flags_hbm, w_hbm, goal_hbm), results = refs[:6], refs[6:10], refs[10:13]
    (q, qt, both_kv, weight, goal, dist, fall, pos, cum, lg, mine, count, totals) = refs[13:26]
    k, v, kt, vt = (both_kv.at[i] for i in range(4))
    refs = (None,) * 2 + refs
    ahead, behind = refs[28:37], refs[37:46]
    (picked, gram, zall, gz, o_buf, ot_buf, g_buf, gt_buf, hk_buf, hv_buf) = refs[46:56]
    ahead_sems, behind_sems = refs[56:58], refs[58:60]
    (load_sem, cs, cr, ws, wr, gs, gr, zs, zr) = refs[60:69]
    (hq, hk, hv, g_rest, gt_rest, r_buf, rb_buf, q_turned, qt_turned, table, flags, out_sem) = refs[69:]
    me, z = lax.axis_index("seq"), lax.axis_index("head")
    up, down = lax.rem(z + 1, groups), lax.rem(z + groups - 1, groups)
    far = lax.rem(z + 2, groups)
    length, width = q.shape
    d = width // heads
    scale = d ** -0.5
    rows = width // n
    mine_rows = pl.ds(pl.multiple_of(me * rows, rows), rows)
    core = lax.rem(me, 2)
    mine_columns = pl.ds(pl.multiple_of(core * (width // 2), width // 2), width // 2)
    their_columns = pl.ds(pl.multiple_of((1 - core) * (width // 2), width // 2), width // 2)
    sources = (table_hbm, flags_hbm, w_hbm.at[mine_rows], inputs[0], inputs[3], w_hbm, goal_hbm)
    loads = [
        pltpu.make_async_copy(src, dst, load_sem.at[i])
        for i, (src, dst) in enumerate(zip(sources, (table, flags, picked.at[z], q, qt, weight, goal)))
    ]
    loads[0].start()
    loads[1].start()
    for sem, columns in ((7, their_columns), (8, mine_columns)):
        for i, j in enumerate((1, 2, 4, 5)):
            pltpu.make_async_copy(inputs[j].at[:, columns], both_kv.at[i, :, columns], load_sem.at[sem]).start()
        if sem == 7:
            loads[2].start()
    for load in loads[3:]:
        load.start()
    barrier_start(n, me, up, down)
    loads[0].wait()
    loads[1].wait()

    @pl.loop(0, heads)
    def _(h):
        fraction = jnp.full((1, length), table[h], jnp.int32).astype(F32) / (LEVELS - 1)
        rates = jnp.exp(math.log(1.0 / 32.0) + fraction * math.log(16.0 / (length * n)))
        lg[h] = jnp.log1p(-rates)

    reset_counts(flags, pos, cum)
    total = jnp.broadcast_to(jnp.sum(flags[...].astype(F32), axis=1, keepdims=True), (1, 128))
    mine[0] = total
    count[core] = total
    forward = Scan(me, n, heads, length, lg, count, totals, ahead, ahead_sems, False)
    backward = Scan(me, n, heads, length, lg, count, totals, behind, behind_sems, True)
    arrival(both_kv.at[:, :, their_columns], load_sem.at[7])

    def own_state(h, target, i):
        c = cols(h, d)
        w = scale * jnp.exp((length - 1.0 - pos[...]) * lg[h, :, 0:d] + (KEPT_LOG * total - cum[...]))
        kw = (k[:, c].astype(F32) * w).astype(BF16)
        ktw = (kt[:, c].astype(F32) * w).astype(BF16)
        both = dot(kw, jnp.concatenate([v[:, c], vt[:, c]], axis=1), ((0,), (0,)))
        target[i, 0] = both[:, :d].astype(BF16)
        target[i, 1] = (both[:, d:] + dot(ktw, v[:, c], ((0,), (0,)))).astype(BF16)

    def own_part(part, whose, target):
        pl.loop(2 * part, 2 * part + 2, unroll=2)(lambda i: own_state(whose(i), target, i))

    own_part(0, forward.theirs, forward.gift)
    own_part(1, forward.theirs, forward.gift)
    loads[2].wait()
    barrier_end(n)
    half = rows // 2
    low, high = slice(0, half), slice(half, rows)

    def w_send(slot, part, lane, to):
        remote(picked.at[slot, part], picked.at[slot, part], ws.at[0], wr.at[lane], head=to).start()

    w_send(z, low, 0, up)
    w_send(z, high, 1, down)
    w_send(z, high, 2, up)
    w_send(z, low, 2, down)
    remote(mine.at[0], count.at[core], cs.at[0], cr.at[0], seq=forward.sibling).start()

    forward.give(0)
    forward.give(1)
    arrival(both_kv.at[:, :, mine_columns], load_sem.at[8])
    own_part(0, forward.mine, forward.own)
    arrival(count.at[1 - core], cr.at[0])
    totals[forward.chip] = count[0] + count[1]
    forward.give_wait(0)
    forward.combine(0)
    for p in forward.others():
        remote(totals.at[forward.chip], totals.at[forward.chip], cs.at[0], cr.at[1], seq=2 * p + core).start()
    forward.out(0)
    own_part(1, forward.mine, forward.own)
    forward.give_wait(1)
    forward.combine(1)
    forward.out(1)
    loads[3].wait()
    loads[4].wait()

    def inner(h):
        c = cols(h, d)
        w = weights_of(h, d, lg, dist, fall)
        a = dot(q[:, c], k[:, c], ((1,), (1,)))
        at = dot(
            jnp.concatenate([qt[:, c], q[:, c]], axis=1), jnp.concatenate([k[:, c], kt[:, c]], axis=1), ((1,), (1,))
        )
        p = (a * w).astype(BF16)
        pt = (at * w).astype(BF16)
        both = dot(p, jnp.concatenate([v[:, c], vt[:, c]], axis=1))
        o_buf[:, c] = both[:, :d]
        ot_buf[:, c] = both[:, d:] + dot(pt, v[:, c])

    decay_tables(flags, dist, fall)
    pl.loop(0, heads // 2, unroll=2)(inner)
    arrival(picked.at[down, low], wr.at[0])
    w_send(down, low, 2, up)
    arrival(picked.at[up, high], wr.at[1])
    w_send(up, high, 2, down)
    arrival(totals.at[0:n // 2 - 1], cr.at[1])
    forward.out_wait(0)
    forward.scan(0)
    forward.home(0)
    forward.out_wait(1)
    forward.scan(1)
    forward.home(1)
    pl.loop(heads // 2, heads, unroll=2)(inner)
    tile = 256

    def gram_tile(i):
        c = slice(i * tile, (i + 1) * tile)
        part = dot(picked[...].reshape(groups * rows, weight.shape[1]), weight[c, :], ((1,), (1,)))
        gram[:, mine_rows, c] = part.astype(BF16).reshape(groups, rows, tile)

    gathers = [GramGather(me, gram, part, 2, gs, gr) for part in range(2)]

    def head_of(i):
        part, place = i // 4, i % 4
        return forward.mine(2 * part + place) if place < 2 else forward.theirs(2 * part + place - 2)

    def z_send(i):
        c = cols(head_of(i), d)
        remote(zall.at[z, :, c], zall.at[z, :, c], zs.at[0], zr.at[i], head=up).start()
        remote(zall.at[z, :, c], zall.at[z, :, c], zs.at[0], zr.at[i], head=down).start()

    def output(i):
        h = head_of(i)
        c = cols(h, d)
        dq = jnp.exp((pos[...] + 1.0) * lg[h, :, 0:d] + cum[...])
        s, st = forward.state[h, 0], forward.state[h, 1]
        both = dot(q[:, c], jnp.concatenate([s, st], axis=1))
        o = o_buf[:, c] + dq * both[:, :d]
        ot = ot_buf[:, c] + dq * (both[:, d:] + dot(qt[:, c], s))
        o_buf[:, c] = o
        ot_buf[:, c] = ot
        r = lax.rsqrt(jnp.mean(o * o, axis=1, keepdims=True) + EPS)
        m = jnp.mean(o * ot, axis=1, keepdims=True)
        zall[z, 0:length, c] = (o * r).astype(BF16)
        zall[z, length:, c] = (r * ot - o * (r * r * r * m)).astype(BF16)

        z_send(i)

    forward.home_wait(0)
    forward.settle(0)
    output(0)
    output(1)
    for i in range(2):
        forward.settle_wait(i)
        output(2 + i)
    arrival(picked.at[0:2], wr.at[2])
    loads[5].wait()
    for part in range(2):
        gram_tile(2 * part)
        gram_tile(2 * part + 1)
        gathers[part].round(0)
    forward.home_wait(1)
    forward.settle(1)
    output(4)
    output(5)
    for i in range(2):
        forward.settle_wait(2 + i)
        output(6 + i)
    loads[6].wait()

    def goal_tile(i):
        c = slice(i * tile, (i + 1) * tile)
        gz[0:length, c] = -dot(goal[...], weight[c, :], ((1,), (1,)))

    groups_of = (0, 0, 0, 0, 1, 1, 2, 2)

    def near(i):
        arrival(zall.at[0:2, :, cols(head_of(i), d)], zr.at[i])

    def forward_on(i):
        c = cols(head_of(i), d)
        lane = heads + groups_of[i]
        piece = zall.at[down, 0:length, c]
        remote(piece, piece, zs.at[0], zr.at[lane], head=up).start()
        piece = zall.at[up, length:, c]
        remote(piece, piece, zs.at[0], zr.at[lane], head=down).start()

    def relay(i):
        near(i)
        forward_on(i)

    def relay_early(i):
        near(i)
        pl.when(core == 0)(lambda: forward_on(i))

    def forward_late():
        @pl.when(core == 1)
        def _():
            forward_on(6)
            forward_on(7)

    def distant(first, number):
        arrival(zall.at[far, :, 0:number * d], zr.at[heads + groups_of[first]])

    def add(pairs, source):
        parts = [pl.ds(pl.multiple_of(head_of(2 * p) * d, 2 * d), 2 * d) for p in pairs]

        for i in range(width // tile):
            c = slice(i * tile, (i + 1) * tile)
            for r in (slice(0, length), slice(length, 2 * length)):
                gz[r, c] = sum((dot(zall[source, r, p], gram[source, p, c]) for p in parts), gz[r, c])

    def add_whole(first, last, *sources, fresh=False):
        for i in range(first, last):
            c = slice(i * tile, (i + 1) * tile)
            for r in (slice(0, length), slice(length, 2 * length)):
                start = 0.0 if fresh and r.start else gz[r, c]
                gz[r, c] = sum((dot(zall[g, r, :], gram[g, :, c]) for g in sources), start)

    def prepare(h):
        c = cols(h, d)
        dq = jnp.exp((pos[...] + 1.0) * lg[h, :, 0:d] + cum[...])
        o, ot = o_buf[:, c], ot_buf[:, c]
        r = lax.rsqrt(jnp.mean(o * o, axis=1, keepdims=True) + EPS)
        m = r * r * jnp.mean(o * ot, axis=1, keepdims=True)
        zf = o * r
        o_buf[:, c] = zf
        ot_buf[:, c] = r * ot - zf * m
        r_buf[:, c] = jnp.broadcast_to(r, o.shape)
        rb_buf[:, c] = jnp.broadcast_to(m, o.shape)
        q_turned[c, :] = (q[:, c].astype(F32) * dq).T.astype(BF16)
        qt_turned[c, :] = (qt[:, c].astype(F32) * dq).T.astype(BF16)

    goal_tile(0)
    gathers[0].round(1)
    relay(0)
    gathers[1].round(1)
    goal_tile(1)
    relay(1)
    gathers[0].round(2)
    goal_tile(2)
    gathers[1].round(2)
    relay(2)
    gathers[0].round(3)
    goal_tile(3)
    gathers[1].round(3)
    relay(3)
    gathers[0].round(4)
    relay(4)
    pl.loop(0, 4)(prepare)
    gathers[1].round(4)
    relay(5)
    gathers[0].round(5)
    relay_early(6)
    pl.loop(4, 8)(prepare)
    gathers[1].round(5)
    gathers[0].round(6)
    add_whole(0, 2, z, fresh=True)
    relay_early(7)
    gathers[1].round(6)
    add_whole(2, 4, z, fresh=True)
    add_whole(0, 2, up, down)
    forward_late()
    add_whole(2, 4, up, down)
    distant(0, 4)
    add((0, 1), far)
    distant(4, 2)
    add((2,), far)
    distant(6, 2)
    add((3,), far)

    def norm_back(h, target, i):
        c = cols(h, d)
        zf, ztf = o_buf[:, c], ot_buf[:, c]
        gzh, gzt = gz[0:length, c], gz[length:, c]
        a = jnp.mean(zf * gzh, axis=1, keepdims=True)
        at = jnp.mean(ztf * gzh + zf * gzt, axis=1, keepdims=True)
        r = r_buf[:, c]
        g = r * (gzh - zf * a)
        gt = r * (gzt - ztf * a - zf * at) - rb_buf[:, c] * g
        for value, top, rest in ((g, g_buf, g_rest), (gt, gt_buf, gt_rest)):
            high = value.astype(BF16)
            top[:, c] = high
            rest[:, c] = (value - high.astype(F32)).astype(BF16)
        both = dot(q_turned[c, :], jnp.concatenate([g, gt], axis=1).astype(BF16))
        target[i, 0] = both[:, :d].astype(BF16)
        target[i, 1] = (both[:, d:] + dot(qt_turned[c, :], g.astype(BF16))).astype(BF16)

    def norm_part(part, whose, target):
        pl.loop(2 * part, 2 * part + 2, unroll=2)(lambda i: norm_back(whose(i), target, i))

    norm_part(0, backward.theirs, backward.gift)
    backward.give(0)
    norm_part(1, backward.theirs, backward.gift)
    backward.give(1)
    norm_part(0, backward.mine, backward.own)
    backward.give_wait(0)
    backward.combine(0)
    backward.out(0)
    norm_part(1, backward.mine, backward.own)
    backward.give_wait(1)
    backward.combine(1)
    backward.out(1)

    def inner_back(h):
        c = cols(h, d)
        w = weights_of(h, d, lg, dist, fall)
        dq = jnp.exp((pos[...] + 1.0) * lg[h, :, 0:d] + cum[...])
        qh, kh, vh, qth, kth, vth, g, gt = (x[:, c] for x in (q, k, v, qt, kt, vt, g_buf, gt_buf))
        a = dot(qh, kh, ((1,), (1,)))
        at = dot(jnp.concatenate([qth, qh], axis=1), jnp.concatenate([kh, kth], axis=1), ((1,), (1,)))
        p = (a * w).astype(BF16)
        pt = (at * w).astype(BF16)
        g_lo, gt_lo = g_rest[:, c], gt_rest[:, c]
        b = dot(jnp.concatenate([g, g_lo], axis=1), jnp.concatenate([vh, vh], axis=1), ((1,), (1,)))
        b = (b * w).astype(BF16)
        bt = dot(
            jnp.concatenate([gt, gt_lo, g, g_lo], axis=1), jnp.concatenate([vh, vh, vth, vth], axis=1), ((1,), (1,))
        )
        bt = (bt * w).astype(BF16)
        s, st = forward.state[h, 0], forward.state[h, 1]
        outer = dot(jnp.concatenate([gt, g], axis=1), jnp.concatenate([s, st], axis=1), ((1,), (1,)))
        hq[:, c] = (
            dot(jnp.concatenate([bt, b], axis=1), jnp.concatenate([kh, kth], axis=0)) + dq * outer
        ).astype(BF16)
        hk_buf[:, c] = dot(jnp.concatenate([bt, b], axis=0), jnp.concatenate([qh, qth], axis=0), ((0,), (0,)))
        hv_buf[:, c] = dot(
            jnp.concatenate([pt, p, pt, p], axis=0), jnp.concatenate([g, gt, g_lo, gt_lo], axis=0), ((0,), (0,))
        )

    pl.loop(0, 4, unroll=2)(inner_back)
    forward.finish()
    for gather in gathers:
        gather.finish()

    pltpu.make_async_copy(totals, totals, cs.at[0]).wait()
    pltpu.make_async_copy(picked.at[0:3], picked.at[0:3], ws.at[0]).wait()
    pltpu.make_async_copy(zall.at[0:3], zall.at[0:3], zs.at[0]).wait()

    backward.out_wait(0)
    backward.scan(0)
    backward.home(0)
    backward.out_wait(1)
    backward.scan(1)
    backward.home(1)
    pl.loop(4, heads, unroll=2)(inner_back)
    pltpu.make_async_copy(hq, results[0], out_sem.at[0]).start()

    def last(i):
        h = lax.rem(backward.mine(i), heads)
        c = cols(h, d)
        w = scale * jnp.exp((length - 1.0 - pos[...]) * lg[h, :, 0:d] + (KEPT_LOG * total - cum[...]))
        s, st = backward.state[h, 0], backward.state[h, 1]
        ks = dot(jnp.concatenate([v[:, c], vt[:, c]], axis=1), jnp.concatenate([st, s], axis=1), ((1,), (1,)))
        vs = dot(jnp.concatenate([k[:, c], kt[:, c]], axis=1), jnp.concatenate([st, s], axis=0))
        hk[:, c] = (hk_buf[:, c] + w * ks).astype(BF16)
        hv[:, c] = (hv_buf[:, c] + w * vs).astype(BF16)

    def emit(kind, h):
        c = cols(h, d)
        pltpu.make_async_copy((hk, hv)[kind].at[:, c], results[1 + kind].at[:, c], out_sem.at[1 + kind]).start()

    def finish(i):
        last(i)
        emit(0, lax.rem(backward.mine(i), heads))
        emit(1, lax.rem(backward.mine(i), heads))

    backward.home_wait(0)
    backward.settle(0)
    finish(0)
    finish(1)
    backward.home_wait(1)
    backward.settle(1)
    finish(2)
    finish(3)
    for i in range(heads // 2):
        backward.settle_wait(i)
        finish(heads // 2 + i)
    backward.finish()
    for kind, buffer in enumerate((hq, hk, hv)):
        pltpu.make_async_copy(buffer, results[kind], out_sem.at[kind]).wait()


def store_kernel(*refs):
    copies = [pltpu.make_async_copy(refs[i], refs[3 + i], refs[6].at[i]) for i in range(3)]
    for copy in copies:
        copy.start()
    for copy in copies:
        copy.wait()


def on_device(n, groups, probe, source, content, probe_t, source_t, content_t, table, flags, weight, goal):
    length, width = probe.shape
    heads = table.shape[0]
    d = width // heads
    flags = flags.reshape(1, length)
    vmem, hbm = (pl.BlockSpec(memory_space=m) for m in (pltpu.VMEM, pltpu.HBM))
    pair = pltpu.VMEM((heads // 2, 2, d, d), BF16)
    slots = pltpu.VMEM((n // 2 * Scan.PARTS, 2 * heads * d // n // Scan.PARTS, d), BF16)
    scan = [pair, pair, pair, slots, slots, slots, slots, pltpu.VMEM((heads, 2, d, d), BF16), pair]
    narrow, wide = pltpu.VMEM((length, width), BF16), pltpu.VMEM((length, width), F32)
    rows = width // n
    dma = pltpu.SemaphoreType.DMA
    out = jax.ShapeDtypeStruct((length, width), BF16)
    results = pl.pallas_call(
        functools.partial(kernel, n, heads, groups),
        out_shape=(out, out, out),
        in_specs=[hbm] * 10,
        out_specs=[pl.BlockSpec(memory_space=pl.ANY)] * 3,
        scratch_shapes=[
            narrow, narrow, pltpu.VMEM((4, length, width), BF16), pltpu.VMEM(weight.shape, BF16), pltpu.VMEM(goal.shape, BF16),
            pltpu.VMEM((length, length), F32), pltpu.VMEM((length, length), F32),
            pltpu.VMEM((length, d), F32), pltpu.VMEM((length, d), F32),
            pltpu.VMEM((heads, 1, length), F32), pltpu.VMEM((1, 1, d), F32), pltpu.VMEM((2, 1, d), F32), pltpu.VMEM((n // 2, 1, d), F32),
            *scan, *scan,
            pltpu.VMEM((groups, rows, weight.shape[1]), BF16),
            pltpu.VMEM((groups, width, width), BF16),
            pltpu.VMEM((groups, 2 * length, width), BF16),
            pltpu.VMEM((2 * length, width), F32),
            wide, wide, narrow, narrow, wide, wide,
            *[dma((4 + heads // 2,)), dma((4 * Scan.PARTS,))] * 2,
            dma((9,)), dma((1,)), dma((2,)), dma((1,)), dma((3,)), dma((2,)), dma((26,)), dma((1,)), dma((heads + 3,)),
            narrow, narrow, narrow, narrow, narrow, wide, wide,
            pltpu.VMEM((width, length), BF16), pltpu.VMEM((width, length), BF16), pltpu.SMEM(table.shape, jnp.int32), pltpu.VMEM(flags.shape, jnp.int32),
            dma((3,)),
        ],
        compiler_params=pltpu.CompilerParams(collective_id=0, has_side_effects=True, vmem_limit_bytes=52 << 20),
        name="retention_hvp",
    )(probe, source, content, probe_t, source_t, content_t, *(pltpu.with_memory_space_constraint(x, pltpu.HBM) for x in (table, flags)), weight, goal)
    return pl.pallas_call(
        store_kernel,
        out_shape=(out, out, out),
        in_specs=[vmem] * 3,
        out_specs=[hbm] * 3,
        scratch_shapes=[dma((3,))],
        compiler_params=pltpu.CompilerParams(vmem_limit_bytes=4 << 20),
        name="store",
    )(*results)


def solution(mesh):
    n, groups = mesh.shape["seq"], mesh.shape["head"]
    both = P("seq", "head")
    return jax.shard_map(
        functools.partial(on_device, n, groups),
        mesh=mesh,
        in_specs=(both,) * 6 + (P("head"), P("seq"), P("head", None), P("seq", None)),
        out_specs=(both,) * 3,
        check_vma=False,
    )
```

```python
import functools
import math

import jax
import jax.numpy as jnp
from jax import lax
from jax.experimental import pallas as pl
from jax.experimental.pallas import tpu as pltpu
from jax.sharding import PartitionSpec as P

LEVELS = 8
KEPT_LOG = math.log(0.7)
EPS = 1e-06
F32 = jnp.float32
BF16 = jnp.bfloat16
MESH = pl.DeviceIdType.MESH
FAR = 1e9
UNROLL = 2


def dot(a, b, dims=((1,), (0,))):
    return lax.dot_general(a, b, (dims, ((), ())), preferred_element_type=F32)


def cols(h, d):
    return pl.ds(pl.multiple_of(h * d, d), d)


def reset_counts(flags_ref, pos, cum):
    t = pos.shape[0]
    row = lax.broadcasted_iota(jnp.int32, (t, t), 0)
    col = lax.broadcasted_iota(jnp.int32, (t, t), 1)
    flags = jnp.broadcast_to(flags_ref[...].astype(F32), (t, t))
    cum_col = jnp.sum(jnp.where(col <= row, flags, 0.0), axis=1, keepdims=True)
    pos[...] = lax.broadcasted_iota(jnp.int32, pos.shape, 0).astype(F32)
    cum[...] = KEPT_LOG * jnp.broadcast_to(cum_col, cum.shape)


def decay_tables(flags_ref, dist, fall):
    t = dist.shape[0]
    row = lax.broadcasted_iota(jnp.int32, (t, t), 0)
    col = lax.broadcasted_iota(jnp.int32, (t, t), 1)
    flags = jnp.broadcast_to(flags_ref[...].astype(F32), (t, t))
    cum_col = jnp.sum(jnp.where(col <= row, flags, 0.0), axis=1, keepdims=True)
    flag_col = jnp.sum(jnp.where(col == row, flags, 0.0), axis=1, keepdims=True)
    cum_row = jnp.sum(jnp.where(row <= col, flag_col, 0.0), axis=0, keepdims=True)
    dist[...] = jnp.where(row >= col, (row - col).astype(F32), FAR)
    fall[...] = KEPT_LOG * (cum_col - cum_row)


def barrier_start(n, me, up, down):
    barrier = pltpu.get_barrier_semaphore()
    for z in (up, down):
        pl.semaphore_signal(barrier, inc=1, device_id={"head": z}, device_id_type=MESH)

    @pl.loop(1, n)
    def _(step):
        pl.semaphore_signal(barrier, inc=1, device_id={"seq": lax.rem(me + step, n)}, device_id_type=MESH)


def barrier_end(n):
    pl.semaphore_wait(pltpu.get_barrier_semaphore(), n + 1)


def weights_of(h, d, lg_ref, dist, fall):
    return jnp.exp(dist[...] * lg_ref[h] + fall[...]) * (d ** -0.5)


def remote(src, dst, send_sem, recv_sem, **where):
    return pltpu.make_async_remote_copy(
        src_ref=src, dst_ref=dst, send_sem=send_sem, recv_sem=recv_sem, device_id=where, device_id_type=MESH
    )


def arrival(dst, recv_sem):
    pltpu.make_async_copy(dst, dst, recv_sem).wait()


class GramGather:
    def __init__(self, me, full, part, parts, send_sem, recv_sem):
        c = lax.rem(me, 2)
        x, y = lax.rem(me // 2, 4), me // 8
        self.me, self.c, self.f, self.s = me, c, x + c * (y - x), y + c * (x - y)
        columns = full.shape[2] // parts
        self.full = full.at[:, :, part * columns:(part + 1) * columns]
        self.send_sem, self.recv_sem, self.base = send_sem.at[part], recv_sem, 13 * part
        self.rows = full.shape[1] // 32

    def at(self, df, s_off, absolute=False):
        f = df if absolute else lax.rem(self.f + df + 4, 4)
        s = lax.rem(self.s + s_off + 4, 4)
        return (f * (1 + 3 * self.c) + s * (4 - 3 * self.c)) * 2 + self.c

    def view(self, piece, half=None):
        rows = pl.ds(pl.multiple_of(piece * self.rows, self.rows), self.rows)
        if half is None:
            return self.full.at[:, rows, :]
        return self.full.at[2 * half:2 * half + 2, rows, :]

    def send(self, piece, to, lane, half=None):
        view = self.view(piece, half)
        remote(view, view, self.send_sem, self.recv_sem.at[self.base + lane], seq=to).start()

    def wait(self, piece, lane):
        arrival(self.view(piece), self.recv_sem.at[self.base + lane])

    def spread(self, piece, df):
        self.send(piece, self.at(0, 1), self.lane(-1, df))
        self.send(piece, self.at(0, -1), self.lane(1, df))
        self.sideways(piece)

    def sideways(self, piece):
        self.send(piece, self.me + 1 - 2 * self.c, 12)

    def lane(self, step, df):
        return 3 + (4 if step == 1 else 0) + df % 4

    def pass_on(self, step, df, half):
        piece = self.at(df, step)
        self.wait(piece, self.lane(step, df))
        self.send(piece, self.at(0, -step), 11, half)
        self.sideways(piece)

    def round(self, k):
        if k == 0:
            self.send(self.me, self.at(1, 0), 0)
            self.send(self.me, self.at(-1, 0), 1)
            self.spread(self.me, 0)
        elif k == 1:
            for step, half in ((-1, 0), (1, 1)):
                self.wait(self.at(step, 0), half)
                self.send(self.at(step, 0), self.at(-step, 0), 2, half)
            for step in (-1, 1):
                self.spread(self.at(step, 0), step)
            for step, half in ((-1, 0), (1, 1)):
                self.pass_on(step, 0, half)
        elif k == 2:
            self.wait(self.at(2, 0), 2)
            self.spread(self.at(2, 0), 2)
        elif k == 3:
            for df in (-1, 1):
                for step, half in ((-1, 0), (1, 1)):
                    self.pass_on(step, df, half)
        elif k == 4:
            for step, half in ((-1, 0), (1, 1)):
                self.pass_on(step, 2, half)
        elif k == 5:
            four = self.full.at[:, 0:4 * self.rows, :]
            arrival(four, self.recv_sem.at[self.base + 11])
            for df in range(4):
                self.sideways(self.at(df, 2))
        else:
            arrival(self.full.at[:, 0:16 * self.rows, :], self.recv_sem.at[self.base + 12])

    def finish(self):
        sent = self.full.at[:, 0:31 * self.rows, :]
        pltpu.make_async_copy(sent, sent, self.send_sem).wait()


class Scan:
    PARTS = 2

    def __init__(self, me, n, heads, length, lg, count, totals, buffers, sems, reverse):
        self.own, self.gift, self.peer, self.tot, self.recv, self.back, self.entry, self.state, self.gift2 = buffers
        self.pair_sem, self.hop_sem = sems
        self.c, self.chip, self.chips = lax.rem(me, 2), me // 2, n // 2
        self.sibling = me + 1 - 2 * self.c
        self.half = heads // 2
        self.step = self.half // self.PARTS
        self.length, self.lg, self.count, self.totals, self.reverse = length, lg, count, totals, reverse
        self.per = self.chips // self.step
        self.rows = self.tot.shape[1] // 2
        self.d = self.tot.shape[2]

    def mine(self, i):
        return self.half * self.c + i

    def theirs(self, i):
        return self.half * (1 - self.c) + i

    def members(self, part):
        return range(part * self.step, (part + 1) * self.step)

    def give(self, part):
        some = slice(part * self.step, (part + 1) * self.step)
        remote(
            self.gift.at[some], self.peer.at[some], self.pair_sem.at[0], self.pair_sem.at[2 + part], seq=self.sibling
        ).start()

    def give_wait(self, part):
        arrival(self.peer.at[part * self.step:(part + 1) * self.step], self.pair_sem.at[2 + part])

    def decay(self, h, core):
        return jnp.exp(float(self.length) * self.lg[h, :, 0:self.d] + KEPT_LOG * self.count[core])

    def ordered(self, i, half):
        mine, peer = self.own[i, half].astype(F32), self.peer[i, half].astype(F32)
        return jnp.where(self.c == 0, mine, peer), jnp.where(self.c == 0, peer, mine)

    def slices(self, i):
        first = (i // self.step) * self.chips + (i % self.step) * self.per
        return slice(first, first + self.per)

    def combine(self, part):
        for i in self.members(part):
            factor = self.decay(self.mine(i), 0 if self.reverse else 1)
            for half in range(2):
                first, second = self.ordered(i, half)
                total = first + factor * second if self.reverse else first * factor + second
                self.tot[self.slices(i), half * self.rows:(half + 1) * self.rows, :] = (
                    total.astype(BF16).reshape(self.per, self.rows, self.d)
                )

    def others(self):
        x, y = lax.rem(self.chip, 4), self.chip // 4
        for dy, dx in sorted(
            ((a, b) for a in range(4) for b in range(4) if a or b), key=lambda t: -min(t[0], 4 - t[0]) - min(t[1], 4 - t[1])
        ):
            yield lax.rem(y + dy, 4) * 4 + lax.rem(x + dx, 4)

    def spread(self, part, src, dst, hop):
        base = part * self.chips
        send_sem, recv_sem = self.hop_sem.at[4 * part + 2 * hop], self.hop_sem.at[4 * part + 2 * hop + 1]
        for p in self.others():
            remote(src.at[base + p], dst.at[base + self.chip], send_sem, recv_sem, seq=2 * p + self.c).start()

    def collect(self, part, src, dst, hop):
        sent, got = src.at[0:self.chips - 1], dst.at[0:self.chips - 1]
        pltpu.make_async_copy(sent, sent, self.hop_sem.at[4 * part + 2 * hop]).wait()
        arrival(got, self.hop_sem.at[4 * part + 2 * hop + 1])

    def out(self, part):
        self.spread(part, self.tot, self.recv, 0)

    def out_wait(self, part):
        self.collect(part, self.tot, self.recv, 0)

    def scan(self, part):
        base = part * self.chips
        self.recv[base + self.chip] = self.tot[base + self.chip]
        lg = self.lg[self.mine(part * self.step + self.chip // self.per), :, 0:self.d]

        def step(i, run):
            p = self.chips - 1 - i if self.reverse else i
            self.back[base + p] = run.astype(BF16)
            factor = jnp.exp(2.0 * self.length * lg + KEPT_LOG * self.totals[p])
            return run * factor + self.recv[base + p].astype(F32)

        lax.fori_loop(0, self.chips, step, jnp.zeros(self.recv.shape[1:], F32), unroll=self.chips)
        self.entry[base + self.chip] = self.back[base + self.chip]

    def home(self, part):
        self.spread(part, self.back, self.entry, 1)

    def home_wait(self, part):
        self.collect(part, self.back, self.entry, 1)

    def settle(self, part):
        for i in self.members(part):
            factor = self.decay(self.mine(i), 1 if self.reverse else 0)
            for half in range(2):
                first, second = self.ordered(i, half)
                edge = self.entry[self.slices(i), half * self.rows:(half + 1) * self.rows, :]
                edge = edge.reshape(self.d, self.d).astype(F32)
                inside = factor * edge + (second if self.reverse else first)
                keep = (self.c == 1) if self.reverse else (self.c == 0)
                self.gift2[i, half] = jnp.where(keep, inside, edge).astype(BF16)
                self.state[self.mine(i), half] = jnp.where(keep, edge, inside).astype(BF16)
        for i in self.members(part):
            remote(
                self.gift2.at[i], self.state.at[self.mine(i)],
                self.pair_sem.at[1], self.pair_sem.at[4 + i], seq=self.sibling,
            ).start()

    def settle_wait(self, i):
        arrival(self.state.at[self.theirs(i)], self.pair_sem.at[4 + i])

    def finish(self):
        pltpu.make_async_copy(self.gift, self.gift, self.pair_sem.at[0]).wait()
        pltpu.make_async_copy(self.gift2, self.gift2, self.pair_sem.at[1]).wait()


def kernel(n, heads, groups, *refs):
    inputs, (table_hbm, flags_hbm, w_hbm, goal_hbm), results = refs[:6], refs[6:10], refs[10:13]
    (q, qt, both_kv, weight, goal, dist, fall, pos, cum, lg, mine, count, totals) = refs[13:26]
    k, v, kt, vt = (both_kv.at[i] for i in range(4))
    refs = (None,) * 2 + refs
    ahead, behind = refs[28:37], refs[37:46]
    (picked, gram, zall, gz, o_buf, ot_buf, g_buf, gt_buf, hk_buf, hv_buf) = refs[46:56]
    ahead_sems, behind_sems = refs[56:58], refs[58:60]
    (load_sem, cs, cr, ws, wr, gs, gr, zs, zr) = refs[60:69]
    (hq, hk, hv, g_rest, gt_rest, r_buf, rb_buf, q_turned, qt_turned, table, flags, out_sem) = refs[69:]
    me, z = lax.axis_index("seq"), lax.axis_index("head")
    up, down = lax.rem(z + 1, groups), lax.rem(z + groups - 1, groups)
    far = lax.rem(z + 2, groups)
    length, width = q.shape
    d = width // heads
    scale = d ** -0.5
    rows = width // n
    mine_rows = pl.ds(pl.multiple_of(me * rows, rows), rows)
    core = lax.rem(me, 2)
    mine_columns = pl.ds(pl.multiple_of(core * (width // 2), width // 2), width // 2)
    their_columns = pl.ds(pl.multiple_of((1 - core) * (width // 2), width // 2), width // 2)
    sources = (table_hbm, flags_hbm, w_hbm.at[mine_rows], inputs[0], inputs[3], w_hbm, goal_hbm)
    loads = [
        pltpu.make_async_copy(src, dst, load_sem.at[i])
        for i, (src, dst) in enumerate(zip(sources, (table, flags, picked.at[z], q, qt, weight, goal)))
    ]
    loads[0].start()
    loads[1].start()
    for sem, columns in ((7, their_columns), (8, mine_columns)):
        for i, j in enumerate((1, 2, 4, 5)):
            pltpu.make_async_copy(inputs[j].at[:, columns], both_kv.at[i, :, columns], load_sem.at[sem]).start()
        if sem == 7:
            loads[2].start()
    for load in loads[3:]:
        load.start()
    barrier_start(n, me, up, down)
    loads[0].wait()
    loads[1].wait()

    @pl.loop(0, heads)
    def _(h):
        fraction = jnp.full((1, length), table[h], jnp.int32).astype(F32) / (LEVELS - 1)
        rates = jnp.exp(math.log(1.0 / 32.0) + fraction * math.log(16.0 / (length * n)))
        lg[h] = jnp.log1p(-rates)

    reset_counts(flags, pos, cum)
    total = jnp.broadcast_to(jnp.sum(flags[...].astype(F32), axis=1, keepdims=True), (1, 128))
    mine[0] = total
    count[core] = total
    forward = Scan(me, n, heads, length, lg, count, totals, ahead, ahead_sems, False)
    backward = Scan(me, n, heads, length, lg, count, totals, behind, behind_sems, True)
    arrival(both_kv.at[:, :, their_columns], load_sem.at[7])

    def own_state(h, target, i):
        c = cols(h, d)
        w = scale * jnp.exp((length - 1.0 - pos[...]) * lg[h, :, 0:d] + (KEPT_LOG * total - cum[...]))
        kw = (k[:, c].astype(F32) * w).astype(BF16)
        ktw = (kt[:, c].astype(F32) * w).astype(BF16)
        both = dot(kw, jnp.concatenate([v[:, c], vt[:, c]], axis=1), ((0,), (0,)))
        target[i, 0] = both[:, :d].astype(BF16)
        target[i, 1] = (both[:, d:] + dot(ktw, v[:, c], ((0,), (0,)))).astype(BF16)

    def own_part(part, whose, target):
        pl.loop(2 * part, 2 * part + 2, unroll=2)(lambda i: own_state(whose(i), target, i))

    own_part(0, forward.theirs, forward.gift)
    own_part(1, forward.theirs, forward.gift)
    loads[2].wait()
    barrier_end(n)
    half = rows // 2
    low, high = slice(0, half), slice(half, rows)

    def w_send(slot, part, lane, to):
        remote(picked.at[slot, part], picked.at[slot, part], ws.at[0], wr.at[lane], head=to).start()

    w_send(z, low, 0, up)
    w_send(z, high, 1, down)
    w_send(z, high, 2, up)
    w_send(z, low, 2, down)
    remote(mine.at[0], count.at[core], cs.at[0], cr.at[0], seq=forward.sibling).start()

    forward.give(0)
    forward.give(1)
    arrival(both_kv.at[:, :, mine_columns], load_sem.at[8])
    own_part(0, forward.mine, forward.own)
    arrival(count.at[1 - core], cr.at[0])
    totals[forward.chip] = count[0] + count[1]
    forward.give_wait(0)
    forward.combine(0)
    for p in forward.others():
        remote(totals.at[forward.chip], totals.at[forward.chip], cs.at[0], cr.at[1], seq=2 * p + core).start()
    forward.out(0)
    own_part(1, forward.mine, forward.own)
    forward.give_wait(1)
    forward.combine(1)
    forward.out(1)
    loads[3].wait()
    loads[4].wait()

    def inner(h):
        c = cols(h, d)
        w = weights_of(h, d, lg, dist, fall)
        a = dot(q[:, c], k[:, c], ((1,), (1,)))
        at = dot(
            jnp.concatenate([qt[:, c], q[:, c]], axis=1), jnp.concatenate([k[:, c], kt[:, c]], axis=1), ((1,), (1,))
        )
        p = (a * w).astype(BF16)
        pt = (at * w).astype(BF16)
        both = dot(p, jnp.concatenate([v[:, c], vt[:, c]], axis=1))
        o_buf[:, c] = both[:, :d]
        ot_buf[:, c] = both[:, d:] + dot(pt, v[:, c])

    decay_tables(flags, dist, fall)
    pl.loop(0, heads // 2, unroll=2)(inner)
    arrival(picked.at[down, low], wr.at[0])
    w_send(down, low, 2, up)
    arrival(picked.at[up, high], wr.at[1])
    w_send(up, high, 2, down)
    arrival(totals.at[0:n // 2 - 1], cr.at[1])
    forward.out_wait(0)
    forward.scan(0)
    forward.home(0)
    forward.out_wait(1)
    forward.scan(1)
    forward.home(1)
    pl.loop(heads // 2, heads, unroll=2)(inner)
    tile = 256

    def gram_tile(i):
        c = slice(i * tile, (i + 1) * tile)
        part = dot(picked[...].reshape(groups * rows, weight.shape[1]), weight[c, :], ((1,), (1,)))
        gram[:, mine_rows, c] = part.astype(BF16).reshape(groups, rows, tile)

    gathers = [GramGather(me, gram, part, 2, gs, gr) for part in range(2)]

    def head_of(i):
        part, place = i // 4, i % 4
        return forward.mine(2 * part + place) if place < 2 else forward.theirs(2 * part + place - 2)

    def z_send(i):
        c = cols(head_of(i), d)
        remote(zall.at[z, :, c], zall.at[z, :, c], zs.at[0], zr.at[i], head=up).start()
        remote(zall.at[z, :, c], zall.at[z, :, c], zs.at[0], zr.at[i], head=down).start()

    def output(i):
        h = head_of(i)
        c = cols(h, d)
        dq = jnp.exp((pos[...] + 1.0) * lg[h, :, 0:d] + cum[...])
        s, st = forward.state[h, 0], forward.state[h, 1]
        both = dot(q[:, c], jnp.concatenate([s, st], axis=1))
        o = o_buf[:, c] + dq * both[:, :d]
        ot = ot_buf[:, c] + dq * (both[:, d:] + dot(qt[:, c], s))
        o_buf[:, c] = o
        ot_buf[:, c] = ot
        r = lax.rsqrt(jnp.mean(o * o, axis=1, keepdims=True) + EPS)
        m = jnp.mean(o * ot, axis=1, keepdims=True)
        zall[z, 0:length, c] = (o * r).astype(BF16)
        zall[z, length:, c] = (r * ot - o * (r * r * r * m)).astype(BF16)

        z_send(i)

    forward.home_wait(0)
    forward.settle(0)
    output(0)
    output(1)
    arrival(picked.at[0:2], wr.at[2])
    loads[5].wait()
    gram_tile(0)
    gram_tile(1)
    gathers[0].round(0)
    for i in range(2):
        forward.settle_wait(i)
        output(2 + i)
    gram_tile(2)
    gram_tile(3)
    gathers[1].round(0)
    forward.home_wait(1)
    forward.settle(1)
    output(4)
    output(5)
    for i in range(2):
        forward.settle_wait(2 + i)
        output(6 + i)
    loads[6].wait()

    def goal_tile(i):
        c = slice(i * tile, (i + 1) * tile)
        gz[0:length, c] = -dot(goal[...], weight[c, :], ((1,), (1,)))

    groups_of = (0, 0, 0, 0, 1, 1, 2, 2)

    def near(i):
        arrival(zall.at[0:2, :, cols(head_of(i), d)], zr.at[i])

    def forward_on(i):
        c = cols(head_of(i), d)
        lane = heads + groups_of[i]
        piece = zall.at[down, 0:length, c]
        remote(piece, piece, zs.at[0], zr.at[lane], head=up).start()
        piece = zall.at[up, length:, c]
        remote(piece, piece, zs.at[0], zr.at[lane], head=down).start()

    def relay(i):
        near(i)
        forward_on(i)

    def relay_early(i):
        near(i)
        pl.when(core == 0)(lambda: forward_on(i))

    def forward_late():
        @pl.when(core == 1)
        def _():
            forward_on(6)
            forward_on(7)

    def distant(first, number):
        arrival(zall.at[far, :, 0:number * d], zr.at[heads + groups_of[first]])

    def add(pairs, source):
        parts = [pl.ds(pl.multiple_of(head_of(2 * p) * d, 2 * d), 2 * d) for p in pairs]

        for i in range(width // tile):
            c = slice(i * tile, (i + 1) * tile)
            for r in (slice(0, length), slice(length, 2 * length)):
                gz[r, c] = sum((dot(zall[source, r, p], gram[source, p, c]) for p in parts), gz[r, c])

    def add_whole(first, last, *sources, fresh=False):
        for i in range(first, last):
            c = slice(i * tile, (i + 1) * tile)
            for r in (slice(0, length), slice(length, 2 * length)):
                start = 0.0 if fresh and r.start else gz[r, c]
                gz[r, c] = sum((dot(zall[g, r, :], gram[g, :, c]) for g in sources), start)

    def prepare(h):
        c = cols(h, d)
        dq = jnp.exp((pos[...] + 1.0) * lg[h, :, 0:d] + cum[...])
        o, ot = o_buf[:, c], ot_buf[:, c]
        r = lax.rsqrt(jnp.mean(o * o, axis=1, keepdims=True) + EPS)
        m = r * r * jnp.mean(o * ot, axis=1, keepdims=True)
        zf = o * r
        o_buf[:, c] = zf
        ot_buf[:, c] = r * ot - zf * m
        r_buf[:, c] = jnp.broadcast_to(r, o.shape)
        rb_buf[:, c] = jnp.broadcast_to(m, o.shape)
        q_turned[c, :] = (q[:, c].astype(F32) * dq).T.astype(BF16)
        qt_turned[c, :] = (qt[:, c].astype(F32) * dq).T.astype(BF16)

    goal_tile(0)
    gathers[0].round(1)
    relay(0)
    gathers[1].round(1)
    goal_tile(1)
    relay(1)
    gathers[0].round(2)
    goal_tile(2)
    gathers[1].round(2)
    relay(2)
    gathers[0].round(3)
    goal_tile(3)
    gathers[1].round(3)
    relay(3)
    gathers[0].round(4)
    relay(4)
    pl.loop(0, 4)(prepare)
    gathers[1].round(4)
    relay(5)
    gathers[0].round(5)
    relay_early(6)
    pl.loop(4, 8)(prepare)
    gathers[1].round(5)
    gathers[0].round(6)
    add_whole(0, 2, z, fresh=True)
    relay_early(7)
    gathers[1].round(6)
    add_whole(2, 4, z, fresh=True)
    add_whole(0, 2, up, down)
    forward_late()
    add_whole(2, 4, up, down)
    distant(0, 4)
    add((0, 1), far)
    distant(4, 2)
    add((2,), far)
    distant(6, 2)
    add((3,), far)

    def norm_back(h, target, i):
        c = cols(h, d)
        zf, ztf = o_buf[:, c], ot_buf[:, c]
        gzh, gzt = gz[0:length, c], gz[length:, c]
        a = jnp.mean(zf * gzh, axis=1, keepdims=True)
        at = jnp.mean(ztf * gzh + zf * gzt, axis=1, keepdims=True)
        r = r_buf[:, c]
        g = r * (gzh - zf * a)
        gt = r * (gzt - ztf * a - zf * at) - rb_buf[:, c] * g
        for value, top, rest in ((g, g_buf, g_rest), (gt, gt_buf, gt_rest)):
            high = value.astype(BF16)
            top[:, c] = high
            rest[:, c] = (value - high.astype(F32)).astype(BF16)
        both = dot(q_turned[c, :], jnp.concatenate([g, gt], axis=1).astype(BF16))
        target[i, 0] = both[:, :d].astype(BF16)
        target[i, 1] = (both[:, d:] + dot(qt_turned[c, :], g.astype(BF16))).astype(BF16)

    def norm_part(part, whose, target):
        pl.loop(2 * part, 2 * part + 2, unroll=2)(lambda i: norm_back(whose(i), target, i))

    norm_part(0, backward.theirs, backward.gift)
    backward.give(0)
    norm_part(1, backward.theirs, backward.gift)
    backward.give(1)
    norm_part(0, backward.mine, backward.own)
    backward.give_wait(0)
    backward.combine(0)
    backward.out(0)
    norm_part(1, backward.mine, backward.own)
    backward.give_wait(1)
    backward.combine(1)
    backward.out(1)

    def inner_back(h):
        c = cols(h, d)
        w = weights_of(h, d, lg, dist, fall)
        dq = jnp.exp((pos[...] + 1.0) * lg[h, :, 0:d] + cum[...])
        qh, kh, vh, qth, kth, vth, g, gt = (x[:, c] for x in (q, k, v, qt, kt, vt, g_buf, gt_buf))
        a = dot(qh, kh, ((1,), (1,)))
        at = dot(jnp.concatenate([qth, qh], axis=1), jnp.concatenate([kh, kth], axis=1), ((1,), (1,)))
        p = (a * w).astype(BF16)
        pt = (at * w).astype(BF16)
        g_lo, gt_lo = g_rest[:, c], gt_rest[:, c]
        b = dot(jnp.concatenate([g, g_lo], axis=1), jnp.concatenate([vh, vh], axis=1), ((1,), (1,)))
        b = (b * w).astype(BF16)
        bt = dot(
            jnp.concatenate([gt, gt_lo, g, g_lo], axis=1), jnp.concatenate([vh, vh, vth, vth], axis=1), ((1,), (1,))
        )
        bt = (bt * w).astype(BF16)
        s, st = forward.state[h, 0], forward.state[h, 1]
        outer = dot(jnp.concatenate([gt, g], axis=1), jnp.concatenate([s, st], axis=1), ((1,), (1,)))
        hq[:, c] = (
            dot(jnp.concatenate([bt, b], axis=1), jnp.concatenate([kh, kth], axis=0)) + dq * outer
        ).astype(BF16)
        hk_buf[:, c] = dot(jnp.concatenate([bt, b], axis=0), jnp.concatenate([qh, qth], axis=0), ((0,), (0,)))
        hv_buf[:, c] = dot(
            jnp.concatenate([pt, p, pt, p], axis=0), jnp.concatenate([g, gt, g_lo, gt_lo], axis=0), ((0,), (0,))
        )

    pl.loop(0, 4, unroll=2)(inner_back)
    forward.finish()
    for gather in gathers:
        gather.finish()

    pltpu.make_async_copy(totals, totals, cs.at[0]).wait()
    pltpu.make_async_copy(picked.at[0:3], picked.at[0:3], ws.at[0]).wait()
    pltpu.make_async_copy(zall.at[0:3], zall.at[0:3], zs.at[0]).wait()

    backward.out_wait(0)
    backward.scan(0)
    backward.home(0)
    backward.out_wait(1)
    backward.scan(1)
    backward.home(1)
    pl.loop(4, heads, unroll=2)(inner_back)
    pltpu.make_async_copy(hq, results[0], out_sem.at[0]).start()

    def last(i):
        h = lax.rem(backward.mine(i), heads)
        c = cols(h, d)
        w = scale * jnp.exp((length - 1.0 - pos[...]) * lg[h, :, 0:d] + (KEPT_LOG * total - cum[...]))
        s, st = backward.state[h, 0], backward.state[h, 1]
        ks = dot(jnp.concatenate([v[:, c], vt[:, c]], axis=1), jnp.concatenate([st, s], axis=1), ((1,), (1,)))
        vs = dot(jnp.concatenate([k[:, c], kt[:, c]], axis=1), jnp.concatenate([st, s], axis=0))
        hk[:, c] = (hk_buf[:, c] + w * ks).astype(BF16)
        hv[:, c] = (hv_buf[:, c] + w * vs).astype(BF16)

    def emit(kind, h):
        c = cols(h, d)
        pltpu.make_async_copy((hk, hv)[kind].at[:, c], results[1 + kind].at[:, c], out_sem.at[1 + kind]).start()

    def finish(i):
        last(i)
        emit(0, lax.rem(backward.mine(i), heads))
        emit(1, lax.rem(backward.mine(i), heads))

    backward.home_wait(0)
    backward.settle(0)
    finish(0)
    finish(1)
    backward.home_wait(1)
    backward.settle(1)
    finish(2)
    finish(3)
    for i in range(heads // 2):
        backward.settle_wait(i)
        finish(heads // 2 + i)
    backward.finish()
    for kind, buffer in enumerate((hq, hk, hv)):
        pltpu.make_async_copy(buffer, results[kind], out_sem.at[kind]).wait()


def store_kernel(*refs):
    copies = [pltpu.make_async_copy(refs[i], refs[3 + i], refs[6].at[i]) for i in range(3)]
    for copy in copies:
        copy.start()
    for copy in copies:
        copy.wait()


def on_device(n, groups, probe, source, content, probe_t, source_t, content_t, table, flags, weight, goal):
    length, width = probe.shape
    heads = table.shape[0]
    d = width // heads
    flags = flags.reshape(1, length)
    vmem, hbm = (pl.BlockSpec(memory_space=m) for m in (pltpu.VMEM, pltpu.HBM))
    pair = pltpu.VMEM((heads // 2, 2, d, d), BF16)
    slots = pltpu.VMEM((n // 2 * Scan.PARTS, 2 * heads * d // n // Scan.PARTS, d), BF16)
    scan = [pair, pair, pair, slots, slots, slots, slots, pltpu.VMEM((heads, 2, d, d), BF16), pair]
    narrow, wide = pltpu.VMEM((length, width), BF16), pltpu.VMEM((length, width), F32)
    rows = width // n
    dma = pltpu.SemaphoreType.DMA
    out = jax.ShapeDtypeStruct((length, width), BF16)
    results = pl.pallas_call(
        functools.partial(kernel, n, heads, groups),
        out_shape=(out, out, out),
        in_specs=[hbm] * 10,
        out_specs=[pl.BlockSpec(memory_space=pl.ANY)] * 3,
        scratch_shapes=[
            narrow, narrow, pltpu.VMEM((4, length, width), BF16), pltpu.VMEM(weight.shape, BF16), pltpu.VMEM(goal.shape, BF16),
            pltpu.VMEM((length, length), F32), pltpu.VMEM((length, length), F32),
            pltpu.VMEM((length, d), F32), pltpu.VMEM((length, d), F32),
            pltpu.VMEM((heads, 1, length), F32), pltpu.VMEM((1, 1, d), F32), pltpu.VMEM((2, 1, d), F32), pltpu.VMEM((n // 2, 1, d), F32),
            *scan, *scan,
            pltpu.VMEM((groups, rows, weight.shape[1]), BF16),
            pltpu.VMEM((groups, width, width), BF16),
            pltpu.VMEM((groups, 2 * length, width), BF16),
            pltpu.VMEM((2 * length, width), F32),
            wide, wide, narrow, narrow, wide, wide,
            *[dma((4 + heads // 2,)), dma((4 * Scan.PARTS,))] * 2,
            dma((9,)), dma((1,)), dma((2,)), dma((1,)), dma((3,)), dma((2,)), dma((26,)), dma((1,)), dma((heads + 3,)),
            narrow, narrow, narrow, narrow, narrow, wide, wide,
            pltpu.VMEM((width, length), BF16), pltpu.VMEM((width, length), BF16), pltpu.SMEM(table.shape, jnp.int32), pltpu.VMEM(flags.shape, jnp.int32),
            dma((3,)),
        ],
        compiler_params=pltpu.CompilerParams(collective_id=0, has_side_effects=True, vmem_limit_bytes=52 << 20),
        name="retention_hvp",
    )(probe, source, content, probe_t, source_t, content_t, *(pltpu.with_memory_space_constraint(x, pltpu.HBM) for x in (table, flags)), weight, goal)
    return pl.pallas_call(
        store_kernel,
        out_shape=(out, out, out),
        in_specs=[vmem] * 3,
        out_specs=[hbm] * 3,
        scratch_shapes=[dma((3,))],
        compiler_params=pltpu.CompilerParams(vmem_limit_bytes=4 << 20),
        name="store",
    )(*results)


def solution(mesh):
    n, groups = mesh.shape["seq"], mesh.shape["head"]
    both = P("seq", "head")
    return jax.shard_map(
        functools.partial(on_device, n, groups),
        mesh=mesh,
        in_specs=(both,) * 6 + (P("head"), P("seq"), P("head", None), P("seq", None)),
        out_specs=(both,) * 3,
        check_vma=False,
    )
```
